8 devices in a mesh: sys: 1 (over z), col: 2 (over y), row: 4 (over x, core).
Axes of the slice: x: 2, y: 2, z: 1, core: 2. Of those that a mesh axis runs over, the one named last changes fastest.
Arguments:
- lower_tri: float32 [2, 64, 64, 4096], P('sys', 'row', None, 'col')
Outputs:
- output 1: float32 [2, 64, 64, 4096], P('sys', 'row', None, 'col')
- output 2: float32 [2, 4, 2, 64, 64], P('sys')
- output 3: float32 [2, 4, 64, 64, 64], P('sys', None, 'row')
- output 4: float32 [2, 4, 64, 64], P('sys')
All inputs are finite; a program needn't handle non-finite values.
Results may differ from the reference program's by a relative error of at most 0.001.
Values sent between devices are 32-bit elements.
A program may use at most 1 GiB of HBM per device.

```python
import jax
import jax.numpy as jnp
from jax import lax

N = 4096
NB = 64
PANELS = 4
PROC_ROWS = 4
PROC_COLS = 2
N_BLOCKS = N // NB
MAX_PREC = lax.Precision.HIGHEST


def mat_dot(left_op, right_op):
    return jnp.dot(left_op, right_op, precision=MAX_PREC, preferred_element_type=jnp.float32)


def load_blocks(stored):
    rows_nat = stored.reshape(PROC_ROWS, N_BLOCKS // PROC_ROWS, NB, N).transpose(1, 0, 2, 3).reshape(N, N)
    return rows_nat.reshape(N, PROC_COLS, N_BLOCKS // PROC_COLS, NB).transpose(0, 2, 1, 3).reshape(N, N)


def store_rows(nat_rows, n_procs):
    n_width = nat_rows.shape[1]
    return nat_rows.reshape(N_BLOCKS // n_procs, n_procs, NB, n_width).transpose(1, 0, 2, 3).reshape(N, n_width)


def store_matrix(nat_mat):
    rows_st = store_rows(nat_mat, PROC_ROWS)
    return rows_st.reshape(N, N_BLOCKS // PROC_COLS, PROC_COLS, NB).transpose(0, 2, 1, 3).reshape(N_BLOCKS, NB, N)


def setup_inputs(seed: int = 0, part: int = 0) -> dict:
    base_key = jax.random.fold_in(jax.random.key(seed), part)
    key_noise, key_basis, key_spread = jax.random.split(base_key, 3)
    noise_mat = jax.random.normal(key_noise, (2, N, N), jnp.float32)
    sym_part = (noise_mat + jnp.swapaxes(noise_mat, 1, 2)) * (2.0 * NB) ** -0.5
    basis_vecs = jax.random.normal(key_basis, (2, N, NB), jnp.float32) * N ** -0.5
    spread_vals = jax.random.uniform(key_spread, (2, NB), jnp.float32, 2.0, 6.0) * (N / NB) ** 0.5
    strong_part = jnp.einsum('xnr,xmr->xnm', basis_vecs * spread_vals[:, None, :], basis_vecs)
    full_low = jnp.tril(sym_part + strong_part)
    return {'lower_tri': jax.vmap(store_matrix)(full_low)}


def householder_panel(panel_cols):
    row_ids = jnp.arange(panel_cols.shape[0])
    col_ids = jnp.arange(NB)

    def qr_step(col_idx, state_in):
        work_mat, refl_vecs, tau_vals = state_in
        x_col = lax.dynamic_index_in_dim(work_mat, col_idx, axis=1, keepdims=False)
        at_piv = row_ids == col_idx
        below_piv = row_ids > col_idx
        alpha_val = jnp.sum(jnp.where(at_piv, x_col, 0.0))
        sigma_val = jnp.sum(jnp.where(below_piv, x_col * x_col, 0.0))
        norm_val = jnp.sqrt(alpha_val * alpha_val + sigma_val)
        beta_val = jnp.where(alpha_val >= 0, -norm_val, norm_val)
        tau_val = (beta_val - alpha_val) / beta_val
        new_vec = jnp.where(below_piv, x_col / (alpha_val - beta_val), jnp.where(at_piv, 1.0, 0.0))
        proj_row = jnp.where(col_ids > col_idx, mat_dot(new_vec, work_mat), 0.0)
        work_mat = work_mat - (tau_val * new_vec)[:, None] * proj_row[None, :]
        new_col = jnp.where(at_piv, beta_val, jnp.where(below_piv, 0.0, x_col))
        is_col = col_ids[None, :] == col_idx
        work_mat = jnp.where(is_col, new_col[:, None], work_mat)
        refl_vecs = jnp.where(is_col, new_vec[:, None], refl_vecs)
        tau_vals = jnp.where(col_ids == col_idx, tau_val, tau_vals)
        return work_mat, refl_vecs, tau_vals

    init_state = (panel_cols, jnp.zeros_like(panel_cols), jnp.zeros((NB,), jnp.float32))
    work_mat, refl_vecs, tau_vals = lax.fori_loop(0, NB, qr_step, init_state)
    return refl_vecs, tau_vals, work_mat[:NB]


def build_tri(tau_vals, gram_mat):
    col_ids = jnp.arange(NB)

    def tri_step(col_idx, t_factor):
        s_col = jnp.where(col_ids < col_idx, lax.dynamic_index_in_dim(gram_mat, col_idx, axis=1, keepdims=False), 0.0)
        tau_val = lax.dynamic_index_in_dim(tau_vals, col_idx, axis=0, keepdims=False)
        t_col = -tau_val * mat_dot(t_factor, s_col)
        t_col = jnp.where(col_ids == col_idx, tau_val, t_col)
        return jnp.where(col_ids[None, :] == col_idx, t_col[:, None], t_factor)

    return lax.fori_loop(0, NB, tri_step, jnp.zeros((NB, NB), jnp.float32))


def reduce_matrix(stored):
    nat_mat = load_blocks(stored)
    band_list = []
    refl_list = []
    tfac_list = []
    for panel_idx in range(PANELS):
        lead_pos = panel_idx * NB
        trail_start = lead_pos + NB
        diag_blk = nat_mat[lead_pos:trail_start, lead_pos:trail_start]
        refl_vecs, tau_vals, rfac_blk = householder_panel(nat_mat[trail_start:, lead_pos:trail_start])
        t_factor = build_tri(tau_vals, mat_dot(refl_vecs.T, refl_vecs))
        trail_mat = nat_mat[trail_start:, trail_start:]
        y_raw = mat_dot(trail_mat, refl_vecs) + mat_dot(trail_mat.T, refl_vecs) - jnp.diagonal(trail_mat)[:, None] * refl_vecs
        y_mat = mat_dot(y_raw, t_factor)
        corr_mat = mat_dot(t_factor.T, mat_dot(refl_vecs.T, y_mat))
        w_mat = y_mat - 0.5 * mat_dot(refl_vecs, corr_mat)
        update = mat_dot(refl_vecs, w_mat.T) + mat_dot(w_mat, refl_vecs.T)
        nat_mat = nat_mat.at[trail_start:, trail_start:].set(trail_mat - jnp.tril(update))
        band_list.append(jnp.stack([diag_blk, rfac_blk]))
        v_full = jnp.concatenate([jnp.zeros((trail_start, NB), jnp.float32), refl_vecs], axis=0)
        refl_list.append(store_rows(v_full, PROC_ROWS).reshape(N_BLOCKS, NB, NB))
        tfac_list.append(t_factor)
    done_rows = PANELS * NB
    trail_out = jnp.pad(nat_mat[done_rows:, done_rows:], ((done_rows, 0), (done_rows, 0)))
    return store_matrix(trail_out), jnp.stack(band_list), jnp.stack(refl_list), jnp.stack(tfac_list)


def reference(lower_tri):
    trail_all, band_all, refl_all, tfac_all = lax.map(reduce_matrix, lower_tri)
    return (trail_all, band_all, refl_all, tfac_all)
```

```python
import functools

import jax
import jax.numpy as jnp
from jax import lax
from jax.experimental import pallas as pl
from jax.experimental.pallas import tpu as pltpu
from jax.sharding import PartitionSpec as P

PANELS = 4
NB = 64
N = 4096
QTR = 1024
N_CH = N // 128
TR, TC = 256, 512
F32 = jnp.float32
BF16 = jnp.bfloat16
MESH = pl.DeviceIdType.MESH
VMEM_LIMIT = 60 * 1024 * 1024


def split3(a):
    hi = a.astype(BF16)
    rest = a - hi.astype(F32)
    mid = rest.astype(BF16)
    low = (rest - mid.astype(F32)).astype(BF16)
    return hi, mid, low


def bdot(a, b, ca=1, cb=0):
    return lax.dot_general(a, b, (((ca,), (cb,)), ((), ())), preferred_element_type=F32)


def fold_rows(x):
    n = x.shape[0] // 3
    return x[2 * n :] + x[n : 2 * n] + x[:n]


def mm(a, b, cb=0):
    lhs = jnp.concatenate(split3(a), axis=0)
    b1, b2, b3 = split3(b)
    return fold_rows(bdot(lhs, b3, 1, cb) + bdot(lhs, b2, 1, cb) + bdot(lhs, b1, 1, cb))


def gram(a_ref, b_ref, mask=None):
    acc = None
    for t in range(N // 512):
        sl = slice(t * 512, (t + 1) * 512)
        lhs = jnp.concatenate(split3(a_ref[:, sl]), axis=0)
        rhs = jnp.concatenate(split3(b_ref[:, sl]), axis=0)
        part = bdot(lhs, rhs, 1, 1)
        acc = part if acc is None else acc + part
    acc = fold_rows(acc)
    return acc[:, 128:192] + acc[:, 64:128] + acc[:, 0:64]


def bcast(v):
    return jnp.broadcast_to(v, (8, 128))


def qr_step(a_ref, xcur, xnext, stats, pc, pl0, gi, s, last_of_pair, accs):
    beta_ref, inv_ref, tau_ref = stats
    lane = lax.broadcasted_iota(jnp.int32, (8, 128), 1)
    sub = lax.broadcasted_iota(jnp.int32, (8, 1), 0)
    n_g = 8 - gi
    j = gi * 8 + s
    p = pl0 + j
    rows = [slice((gi + g) * 8, (gi + g + 1) * 8) for g in range(n_g)]
    dots = [jnp.sum(acc, axis=1, keepdims=True) for acc in accs]
    pvs = [jnp.sum(jnp.where(lane == p, a_ref[pc, r, :], 0.0), axis=1, keepdims=True) for r in rows]
    sigma = jnp.sum(jnp.where(sub == s, dots[0], 0.0), axis=0, keepdims=True)
    alpha = jnp.sum(jnp.where(sub == s, pvs[0], 0.0), axis=0, keepdims=True)
    sq = alpha * alpha + sigma
    inv_norm = lax.rsqrt(sq)
    norm = jnp.sqrt(sq)
    pos = alpha >= 0
    beta = jnp.where(pos, -norm, norm)
    ninvb = jnp.where(pos, inv_norm, -inv_norm)
    denom = alpha - beta
    inv_den = 1.0 / denom
    tau = denom * ninvb
    cs = [(pv + d * inv_den) * ninvb for pv, d in zip(pvs, dots)]
    cs[0] = jnp.where(sub > s, cs[0], 0.0)
    beta_ref[pl.ds(j, 1), :] = jnp.broadcast_to(beta, (1, 128))
    inv_ref[pl.ds(j, 1), :] = jnp.broadcast_to(inv_den, (1, 128))
    tau_ref[pl.ds(j, 1), :] = jnp.broadcast_to(tau, (1, 128))
    c_next = jnp.sum(jnp.where(sub == s + 1, cs[0], 0.0), axis=0, keepdims=True)
    if last_of_pair and n_g > 1:
        c_next = c_next + jnp.where(s == 7, cs[1][0:1], 0.0)
    jn = jnp.minimum(j + 1, NB - 1)
    c_next = bcast(c_next)
    den_b = bcast(denom)
    for ch in range(N_CH):
        xt = xcur[ch]
        if ch == pc:
            xt = jnp.where(lane == p, den_b, xt)
        xn = a_ref[ch, pl.ds(jn, 8, stride=0), :] - c_next * xt
        if ch == pc:
            xn = jnp.where(lane > p + 1, xn, 0.0)
        xnext[ch] = xn
    cs = [bcast(c) for c in cs]
    out = [jnp.zeros((8, 128), F32) for _ in range(n_g)]
    for ch in range(N_CH):
        xt = xcur[ch]
        if ch == pc:
            xt = jnp.where(lane == p, den_b, xt)
        xn = xnext[ch]
        for g in range(n_g):
            a = a_ref[ch, rows[g], :] - cs[g] * xt
            a_ref[ch, rows[g], :] = a
            out[g] = out[g] + a * xn
    return tuple(out)


def qr_panel(a_ref, x_refs, stats, pc, pl0):
    lane = lax.broadcasted_iota(jnp.int32, (8, 128), 1)
    accs = [jnp.zeros((8, 128), F32) for _ in range(8)]
    for ch in range(N_CH):
        x = bcast(a_ref[ch, 0:1, :])
        if ch == pc:
            x = jnp.where(lane > pl0, x, 0.0)
        x_refs[0][ch] = x
        for g in range(8):
            accs[g] = accs[g] + a_ref[ch, g * 8 : g * 8 + 8, :] * x
    accs = tuple(accs)
    for gi in range(8):

        def pair(h, accs, gi=gi):
            for par in range(2):
                accs = qr_step(a_ref, x_refs[par], x_refs[1 - par], stats, pc, pl0, gi, h * 2 + par, par == 1, accs)
            return accs

        accs = lax.fori_loop(0, 4, pair, accs)[1:]


def finish_panel(a_ref, stats, vt_ref, rt_ref, pc, pl0):
    beta_ref, inv_ref, tau_ref = stats
    lane = lax.broadcasted_iota(jnp.int32, (8, 128), 1)
    sub = lax.broadcasted_iota(jnp.int32, (8, 128), 0)
    for g in range(8):
        rows = slice(g * 8, g * 8 + 8)
        inv = inv_ref[rows, :]
        for ch in range(N_CH):
            sl = slice(ch * 128, (ch + 1) * 128)
            a = a_ref[ch, rows, :]
            v = a * inv
            if ch == pc:
                rel = lane - pl0 - (g * 8 + sub)
                rt_ref[rows, :] = jnp.where(rel < 0, a, jnp.where(rel == 0, beta_ref[rows, :], 0.0))
                v = jnp.where(rel > 0, v, jnp.where(rel == 0, 1.0, 0.0))
            vt_ref[rows, sl] = v


def build_tri(gram_mat, tau_col):
    row = lax.broadcasted_iota(jnp.int32, (NB, NB), 0)
    col = lax.broadcasted_iota(jnp.int32, (NB, NB), 1)
    t = jnp.where(row == col, tau_col, 0.0)
    for lg in range(6):
        rb = lax.shift_right_logical(row, lg)
        cb = lax.shift_right_logical(col, lg)
        u = jnp.where((cb == rb + 1) & (lax.rem(rb, 2) == 0), gram_mat, 0.0)
        t = t - mm(mm(t, u), t)
    return t


def panel_kernel(step, *refs):
    refs = list(refs)
    n_rem = PANELS - step
    if step > 0:
        vt_ref, yt_ref, t_ref, tt_ref = refs[:4]
        refs = refs[4:]
    if n_rem:
        pt_ref = refs.pop(0)
    if step > 0:
        wt_ref = refs.pop(0)
    if n_rem:
        d_ref, r_ref, vn_ref, tn_ref, ttn_ref = refs[:5]
        refs = refs[5:]
        if n_rem > 1:
            rem_ref = refs.pop(0)
    if n_rem:
        a_ref, xa, xb, beta_ref, inv_ref, tau_ref = refs
    lane64 = lax.broadcasted_iota(jnp.int32, (NB, 128), 1)
    row64 = lax.broadcasted_iota(jnp.int32, (NB, 128), 0)
    if step > 0:
        for g in range(step):
            sl = slice(g * QTR, g * QTR + 128)
            yt_ref[:, sl] = jnp.where(lane64 < NB, 0.0, yt_ref[:, sl])
        s_mat = gram(vt_ref, yt_ref)
        m_mat = mm(mm(tt_ref[...], s_mat, 1), t_ref[...])
        lhs = jnp.concatenate([tt_ref[...], -0.5 * m_mat], axis=1)
        for t in range(N // 512):
            sl = slice(t * 512, (t + 1) * 512)
            wt_ref[:, sl] = mm(lhs, jnp.concatenate([yt_ref[:, sl], vt_ref[:, sl]], axis=0))
    if not n_rem:
        return
    if step > 0:
        pieces = []
        for q in range(step, PANELS):
            sl = slice(q * QTR, q * QTR + 128)
            wc = wt_ref[:, sl].T[:NB]
            vc = vt_ref[:, sl].T[:NB]
            pieces.append(jnp.concatenate([wc, vc], axis=1))
        lhs = jnp.concatenate(pieces, axis=0)
        for t in range(N // 256):
            sl = slice(t * 256, (t + 1) * 256)
            upd = mm(lhs, jnp.concatenate([vt_ref[:, sl], wt_ref[:, sl]], axis=0))
            for h in range(2):
                a_ref[2 * t + h] = pt_ref[0, :, t * 256 + h * 128 : t * 256 + (h + 1) * 128] - upd[:NB, h * 128 : (h + 1) * 128]
            for q in range(1, n_rem):
                rem_ref[q - 1, :, sl] = pt_ref[q, :, sl] - upd[q * NB : (q + 1) * NB]
    else:
        for ch in range(N_CH):
            sl = slice(ch * 128, (ch + 1) * 128)
            a_ref[ch] = pt_ref[0, :, sl]
        for q in range(1, n_rem):
            rem_ref[q - 1] = pt_ref[q]
    d_ref[...] = jnp.where((lane64 >= row64) & (lane64 < NB), a_ref[step * 8], 0.0)
    for g in range(step + 1):
        a_ref[g * 8] = jnp.where(lane64 < NB, 0.0, a_ref[g * 8])
    pc = ((step + 1) % 4) * (QTR // 128)
    pl0 = NB * ((step + 1) // 4)
    stats = (beta_ref, inv_ref, tau_ref)
    qr_panel(a_ref, (xa, xb), stats, pc, pl0)
    finish_panel(a_ref, stats, vn_ref, r_ref, pc, pl0)
    t_new = build_tri(gram(vn_ref, vn_ref), tau_ref[:, :NB])
    tn_ref[...] = t_new
    ttn_ref[...] = jnp.concatenate([t_new, jnp.zeros((NB, NB), F32)], axis=1).T[:NB]


def panel_call(step, *args):
    n_rem = PANELS - step
    outs = []
    full = jax.ShapeDtypeStruct((NB, N), F32)
    small = jax.ShapeDtypeStruct((NB, NB), F32)
    wide = jax.ShapeDtypeStruct((NB, 128), F32)
    scratch = []
    if step > 0:
        outs.append(full)
    if n_rem:
        outs += [wide, wide, full, small, small]
        if n_rem > 1:
            outs.append(jax.ShapeDtypeStruct((n_rem - 1, NB, N), F32))
        scratch = [pltpu.VMEM((N_CH, NB, 128), F32), pltpu.VMEM((N_CH, 8, 128), F32), pltpu.VMEM((N_CH, 8, 128), F32)] + [pltpu.VMEM((NB, 128), F32)] * 3
    vspec = pl.BlockSpec(memory_space=pltpu.VMEM)
    return pl.pallas_call(
        functools.partial(panel_kernel, step),
        out_shape=outs,
        in_specs=[vspec] * len(args),
        out_specs=[vspec] * len(outs),
        scratch_shapes=scratch,
        compiler_params=pltpu.CompilerParams(vmem_limit_bytes=VMEM_LIMIT),
        name=f"panel{step}",
    )(*args)


def tile_kernel(update, products, final, *refs):
    refs = list(refs)
    l_ref = refs.pop(0)
    if products:
        va, vb = refs[:2]
        refs = refs[2:]
    if update:
        ua, ub, wa, wb = refs[:4]
        refs = refs[4:]
        lo_ref = refs.pop(0)
    if products:
        p1_ref, p2_ref = refs[:2]
        refs = refs[2:]
        vc3, vr3, acc1, acc2 = refs[:4]
        refs = refs[4:]
    if update:
        left6, right6 = refs
    mat = pl.program_id(0)
    ti = pl.program_id(1)
    tj = pl.program_id(2)
    my_row = lax.axis_index('row')
    my_col = lax.axis_index('col')
    mine = lax.rem(my_row, 2) == mat
    lane = lax.broadcasted_iota(jnp.int32, (NB, 128), 1)
    low_half = lane < NB

    def pick(a_ref, b_ref, base, ch):
        sl = pl.ds(pl.multiple_of(base * QTR + ch * 128, 128), 128)
        return jnp.where(mine, a_ref[:, sl], b_ref[:, sl])

    def col_chunks(a_ref, b_ref, u):
        qa = pick(a_ref, b_ref, my_col, u)
        qb = pick(a_ref, b_ref, my_col + 2, u)
        even = jnp.where(low_half, qa, pltpu.roll(qb, NB, 1))
        odd = jnp.where(low_half, pltpu.roll(qa, NB, 1), qb)
        return even, odd

    @pl.when((ti == 0) & (tj == 0))
    def _():
        if products:
            acc2[...] = jnp.zeros_like(acc2)
            vc3[192:256, :] = jnp.zeros((64, 2048), BF16)
            for u in range(8):
                for h, part in enumerate(col_chunks(va, vb, u)):
                    sl = slice((2 * u + h) * 128, (2 * u + h + 1) * 128)
                    for q, piece in enumerate(split3(part)):
                        vc3[q * NB : (q + 1) * NB, sl] = piece
                for q, piece in enumerate(split3(pick(va, vb, my_row, u))):
                    vr3[q * NB : (q + 1) * NB, u * 128 : (u + 1) * 128] = piece
        if update:
            for u in range(8):
                vcs = col_chunks(ua, ub, u)
                wcs = col_chunks(wa, wb, u)
                for h in range(2):
                    sl = slice((2 * u + h) * 128, (2 * u + h + 1) * 128)
                    r1, r2, r3 = split3(jnp.concatenate([wcs[h], vcs[h]], axis=0))
                    for q, piece in enumerate((r3, r2, r1, r2, r1, r1)):
                        right6[q * 128 : (q + 1) * 128, sl] = piece
                left = jnp.concatenate([pick(ua, ub, my_row, u), pick(wa, wb, my_row, u)], axis=0).T
                a1, a2, a3 = split3(left)
                for q, piece in enumerate((a1, a2, a3, a1, a2, a1)):
                    left6[u * 128 : (u + 1) * 128, q * 128 : (q + 1) * 128] = piece

    def run(diag):
        tile = l_ref[0]
        col_sl = pl.ds(pl.multiple_of(tj * TC, TC), TC)
        row_sl = pl.ds(pl.multiple_of(ti * TR, TR), TR)
        if diag or final:
            ri = lax.broadcasted_iota(jnp.int32, (TR, TC), 0) + ti * TR
            ci = lax.broadcasted_iota(jnp.int32, (TR, TC), 1) + tj * TC
            rg = (lax.shift_right_logical(ri, 6) * 4 + my_row) * NB + (ri & 63)
            cg = (lax.shift_right_logical(ci, 6) * 2 + my_col) * NB + (ci & 63)
        if update:
            upd = bdot(left6[row_sl, :], right6[:, col_sl])
            tile = tile - (jnp.where(rg >= cg, upd, 0.0) if diag else upd)
            if final:
                done = PANELS * NB
                lo_ref[0] = jnp.where((rg >= done) & (cg >= done), tile, 0.0)
            else:
                lo_ref[0] = tile
        if products:
            parts = split3(tile)
            vcols = vc3[:, col_sl]
            vrows = vr3[:, row_sl]
            p2 = None
            p1 = None
            for part in (parts[2], parts[1], parts[0]):
                q2 = bdot(vrows, part)
                p2 = q2 if p2 is None else p2 + q2
                q1 = bdot(jnp.where(rg == cg, jnp.zeros((), BF16), part) if diag else part, vcols, 1, 1)
                p1 = q1 if p1 is None else p1 + q1
            acc2[:, col_sl] += p2

            @pl.when(tj == 0)
            def _():
                acc1[...] = p1

            @pl.when(tj > 0)
            def _():
                acc1[...] += p1

            if diag:
                tot = (acc1[:, :128] + acc1[:, 128:]).T
                p1_ref[0, :, row_sl] = tot[NB:] + tot[:NB]

    @pl.when(tj < ti)
    def _():
        run(False)

    @pl.when(tj == ti)
    def _():
        run(True)

    if update and not final and len(update) == 1:

        @pl.when(tj > ti)
        def _():
            lo_ref[0] = jnp.zeros_like(lo_ref[0])

    if products:

        @pl.when((ti == 3) & (tj == 3))
        def _():
            for u in range(8):
                ev = fold_rows(acc2[:, 2 * u * 128 : (2 * u + 1) * 128])
                od = fold_rows(acc2[:, (2 * u + 1) * 128 : (2 * u + 2) * 128])
                sl = slice(u * 128, (u + 1) * 128)
                p2_ref[0, 0, :, sl] = jnp.where(low_half, ev, pltpu.roll(od, NB, 1))
                p2_ref[0, 1, :, sl] = jnp.where(low_half, pltpu.roll(ev, NB, 1), od)


def tile_call(low, v_pair, prev, in_place=False, final=False):
    products = v_pair is not None
    update = prev is not None
    lower_map = lambda m, i, j: (m, i, jnp.minimum(i, j))
    full_map = lambda m, i, j: (m, i, j)
    vspec = pl.BlockSpec(memory_space=pltpu.VMEM)
    args = [low]
    in_specs = [pl.BlockSpec((1, TR, TC), lower_map)]
    outs, out_specs, scratch = [], [], []
    if products:
        args += list(v_pair)
        in_specs += [vspec] * 2
    if update:
        args += list(prev)
        in_specs += [vspec] * 4
        outs.append(jax.ShapeDtypeStruct(low.shape, F32))
        out_specs.append(pl.BlockSpec((1, TR, TC), lower_map if in_place else full_map))
    if products:
        outs += [jax.ShapeDtypeStruct((2, NB, QTR), F32), jax.ShapeDtypeStruct((2, 2, NB, QTR), F32)]
        out_specs += [pl.BlockSpec((1, NB, QTR), lambda m, i, j: (m, 0, 0)), pl.BlockSpec((1, 2, NB, QTR), lambda m, i, j: (m, 0, 0, 0))]
        scratch += [pltpu.VMEM((256, 2048), BF16), pltpu.VMEM((192, QTR), BF16), pltpu.VMEM((TR, 256), F32), pltpu.VMEM((192, 2048), F32)]
    if update:
        scratch += [pltpu.VMEM((QTR, 768), BF16), pltpu.VMEM((768, 2048), BF16)]
    mode = () if not update else ((1, 1) if in_place else (1,))
    return pl.pallas_call(
        functools.partial(tile_kernel, mode, products, final),
        out_shape=outs,
        grid=(2, 4, 4),
        in_specs=in_specs,
        out_specs=out_specs,
        scratch_shapes=scratch,
        input_output_aliases={0: 0} if in_place else {},
        compiler_params=pltpu.CompilerParams(vmem_limit_bytes=VMEM_LIMIT, dimension_semantics=("arbitrary",) * 3),
        name="tiles",
    )(*args)


def barrier(neighbours):
    sem = pltpu.get_barrier_semaphore()
    for dev in neighbours:
        pl.semaphore_signal(sem, inc=1, device_id=dev, device_id_type=MESH)
    pl.semaphore_wait(sem, len(neighbours))


def remote(src, dst, send, recv, dev):
    return pltpu.make_async_remote_copy(src_ref=src, dst_ref=dst, send_sem=send, recv_sem=recv, device_id=dev, device_id_type=MESH)


def place():
    my_row = lax.axis_index('row')
    my_col = lax.axis_index('col')
    return lax.div(my_row, 2), lax.rem(my_row, 2), my_col


def device(x, core, y):
    return {'row': 2 * x + core, 'col': y}


def gather_kernel(slab_ref, pt_ref, send, recv):
    x, core, y = place()
    others = [(dx, dy, f) for dx in range(2) for dy in range(2) for f in range(2) if (dx, dy, f) != (0, 0, 0)]

    def flip(v, d):
        return 1 - v if d else v

    barrier([device(flip(x, dx), flip(core, f), flip(y, dy)) for dx, dy, f in others])
    lanes = pl.ds(pl.multiple_of((2 * x + core) * QTR, QTR), QTR)
    copies = []
    for blk in range(2):
        for idx, (dx, dy, f) in enumerate(others):
            to_core = flip(core, f)
            cp = remote(slab_ref.at[to_core, blk], pt_ref.at[2 * blk + y, :, lanes], send.at[blk, idx], recv.at[blk, idx], device(flip(x, dx), to_core, flip(y, dy)))
            cp.start()
            copies.append(cp)
    for blk in range(2):
        pt_ref[2 * blk + y, :, lanes] = slab_ref[core, blk]
    for cp in copies:
        cp.wait()


def gather_call(slab):
    vspec = pl.BlockSpec(memory_space=pltpu.VMEM)
    return pl.pallas_call(
        gather_kernel,
        out_shape=jax.ShapeDtypeStruct((PANELS, NB, N), F32),
        in_specs=[vspec],
        out_specs=vspec,
        scratch_shapes=[pltpu.SemaphoreType.DMA((2, 7)), pltpu.SemaphoreType.DMA((2, 7))],
        compiler_params=pltpu.CompilerParams(collective_id=0, has_side_effects=True, vmem_limit_bytes=VMEM_LIMIT),
        name="gather",
    )(slab)


def sum_kernel(p1, p2, yt, r_part, r_own, r_p1, r_p2, sbuf, qbuf, send, recv):
    x, core, y = place()
    partner = device(x, 1 - core, y)
    x_nbr = device(1 - x, core, y)
    y_nbr = device(x, core, 1 - y)
    y_cross = device(x, 1 - core, 1 - y)
    barrier([partner, x_nbr, y_nbr, y_cross])
    other = 1 - core
    c_part = remote(p2.at[other], r_part, send.at[0], recv.at[0], partner)
    c_part.start()
    c_y = remote(p1.at[core], r_p1, send.at[1], recv.at[1], y_nbr)
    c_yx = remote(p1.at[other], r_p1, send.at[2], recv.at[1], y_cross)
    c_own = remote(p1.at[other], r_own, send.at[1], recv.at[2], partner)

    @pl.when(core != y)
    def _():
        c_y.start()
        c_yx.start()

    @pl.when(core == y)
    def _():
        c_own.start()

    c_part.wait()
    sbuf[...] = p2[core, 1 - x] + r_part[1 - x]
    c_x = remote(sbuf, r_p2, send.at[3], recv.at[3], x_nbr)
    c_x.start()
    qbuf[...] = p2[core, x] + r_part[x]

    @pl.when(core == y)
    def _():
        c_own.wait_send()
        qbuf[...] += p1[core]

    @pl.when(core != y)
    def _():
        c_own.wait_recv()
        qbuf[...] += r_own[...]
        c_y.wait_send()
        c_yx.wait_send()

    c_y.wait_recv()
    qbuf[...] += r_p1[...]
    c_x.wait()
    qbuf[...] += r_p2[...]

    def lanes(xx, yy, half=None):
        start = (2 * xx + yy) * QTR
        if half is None:
            return pl.ds(pl.multiple_of(start, QTR), QTR)
        return pl.ds(pl.multiple_of(start + half * (QTR // 2), QTR // 2), QTR // 2)

    g_x = remote(qbuf, yt.at[:, lanes(x, y)], send.at[4], recv.at[4], x_nbr)
    g_y = remote(qbuf, yt.at[:, lanes(x, y)], send.at[5], recv.at[5], y_nbr)
    g_x.start()
    g_y.start()
    yt[:, lanes(x, y)] = qbuf[...]
    part_y = yt.at[:, lanes(x, 1 - y, 0)]
    f_x = remote(part_y, part_y, send.at[6], recv.at[6], x_nbr)
    part_x = yt.at[:, lanes(1 - x, y, 1)]
    f_y = remote(part_x, part_x, send.at[7], recv.at[7], y_nbr)
    g_y.wait_recv()
    f_x.start()
    g_x.wait_recv()
    f_y.start()
    g_x.wait_send()
    g_y.wait_send()
    f_x.wait()
    f_y.wait()


def sum_call(p1, p2):
    vspec = pl.BlockSpec(memory_space=pltpu.VMEM)
    qtr = pltpu.VMEM((NB, QTR), F32)
    return pl.pallas_call(
        sum_kernel,
        out_shape=jax.ShapeDtypeStruct((NB, N), F32),
        in_specs=[vspec] * 2,
        out_specs=vspec,
        scratch_shapes=[pltpu.VMEM((2, NB, QTR), F32), qtr, qtr, qtr, qtr, qtr, pltpu.SemaphoreType.DMA((8,)), pltpu.SemaphoreType.DMA((8,))],
        compiler_params=pltpu.CompilerParams(collective_id=1, has_side_effects=True, vmem_limit_bytes=VMEM_LIMIT),
        name="sums",
    )(p1, p2)


def swap_kernel(n, *refs):
    x, core, y = place()
    partner = device(x, 1 - core, y)
    barrier([partner])
    send, recv = refs[2 * n :]
    copies = [remote(refs[i], refs[n + i], send.at[i], recv.at[i], partner) for i in range(n)]
    for cp in copies:
        cp.start()
    for cp in copies:
        cp.wait()


def swap_call(ident, *arrays):
    n = len(arrays)
    vspec = pl.BlockSpec(memory_space=pltpu.VMEM)
    return pl.pallas_call(
        functools.partial(swap_kernel, n),
        out_shape=[jax.ShapeDtypeStruct(a.shape, F32) for a in arrays],
        in_specs=[vspec] * n,
        out_specs=[vspec] * n,
        scratch_shapes=[pltpu.SemaphoreType.DMA((n,)), pltpu.SemaphoreType.DMA((n,))],
        compiler_params=pltpu.CompilerParams(collective_id=ident, has_side_effects=True, vmem_limit_bytes=VMEM_LIMIT),
        name="swap",
    )(*arrays)


def solution(mesh):
    def per_device(lower_tri):
        n_mat, n_rblk, blk, n_cloc = lower_tri.shape
        n_rloc = n_rblk * blk
        my_row = lax.axis_index('row')
        core = lax.rem(my_row, 2)
        low = lower_tri.reshape(n_mat, n_rloc, n_cloc)
        slab = jnp.swapaxes(low[:, :, : 2 * NB], 1, 2).reshape(n_mat, 2, NB, n_rloc)
        pts = gather_call(slab)
        d_list, r_list, t_list, v_list = [], [], [], []
        prev = None
        wt = None
        for k in range(PANELS):
            if k == 0:
                d, r, vt, t, tt, pts = panel_call(0, pts)
                v_other, = swap_call(2, vt)
            else:
                out = panel_call(k, vt, yt, t, tt, pts)
                wt, d, r, vt_new, t, tt = out[:6]
                pts = out[6] if k < PANELS - 1 else None
                w_other, v_new_other = swap_call(3, wt, vt_new)
                prev = (vt, v_other, wt, w_other)
                vt, v_other = vt_new, v_new_other
            if k == 0:
                p1, p2 = tile_call(low, (vt, v_other), None)
            else:
                low, p1, p2 = tile_call(low, (vt, v_other), prev, in_place=k > 1)
            yt = sum_call(p1, p2)
            off = NB * ((k + 1) // 4)
            d_list.append(d[:, :NB].T)
            r_list.append(r[:, off : off + NB].T)
            t_list.append(t)
            pair = jnp.where(core == 0, jnp.stack([vt, v_other]), jnp.stack([v_other, vt]))
            mine = lax.dynamic_slice_in_dim(pair, my_row * QTR, QTR, axis=2)
            v_list.append(jnp.swapaxes(mine, 1, 2).reshape(n_mat, n_rblk, blk, blk))
        wt, = panel_call(PANELS, vt, yt, t, tt)
        packed = jnp.stack([jnp.stack(d_list), jnp.stack(r_list), jnp.stack(t_list)])
        packed = jnp.pad(packed.reshape(3 * PANELS * NB, NB), ((0, 0), (0, 128 - NB)))
        w_other, packed_other = swap_call(4, wt, packed)
        low, = tile_call(low, None, (vt, v_other, wt, w_other), in_place=True, final=True)
        both = jnp.where(core == 0, jnp.stack([packed, packed_other]), jnp.stack([packed_other, packed]))
        both = both[:, :, :NB].reshape(n_mat, 3, PANELS, NB, NB)
        band = jnp.stack([both[:, 0], both[:, 1]], axis=2)
        return low.reshape(lower_tri.shape), band, jnp.stack(v_list, axis=1), both[:, 2]

    spec_low = P('sys', 'row', None, 'col')
    return jax.shard_map(per_device, mesh=mesh, in_specs=(spec_low,), out_specs=(spec_low, P('sys'), P('sys', None, 'row', None, None), P('sys')), check_vma=False)
```

```python
import functools

import jax
import jax.numpy as jnp
from jax import lax
from jax.experimental import pallas as pl
from jax.experimental.pallas import tpu as pltpu
from jax.sharding import PartitionSpec as P

PANELS = 4
NB = 64
N = 4096
QTR = 1024
N_CH = N // 128
TR, TC = 256, 512
F32 = jnp.float32
BF16 = jnp.bfloat16
MESH = pl.DeviceIdType.MESH
VMEM_LIMIT = 60 * 1024 * 1024


def split3(a):
    hi = a.astype(BF16)
    rest = a - hi.astype(F32)
    mid = rest.astype(BF16)
    low = (rest - mid.astype(F32)).astype(BF16)
    return hi, mid, low


def bdot(a, b, ca=1, cb=0):
    return lax.dot_general(a, b, (((ca,), (cb,)), ((), ())), preferred_element_type=F32)


def fold_rows(x):
    n = x.shape[0] // 3
    return x[2 * n :] + x[n : 2 * n] + x[:n]


def mm(a, b, cb=0):
    lhs = jnp.concatenate(split3(a), axis=0)
    b1, b2, b3 = split3(b)
    return fold_rows(bdot(lhs, b3, 1, cb) + bdot(lhs, b2, 1, cb) + bdot(lhs, b1, 1, cb))


def gram(a_ref, b_ref, mask=None):
    acc = None
    for t in range(N // 512):
        sl = slice(t * 512, (t + 1) * 512)
        lhs = jnp.concatenate(split3(a_ref[:, sl]), axis=0)
        rhs = jnp.concatenate(split3(b_ref[:, sl]), axis=0)
        part = bdot(lhs, rhs, 1, 1)
        acc = part if acc is None else acc + part
    acc = fold_rows(acc)
    return acc[:, 128:192] + acc[:, 64:128] + acc[:, 0:64]


def bcast(v):
    return jnp.broadcast_to(v, (8, 128))


def qr_step(a_ref, xcur, xnext, stats, pc, pl0, gi, s, last_of_pair, accs):
    beta_ref, inv_ref, tau_ref = stats
    lane = lax.broadcasted_iota(jnp.int32, (8, 128), 1)
    sub = lax.broadcasted_iota(jnp.int32, (8, 1), 0)
    n_g = 8 - gi
    j = gi * 8 + s
    p = pl0 + j
    rows = [slice((gi + g) * 8, (gi + g + 1) * 8) for g in range(n_g)]
    dots = [jnp.sum(acc, axis=1, keepdims=True) for acc in accs]
    pvs = [jnp.sum(jnp.where(lane == p, a_ref[pc, r, :], 0.0), axis=1, keepdims=True) for r in rows]
    sigma = jnp.sum(jnp.where(sub == s, dots[0], 0.0), axis=0, keepdims=True)
    alpha = jnp.sum(jnp.where(sub == s, pvs[0], 0.0), axis=0, keepdims=True)
    sq = alpha * alpha + sigma
    inv_norm = lax.rsqrt(sq)
    norm = jnp.sqrt(sq)
    pos = alpha >= 0
    beta = jnp.where(pos, -norm, norm)
    ninvb = jnp.where(pos, inv_norm, -inv_norm)
    denom = alpha - beta
    inv_den = 1.0 / denom
    tau = denom * ninvb
    cs = [(pv + d * inv_den) * ninvb for pv, d in zip(pvs, dots)]
    cs[0] = jnp.where(sub > s, cs[0], 0.0)
    beta_ref[pl.ds(j, 1), :] = jnp.broadcast_to(beta, (1, 128))
    inv_ref[pl.ds(j, 1), :] = jnp.broadcast_to(inv_den, (1, 128))
    tau_ref[pl.ds(j, 1), :] = jnp.broadcast_to(tau, (1, 128))
    c_next = jnp.sum(jnp.where(sub == s + 1, cs[0], 0.0), axis=0, keepdims=True)
    if last_of_pair and n_g > 1:
        c_next = c_next + jnp.where(s == 7, cs[1][0:1], 0.0)
    jn = jnp.minimum(j + 1, NB - 1)
    c_next = bcast(c_next)
    den_b = bcast(denom)
    for ch in range(N_CH):
        xt = xcur[ch]
        if ch == pc:
            xt = jnp.where(lane == p, den_b, xt)
        xn = a_ref[ch, pl.ds(jn, 8, stride=0), :] - c_next * xt
        if ch == pc:
            xn = jnp.where(lane > p + 1, xn, 0.0)
        xnext[ch] = xn
    cs = [bcast(c) for c in cs]
    out = [jnp.zeros((8, 128), F32) for _ in range(n_g)]
    for ch in range(N_CH):
        xt = xcur[ch]
        if ch == pc:
            xt = jnp.where(lane == p, den_b, xt)
        xn = xnext[ch]
        for g in range(n_g):
            a = a_ref[ch, rows[g], :] - cs[g] * xt
            a_ref[ch, rows[g], :] = a
            out[g] = out[g] + a * xn
    return tuple(out)


def qr_panel(a_ref, x_refs, stats, pc, pl0):
    lane = lax.broadcasted_iota(jnp.int32, (8, 128), 1)
    accs = [jnp.zeros((8, 128), F32) for _ in range(8)]
    for ch in range(N_CH):
        x = bcast(a_ref[ch, 0:1, :])
        if ch == pc:
            x = jnp.where(lane > pl0, x, 0.0)
        x_refs[0][ch] = x
        for g in range(8):
            accs[g] = accs[g] + a_ref[ch, g * 8 : g * 8 + 8, :] * x
    accs = tuple(accs)
    for gi in range(8):

        def pair(h, accs, gi=gi):
            for par in range(2):
                accs = qr_step(a_ref, x_refs[par], x_refs[1 - par], stats, pc, pl0, gi, h * 2 + par, par == 1, accs)
            return accs

        accs = lax.fori_loop(0, 4, pair, accs)[1:]


def finish_panel(a_ref, stats, vt_ref, rt_ref, pc, pl0):
    beta_ref, inv_ref, tau_ref = stats
    lane = lax.broadcasted_iota(jnp.int32, (8, 128), 1)
    sub = lax.broadcasted_iota(jnp.int32, (8, 128), 0)
    for g in range(8):
        rows = slice(g * 8, g * 8 + 8)
        inv = inv_ref[rows, :]
        for ch in range(N_CH):
            sl = slice(ch * 128, (ch + 1) * 128)
            a = a_ref[ch, rows, :]
            v = a * inv
            if ch == pc:
                rel = lane - pl0 - (g * 8 + sub)
                rt_ref[rows, :] = jnp.where(rel < 0, a, jnp.where(rel == 0, beta_ref[rows, :], 0.0))
                v = jnp.where(rel > 0, v, jnp.where(rel == 0, 1.0, 0.0))
            vt_ref[rows, sl] = v


def build_tri(gram_mat, tau_col):
    row = lax.broadcasted_iota(jnp.int32, (NB, NB), 0)
    col = lax.broadcasted_iota(jnp.int32, (NB, NB), 1)
    t = jnp.where(row == col, tau_col, 0.0)
    for lg in range(6):
        rb = lax.shift_right_logical(row, lg)
        cb = lax.shift_right_logical(col, lg)
        u = jnp.where((cb == rb + 1) & (lax.rem(rb, 2) == 0), gram_mat, 0.0)
        t = t - mm(mm(t, u), t)
    return t


def panel_kernel(step, *refs):
    refs = list(refs)
    n_rem = PANELS - step
    if step > 0:
        vt_ref, yt_ref, t_ref, tt_ref = refs[:4]
        refs = refs[4:]
    if step == 1:
        pieces0, refs = refs[:8], refs[8:]
        pieces1, refs = refs[:8], refs[8:]
    elif n_rem:
        pt_ref = refs.pop(0)
    if step > 0:
        wt_ref = refs.pop(0)
    if n_rem:
        small_ref, vn_ref, tn_ref, ttn_ref = refs[:4]
        refs = refs[4:]
        if step > 0 and n_rem > 1:
            rem_ref = refs.pop(0)
        a_ref, xa, xb, beta_ref, inv_ref, tau_ref = refs
    lane64 = lax.broadcasted_iota(jnp.int32, (NB, 128), 1)
    row64 = lax.broadcasted_iota(jnp.int32, (NB, 128), 0)
    if step > 0:
        for g in range(step):
            sl = slice(g * QTR, g * QTR + 128)
            yt_ref[:, sl] = jnp.where(lane64 < NB, 0.0, yt_ref[:, sl])
        s_mat = gram(vt_ref, yt_ref)
        m_mat = mm(mm(tt_ref[...], s_mat, 1), t_ref[...])
        lhs = jnp.concatenate([tt_ref[...], -0.5 * m_mat], axis=1)
        for t in range(N // 512):
            sl = slice(t * 512, (t + 1) * 512)
            wt_ref[:, sl] = mm(lhs, jnp.concatenate([yt_ref[:, sl], vt_ref[:, sl]], axis=0))
    if not n_rem:
        return
    if step == 1:
        x, core, y = place()
        for dx in range(2):
            for f in range(2):
                row = 2 * (1 - x if dx else x) + (1 - core if f else core)
                lanes = pl.ds(pl.multiple_of(row * QTR, QTR), QTR)
                here, there = 2 * dx + f, 4 + 2 * dx + f
                first = jnp.where(y == 1, pieces0[here][...], pieces0[there][...])
                for ch in range(8):
                    a_ref[row * 8 + ch] = first[:, ch * 128 : (ch + 1) * 128]
                one, two = pieces1[here][...], pieces1[there][...]
                rem_ref[0, :, lanes] = jnp.where(y == 0, one, two)
                rem_ref[1, :, lanes] = jnp.where(y == 1, one, two)
    if step > 0:
        lefts = []
        for q in range(step, PANELS):
            sl = slice(q * QTR, q * QTR + 128)
            wc = wt_ref[:, sl].T[:NB]
            vc = vt_ref[:, sl].T[:NB]
            lefts.append(jnp.concatenate([wc, vc], axis=1))
        lhs = jnp.concatenate(lefts, axis=0)
        for t in range(N // 256):
            sl = slice(t * 256, (t + 1) * 256)
            upd = mm(lhs, jnp.concatenate([vt_ref[:, sl], wt_ref[:, sl]], axis=0))
            for h in range(2):
                old = a_ref[2 * t + h] if step == 1 else pt_ref[0, :, t * 256 + h * 128 : t * 256 + (h + 1) * 128]
                a_ref[2 * t + h] = old - upd[:NB, h * 128 : (h + 1) * 128]
            for q in range(1, n_rem):
                old = rem_ref[q - 1, :, sl] if step == 1 else pt_ref[q, :, sl]
                rem_ref[q - 1, :, sl] = old - upd[q * NB : (q + 1) * NB]
    else:
        for ch in range(N_CH):
            a_ref[ch] = pt_ref[:, ch * 128 : (ch + 1) * 128]
    small_ref[0] = jnp.where((lane64 >= row64) & (lane64 < NB), a_ref[step * 8], 0.0)
    for g in range(step + 1):
        a_ref[g * 8] = jnp.where(lane64 < NB, 0.0, a_ref[g * 8])
    pc = ((step + 1) % 4) * (QTR // 128)
    pl0 = NB * ((step + 1) // 4)
    stats = (beta_ref, inv_ref, tau_ref)
    qr_panel(a_ref, (xa, xb), stats, pc, pl0)
    finish_panel(a_ref, stats, vn_ref, small_ref.at[1], pc, pl0)
    t_new = build_tri(gram(vn_ref, vn_ref), tau_ref[:, :NB])
    tn_ref[...] = t_new
    t_wide = jnp.concatenate([t_new, jnp.zeros((NB, NB), F32)], axis=1)
    small_ref[2] = t_wide
    ttn_ref[...] = t_wide.T[:NB]


def panel_call(step, *args):
    n_rem = PANELS - step
    outs = []
    full = jax.ShapeDtypeStruct((NB, N), F32)
    small = jax.ShapeDtypeStruct((NB, NB), F32)
    scratch = []
    if step > 0:
        outs.append(full)
    if n_rem:
        outs += [jax.ShapeDtypeStruct((3, NB, 128), F32), full, small, small]
        if step > 0 and n_rem > 1:
            outs.append(jax.ShapeDtypeStruct((n_rem - 1, NB, N), F32))
        scratch = [pltpu.VMEM((N_CH, NB, 128), F32), pltpu.VMEM((N_CH, 8, 128), F32), pltpu.VMEM((N_CH, 8, 128), F32)] + [pltpu.VMEM((NB, 128), F32)] * 3
    vspec = pl.BlockSpec(memory_space=pltpu.VMEM)
    return pl.pallas_call(
        functools.partial(panel_kernel, step),
        out_shape=outs,
        in_specs=[vspec] * len(args),
        out_specs=[vspec] * len(outs),
        scratch_shapes=scratch,
        compiler_params=pltpu.CompilerParams(vmem_limit_bytes=VMEM_LIMIT),
        cost_estimate=pl.CostEstimate(flops=20_000_000_000, bytes_accessed=8_000_000, transcendentals=0),
        name=f"panel{step}",
    )(*args)


def tile_kernel(update, products, final, *refs):
    refs = list(refs)
    l_ref = refs.pop(0)
    if products:
        va, vb = refs[:2]
        refs = refs[2:]
    if update:
        ua, ub, wa, wb = refs[:4]
        refs = refs[4:]
    if products and update:
        refs.pop(0)
    if update:
        lo_ref = refs.pop(0)
    if products:
        p1_ref, p2_ref, vo_ref = refs[:3]
        refs = refs[3:]
        vc3, vr3, acc1, acc2 = refs[:4]
        refs = refs[4:]
    if update:
        left6, right6 = refs
    mat = pl.program_id(0)
    ti = pl.program_id(1)
    my_row = lax.axis_index('row')
    my_col = lax.axis_index('col')
    mine = lax.rem(my_row, 2) == mat
    lane = lax.broadcasted_iota(jnp.int32, (NB, 128), 1)
    low_half = lane < NB

    def pick(a_ref, b_ref, base, ch):
        sl = pl.ds(pl.multiple_of(base * QTR + ch * 128, 128), 128)
        return jnp.where(mine, a_ref[:, sl], b_ref[:, sl])

    def col_chunks(a_ref, b_ref, u):
        qa = pick(a_ref, b_ref, my_col, u)
        qb = pick(a_ref, b_ref, my_col + 2, u)
        even = jnp.where(low_half, qa, pltpu.roll(qb, NB, 1))
        odd = jnp.where(low_half, pltpu.roll(qa, NB, 1), qb)
        return even, odd

    @pl.when(ti == 0)
    def _():
        if products:
            acc2[...] = jnp.zeros_like(acc2)
            vc3[192:256, :] = jnp.zeros((64, 2048), BF16)
            for u in range(8):
                for h, part in enumerate(col_chunks(va, vb, u)):
                    sl = slice((2 * u + h) * 128, (2 * u + h + 1) * 128)
                    for q, piece in enumerate(split3(part)):
                        vc3[q * NB : (q + 1) * NB, sl] = piece
                mine_rows = pick(va, vb, my_row, u)
                for q, piece in enumerate(split3(mine_rows)):
                    vr3[q * NB : (q + 1) * NB, u * 128 : (u + 1) * 128] = piece
                vo_ref[0, 0, u * 128 : (u + 1) * 128, :] = mine_rows.T
        if update:
            for u in range(8):
                vcs = col_chunks(ua, ub, u)
                wcs = col_chunks(wa, wb, u)
                for h in range(2):
                    sl = slice((2 * u + h) * 128, (2 * u + h + 1) * 128)
                    r1, r2, r3 = split3(jnp.concatenate([wcs[h], vcs[h]], axis=0))
                    for q, piece in enumerate((r3, r2, r1, r2, r1, r1)):
                        right6[q * 128 : (q + 1) * 128, sl] = piece
                left = jnp.concatenate([pick(ua, ub, my_row, u), pick(wa, wb, my_row, u)], axis=0).T
                a1, a2, a3 = split3(left)
                for q, piece in enumerate((a1, a2, a3, a1, a2, a1)):
                    left6[u * 128 : (u + 1) * 128, q * 128 : (q + 1) * 128] = piece

    row_sl = pl.ds(pl.multiple_of(ti * TR, TR), TR)

    def run(tj, diag):
        col_sl = pl.ds(pl.multiple_of(tj * TC, TC), TC)
        tile = l_ref[0, :, col_sl]
        if diag or final:
            ri = lax.broadcasted_iota(jnp.int32, (TR, TC), 0) + ti * TR
            ci = lax.broadcasted_iota(jnp.int32, (TR, TC), 1) + tj * TC
            rg = (lax.shift_right_logical(ri, 6) * 4 + my_row) * NB + (ri & 63)
            cg = (lax.shift_right_logical(ci, 6) * 2 + my_col) * NB + (ci & 63)
        if update:
            upd = bdot(left6[row_sl, :], right6[:, col_sl])
            tile = tile - (jnp.where(rg >= cg, upd, 0.0) if diag else upd)
            if final:
                done = PANELS * NB
                lo_ref[0, :, col_sl] = jnp.where((rg >= done) & (cg >= done), tile, 0.0)
            else:
                lo_ref[0, :, col_sl] = tile
        if products:
            parts = split3(tile)
            vcols = vc3[:, col_sl]
            vrows = vr3[:, row_sl]
            p2 = None
            p1 = None
            for part in (parts[2], parts[1], parts[0]):
                q2 = bdot(vrows, part)
                p2 = q2 if p2 is None else p2 + q2
                q1 = bdot(jnp.where(rg == cg, jnp.zeros((), BF16), part) if diag else part, vcols, 1, 1)
                p1 = q1 if p1 is None else p1 + q1
            acc2[:, col_sl] += p2
            if diag:
                tot = acc1[...] + p1
                tot = (tot[:, :128] + tot[:, 128:]).T
                p1_ref[0, :, row_sl] = tot[NB:] + tot[:NB]
            else:
                acc1[...] += p1

    if products:
        acc1[...] = jnp.zeros_like(acc1)

    @pl.loop(0, ti)
    def _(tj):
        run(tj, False)

    run(ti, True)

    if update:

        @pl.loop(ti + 1, 4)
        def _(tj):
            lo_ref[0, :, pl.ds(pl.multiple_of(tj * TC, TC), TC)] = jnp.zeros((TR, TC), F32)

    if products:

        @pl.when(ti == 3)
        def _():
            for u in range(8):
                ev = fold_rows(acc2[:, 2 * u * 128 : (2 * u + 1) * 128])
                od = fold_rows(acc2[:, (2 * u + 1) * 128 : (2 * u + 2) * 128])
                sl = slice(u * 128, (u + 1) * 128)
                p2_ref[0, 0, :, sl] = jnp.where(low_half, ev, pltpu.roll(od, NB, 1))
                p2_ref[0, 1, :, sl] = jnp.where(low_half, pltpu.roll(ev, NB, 1), od)


def tile_call(k, low, v_pair, prev, v_out):
    products = v_pair is not None
    update = prev is not None
    strip = pl.BlockSpec((1, TR, 2048), lambda m, i: (m, i, 0))
    vspec = pl.BlockSpec(memory_space=pltpu.VMEM)
    args = [low]
    in_specs = [strip]
    outs, out_specs, scratch, alias = [], [], [], {}
    if products:
        args += list(v_pair)
        in_specs += [vspec] * 2
    if update:
        args += list(prev)
        in_specs += [vspec] * 4
        outs.append(jax.ShapeDtypeStruct(low.shape, F32))
        out_specs.append(strip)
    if products:
        if update:
            alias = {len(args): len(outs) + 2}
            args.append(v_out)
            in_specs.append(pl.BlockSpec(memory_space=pl.ANY))
        outs += [jax.ShapeDtypeStruct((2, NB, QTR), F32), jax.ShapeDtypeStruct((2, 2, NB, QTR), F32), jax.ShapeDtypeStruct((2, PANELS, QTR, NB), F32)]
        out_specs += [pl.BlockSpec((1, NB, QTR), lambda m, i: (m, 0, 0)), pl.BlockSpec((1, 2, NB, QTR), lambda m, i: (m, 0, 0, 0)), pl.BlockSpec((1, 1, QTR, NB), lambda m, i: (m, k, 0, 0))]
        scratch += [pltpu.VMEM((256, 2048), BF16), pltpu.VMEM((192, QTR), BF16), pltpu.VMEM((TR, 256), F32), pltpu.VMEM((192, 2048), F32)]
    if update:
        scratch += [pltpu.VMEM((QTR, 768), BF16), pltpu.VMEM((768, 2048), BF16)]
    return pl.pallas_call(
        functools.partial(tile_kernel, update, products, not products),
        out_shape=outs,
        grid=(2, 4),
        in_specs=in_specs,
        out_specs=out_specs,
        scratch_shapes=scratch,
        input_output_aliases=alias,
        compiler_params=pltpu.CompilerParams(vmem_limit_bytes=VMEM_LIMIT, dimension_semantics=("arbitrary",) * 2),
        cost_estimate=pl.CostEstimate(flops=15_000_000_000, bytes_accessed=32_000_000, transcendentals=0),
        name="tiles",
    )(*args)


def barrier(neighbours):
    sem = pltpu.get_barrier_semaphore()
    for dev in neighbours:
        pl.semaphore_signal(sem, inc=1, device_id=dev, device_id_type=MESH)
    pl.semaphore_wait(sem, len(neighbours))


def remote(src, dst, send, recv, dev):
    return pltpu.make_async_remote_copy(src_ref=src, dst_ref=dst, send_sem=send, recv_sem=recv, device_id=dev, device_id_type=MESH)


def place():
    my_row = lax.axis_index('row')
    my_col = lax.axis_index('col')
    return lax.div(my_row, 2), lax.rem(my_row, 2), my_col


def device(x, core, y):
    return {'row': 2 * x + core, 'col': y}


def gather_kernel(slab_ref, pt_ref, send, recv, fwd_send, fwd_recv):
    x, core, y = place()
    other = 1 - core
    barrier([device(x, other, y), device(1 - x, core, y), device(1 - x, other, y), device(x, core, 1 - y), device(x, other, 1 - y)])
    n_part = 4
    width = QTR // n_part

    def lanes(row, part=None):
        if part is None:
            return pl.ds(pl.multiple_of(row * QTR, QTR), QTR)
        return pl.ds(pl.multiple_of(row * QTR + part * width, width), width)

    def push(to_core, dev, part, s_sem, r_sem):
        return remote(slab_ref.at[to_core, :, part * width : (part + 1) * width], pt_ref.at[:, lanes(2 * x + core, part)], s_sem, r_sem, dev)

    def onward(row, part, idx):
        ref = pt_ref.at[:, lanes(row, part)]
        return remote(ref, ref, fwd_send.at[idx, part], fwd_recv.at[idx, part], device(1 - x, core, y))

    my_row = 2 * x + core
    for part in range(n_part):
        to_y = [push(core, device(x, core, 1 - y), part, send.at[0, part], recv.at[0, part]), push(other, device(x, other, 1 - y), part, send.at[1, part], recv.at[1, part])]
        to_x = [push(core, device(1 - x, core, y), part, send.at[2, part], recv.at[2, part]), push(other, device(1 - x, other, y), part, send.at[3, part], recv.at[3, part])]
        to_p = push(other, device(x, other, y), part, send.at[4, part], recv.at[4, part])

        @pl.when(y == 0)
        def _():
            for cp in to_y + to_x + [to_p]:
                cp.start()

    @pl.when(y == 0)
    def _():
        pt_ref[:, lanes(my_row)] = slab_ref[core]
        for part in range(n_part):
            for idx, (tc, dev) in enumerate([(core, device(x, core, 1)), (other, device(x, other, 1)), (core, device(1 - x, core, 0)), (other, device(1 - x, other, 0)), (other, device(x, other, 0))]):
                cp = push(tc, dev, part, send.at[idx, part], recv.at[idx, part])
                cp.wait_send()
                if idx >= 2:
                    cp.wait_recv()

    @pl.when(y == 1)
    def _():
        for part in range(n_part):
            for idx, row in enumerate([my_row, 2 * x + other]):
                push(core, device(x, core, 0), part, send.at[idx, part], recv.at[idx, part]).wait_recv()
                onward(row, part, idx).start()
        for part in range(n_part):
            for idx in range(2):
                onward(my_row, part, idx).wait()


def gather_call(slab):
    vspec = pl.BlockSpec(memory_space=pltpu.VMEM)
    return pl.pallas_call(
        gather_kernel,
        out_shape=jax.ShapeDtypeStruct((NB, N), F32),
        in_specs=[vspec],
        out_specs=vspec,
        scratch_shapes=[pltpu.SemaphoreType.DMA((5, 4)), pltpu.SemaphoreType.DMA((5, 4)), pltpu.SemaphoreType.DMA((2, 4)), pltpu.SemaphoreType.DMA((2, 4))],
        compiler_params=pltpu.CompilerParams(collective_id=0, has_side_effects=True, vmem_limit_bytes=VMEM_LIMIT),
        name="gather",
    )(slab)


def rest_of_panels(slab, my_row, pt):
    core = lax.rem(my_row, 2)
    own = lax.dynamic_index_in_dim(slab, core, 0, keepdims=False)
    cross = lax.dynamic_index_in_dim(slab, 1 - core, 0, keepdims=False)
    own, cross, pt = lax.optimization_barrier((own, cross, pt))

    def pairs(dx, dy, f, cols):
        out = []
        for col in cols:
            for x in range(2):
                for c in range(2):
                    out.append((col * 4 + 2 * x + c, (col ^ dy) * 4 + 2 * (x ^ dx) + (c ^ f)))
        return out

    result = []
    for blk, cols in ((0, (1,)), (1, (0, 1))):
        pieces = []
        for dy in range(2):
            for dx in range(2):
                for f in range(2):
                    payload = (cross if f else own)[blk]
                    pieces.append(payload if (dx, dy, f) == (0, 0, 0) else lax.ppermute(payload, ('col', 'row'), pairs(dx, dy, f, cols)))
        result += pieces
    return result, pt


def sum_kernel(p1, p2, yt, r_part, r_own, r_p1, r_p2, sbuf, qbuf, send, recv):
    x, core, y = place()
    partner = device(x, 1 - core, y)
    x_nbr = device(1 - x, core, y)
    y_nbr = device(x, core, 1 - y)
    y_cross = device(x, 1 - core, 1 - y)
    barrier([partner, x_nbr, y_nbr, y_cross])
    other = 1 - core
    c_part = remote(p2.at[other], r_part, send.at[0], recv.at[0], partner)
    c_part.start()
    c_y = remote(p1.at[core], r_p1, send.at[1], recv.at[1], y_nbr)
    c_yx = remote(p1.at[other], r_p1, send.at[2], recv.at[1], y_cross)
    c_own = remote(p1.at[other], r_own, send.at[1], recv.at[2], partner)

    @pl.when(core != y)
    def _():
        c_y.start()
        c_yx.start()

    @pl.when(core == y)
    def _():
        c_own.start()

    c_part.wait()
    sbuf[...] = p2[core, 1 - x] + r_part[1 - x]
    c_x = remote(sbuf, r_p2, send.at[3], recv.at[3], x_nbr)
    c_x.start()
    qbuf[...] = p2[core, x] + r_part[x]

    @pl.when(core == y)
    def _():
        c_own.wait_send()
        qbuf[...] += p1[core]

    @pl.when(core != y)
    def _():
        c_own.wait_recv()
        qbuf[...] += r_own[...]
        c_y.wait_send()
        c_yx.wait_send()

    c_y.wait_recv()
    qbuf[...] += r_p1[...]
    c_x.wait()
    qbuf[...] += r_p2[...]

    def lanes(xx, yy, half=None):
        start = (2 * xx + yy) * QTR
        if half is None:
            return pl.ds(pl.multiple_of(start, QTR), QTR)
        return pl.ds(pl.multiple_of(start + half * (QTR // 2), QTR // 2), QTR // 2)

    g_x = remote(qbuf, yt.at[:, lanes(x, y)], send.at[4], recv.at[4], x_nbr)
    g_y = remote(qbuf, yt.at[:, lanes(x, y)], send.at[5], recv.at[5], y_nbr)
    g_x.start()
    g_y.start()
    yt[:, lanes(x, y)] = qbuf[...]
    part_y = yt.at[:, lanes(x, 1 - y, 0)]
    f_x = remote(part_y, part_y, send.at[6], recv.at[6], x_nbr)
    part_x = yt.at[:, lanes(1 - x, y, 1)]
    f_y = remote(part_x, part_x, send.at[7], recv.at[7], y_nbr)
    g_y.wait_recv()
    f_x.start()
    g_x.wait_recv()
    f_y.start()
    g_x.wait_send()
    g_y.wait_send()
    f_x.wait()
    f_y.wait()


def sum_call(p1, p2):
    vspec = pl.BlockSpec(memory_space=pltpu.VMEM)
    qtr = pltpu.VMEM((NB, QTR), F32)
    return pl.pallas_call(
        sum_kernel,
        out_shape=jax.ShapeDtypeStruct((NB, N), F32),
        in_specs=[vspec] * 2,
        out_specs=vspec,
        scratch_shapes=[pltpu.VMEM((2, NB, QTR), F32), qtr, qtr, qtr, qtr, qtr, pltpu.SemaphoreType.DMA((8,)), pltpu.SemaphoreType.DMA((8,))],
        compiler_params=pltpu.CompilerParams(collective_id=1, has_side_effects=True, vmem_limit_bytes=VMEM_LIMIT),
        name="sums",
    )(p1, p2)


def swap_kernel(n, *refs):
    x, core, y = place()
    partner = device(x, 1 - core, y)
    barrier([partner])
    send, recv = refs[2 * n :]
    copies = []
    for i in range(n):
        src, dst = refs[i], refs[n + i]
        if src.shape[-1] == N:
            for q, row in enumerate((y, 2 + y, 2 * x + 1 - y)):
                lanes = pl.ds(pl.multiple_of(row * QTR, QTR), QTR)
                copies.append(remote(src.at[:, lanes], dst.at[:, lanes], send.at[i, q], recv.at[i, q], partner))
        else:
            copies.append(remote(src, dst, send.at[i, 0], recv.at[i, 0], partner))
    for cp in copies:
        cp.start()
    for cp in copies:
        cp.wait()


def swap_call(ident, *arrays):
    n = len(arrays)
    vspec = pl.BlockSpec(memory_space=pltpu.VMEM)
    return pl.pallas_call(
        functools.partial(swap_kernel, n),
        out_shape=[jax.ShapeDtypeStruct(a.shape, F32) for a in arrays],
        in_specs=[vspec] * n,
        out_specs=[vspec] * n,
        scratch_shapes=[pltpu.SemaphoreType.DMA((n, 3)), pltpu.SemaphoreType.DMA((n, 3))],
        compiler_params=pltpu.CompilerParams(collective_id=ident, has_side_effects=True, vmem_limit_bytes=VMEM_LIMIT),
        name="swap",
    )(*arrays)


def solution(mesh):
    def per_device(lower_tri):
        n_mat, n_rblk, blk, n_cloc = lower_tri.shape
        n_rloc = n_rblk * blk
        my_row = lax.axis_index('row')
        core = lax.rem(my_row, 2)
        low = lower_tri.reshape(n_mat, n_rloc, n_cloc)
        slab = jnp.swapaxes(low[:, :, : 2 * NB], 1, 2).reshape(n_mat, 2, NB, n_rloc)
        pt = gather_call(slab[:, 0])
        pts, pt = rest_of_panels(slab, my_row, pt)
        smalls = []
        small, vt, t, tt = panel_call(0, pt)
        smalls.append(small)
        v_other, = swap_call(2, vt)
        p1, p2, v_out = tile_call(0, low, (vt, v_other), None, None)
        for k in range(1, PANELS):
            yt = sum_call(p1, p2)
            wt, small, v_new, t, tt, *pts = panel_call(k, vt, yt, t, tt, *pts)
            smalls.append(small)
            w_other, v_new_other = swap_call(3, wt, v_new)
            prev = (vt, v_other, wt, w_other)
            vt, v_other = v_new, v_new_other
            low, p1, p2, v_out = tile_call(k, low, (vt, v_other), prev, v_out)
        yt = sum_call(p1, p2)
        wt, = panel_call(PANELS, vt, yt, t, tt)
        packed = jnp.stack(smalls)
        w_other, packed_other = swap_call(4, wt, packed)
        low, = tile_call(PANELS, low, None, (vt, v_other, wt, w_other), None)
        both = jnp.where(core == 0, jnp.stack([packed, packed_other]), jnp.stack([packed_other, packed]))
        both = both[..., :NB]
        dr = jnp.swapaxes(both[:, :, :2], 3, 4)
        off = jnp.stack([packed[3, 1, :, NB:], packed_other[3, 1, :, NB:]])
        off = jnp.where(core == 0, off, off[::-1])
        band = dr.at[:, 3, 1].set(jnp.swapaxes(off, 1, 2))
        return low.reshape(lower_tri.shape), band, v_out.reshape(n_mat, PANELS, n_rblk, blk, blk), both[:, :, 2]

    spec_low = P('sys', 'row', None, 'col')
    return jax.shard_map(per_device, mesh=mesh, in_specs=(spec_low,), out_specs=(spec_low, P('sys'), P('sys', None, 'row', None, None), P('sys')), check_vma=False)
```

```python
import functools

import jax
import jax.numpy as jnp
from jax import lax
from jax.experimental import pallas as pl
from jax.experimental.pallas import tpu as pltpu
from jax.sharding import PartitionSpec as P

PANELS = 4
NB = 64
N = 4096
QTR = 1024
LANE = 128
COLS = 2048
N_CH = N // LANE
TR, TC = 256, 512
TILE = (8, LANE)
WIDE = (NB, LANE)
F32 = jnp.float32
BF16 = jnp.bfloat16
MESH = pl.DeviceIdType.MESH
VMEM_LIMIT = 60 * 1024 * 1024


def span(i, width=LANE):
    return slice(i * width, (i + 1) * width)


def quarter(row):
    return pl.ds(pl.multiple_of(row * QTR, QTR), QTR)


def half_quarter(row, half):
    width = QTR // 2
    return pl.ds(pl.multiple_of(row * QTR + half * width, width), width)


def sum_of(terms):
    return functools.reduce(lambda a, b: a + b, terms)


def halves(low_half, a, b):
    return jnp.where(low_half, a, pltpu.roll(b, NB, 1)), jnp.where(low_half, pltpu.roll(a, NB, 1), b)


def split3(a):
    hi = a.astype(BF16)
    rest = a - hi.astype(F32)
    mid = rest.astype(BF16)
    low = (rest - mid.astype(F32)).astype(BF16)
    return hi, mid, low


def bdot(a, b, ca=1, cb=0):
    return lax.dot_general(a, b, (((ca,), (cb,)), ((), ())), preferred_element_type=F32)


def fold_rows(x):
    n = x.shape[0] // 3
    return x[2 * n :] + x[n : 2 * n] + x[:n]


def mm(a, b, cb=0):
    lhs = jnp.concatenate(split3(a), axis=0)
    b1, b2, b3 = split3(b)
    return fold_rows(bdot(lhs, b3, 1, cb) + bdot(lhs, b2, 1, cb) + bdot(lhs, b1, 1, cb))


def gram(a_ref, b_ref, mask=None):
    acc = None
    for t in range(N // 512):
        sl = span(t, 512)
        lhs = jnp.concatenate(split3(a_ref[:, sl]), axis=0)
        rhs = jnp.concatenate(split3(b_ref[:, sl]), axis=0)
        part = bdot(lhs, rhs, 1, 1)
        acc = part if acc is None else acc + part
    acc = fold_rows(acc)
    return sum_of([acc[:, span(q, NB)] for q in reversed(range(3))])


def bcast(v):
    return jnp.broadcast_to(v, TILE)


def qr_step(a_ref, xcur, xnext, stats, pc, pl0, gi, s, last_of_pair, accs):
    beta_ref, inv_ref, tau_ref = stats
    lane = lax.broadcasted_iota(jnp.int32, TILE, 1)
    sub = lax.broadcasted_iota(jnp.int32, (8, 1), 0)
    n_g = 8 - gi
    j = gi * 8 + s
    p = pl0 + j
    rows = [span(gi + g, 8) for g in range(n_g)]
    dots = [jnp.sum(acc, axis=1, keepdims=True) for acc in accs]
    pvs = [jnp.sum(jnp.where(lane == p, a_ref[pc, r, :], 0.0), axis=1, keepdims=True) for r in rows]
    sigma = jnp.sum(jnp.where(sub == s, dots[0], 0.0), axis=0, keepdims=True)
    alpha = jnp.sum(jnp.where(sub == s, pvs[0], 0.0), axis=0, keepdims=True)
    sq = alpha * alpha + sigma
    inv_norm = lax.rsqrt(sq)
    norm = jnp.sqrt(sq)
    pos = alpha >= 0
    beta = jnp.where(pos, -norm, norm)
    ninvb = jnp.where(pos, inv_norm, -inv_norm)
    denom = alpha - beta
    inv_den = 1.0 / denom
    tau = denom * ninvb
    cs = [(pv + d * inv_den) * ninvb for pv, d in zip(pvs, dots)]
    cs[0] = jnp.where(sub > s, cs[0], 0.0)
    beta_ref[pl.ds(j, 1), :] = jnp.broadcast_to(beta, (1, 128))
    inv_ref[pl.ds(j, 1), :] = jnp.broadcast_to(inv_den, (1, 128))
    tau_ref[pl.ds(j, 1), :] = jnp.broadcast_to(tau, (1, 128))
    c_next = jnp.sum(jnp.where(sub == s + 1, cs[0], 0.0), axis=0, keepdims=True)
    if last_of_pair and n_g > 1:
        c_next = c_next + jnp.where(s == 7, cs[1][0:1], 0.0)
    jn = jnp.minimum(j + 1, NB - 1)
    c_next = bcast(c_next)
    den_b = bcast(denom)
    for ch in range(N_CH):
        xt = xcur[ch]
        if ch == pc:
            xt = jnp.where(lane == p, den_b, xt)
        xn = a_ref[ch, pl.ds(jn, 8, stride=0), :] - c_next * xt
        if ch == pc:
            xn = jnp.where(lane > p + 1, xn, 0.0)
        xnext[ch] = xn
    cs = [bcast(c) for c in cs]
    out = [jnp.zeros(TILE, F32) for _ in range(n_g)]
    for ch in range(N_CH):
        xt = xcur[ch]
        if ch == pc:
            xt = jnp.where(lane == p, den_b, xt)
        xn = xnext[ch]
        for g in range(n_g):
            a = a_ref[ch, rows[g], :] - cs[g] * xt
            a_ref[ch, rows[g], :] = a
            out[g] = out[g] + a * xn
    return tuple(out)


def qr_panel(a_ref, x_refs, stats, pc, pl0):
    lane = lax.broadcasted_iota(jnp.int32, TILE, 1)
    accs = [jnp.zeros(TILE, F32) for _ in range(8)]
    for ch in range(N_CH):
        x = bcast(a_ref[ch, 0:1, :])
        if ch == pc:
            x = jnp.where(lane > pl0, x, 0.0)
        x_refs[0][ch] = x
        for g in range(8):
            accs[g] = accs[g] + a_ref[ch, span(g, 8), :] * x
    accs = tuple(accs)
    for gi in range(8):

        def pair(h, accs, gi=gi):
            for par in range(2):
                accs = qr_step(a_ref, x_refs[par], x_refs[1 - par], stats, pc, pl0, gi, h * 2 + par, par == 1, accs)
            return accs

        accs = lax.fori_loop(0, 4, pair, accs)[1:]


def finish_panel(a_ref, stats, vt_ref, rt_ref, pc, pl0):
    beta_ref, inv_ref, tau_ref = stats
    lane = lax.broadcasted_iota(jnp.int32, TILE, 1)
    sub = lax.broadcasted_iota(jnp.int32, TILE, 0)
    for g in range(8):
        rows = span(g, 8)
        inv = inv_ref[rows, :]
        for ch in range(N_CH):
            sl = span(ch)
            a = a_ref[ch, rows, :]
            v = a * inv
            if ch == pc:
                rel = lane - pl0 - (g * 8 + sub)
                rt_ref[rows, :] = jnp.where(rel < 0, a, jnp.where(rel == 0, beta_ref[rows, :], 0.0))
                v = jnp.where(rel > 0, v, jnp.where(rel == 0, 1.0, 0.0))
            vt_ref[rows, sl] = v


def build_tri(gram_mat, tau_col):
    row = lax.broadcasted_iota(jnp.int32, (NB, NB), 0)
    col = lax.broadcasted_iota(jnp.int32, (NB, NB), 1)
    t = jnp.where(row == col, tau_col, 0.0)
    for lg in range(6):
        rb = lax.shift_right_logical(row, lg)
        cb = lax.shift_right_logical(col, lg)
        u = jnp.where((cb == rb + 1) & (lax.rem(rb, 2) == 0), gram_mat, 0.0)
        t = t - mm(mm(t, u), t)
    return t


def panel_kernel(step, *refs):
    refs = list(refs)
    n_rem = PANELS - step
    if step > 0:
        vt_ref, yt_ref, t_ref, tt_ref = refs[:4]
        refs = refs[4:]
    if step == 1:
        pieces, refs = refs[:8], refs[8:]
    elif n_rem:
        pt_ref = refs.pop(0)
    if step > 0:
        wt_ref = refs.pop(0)
    if n_rem:
        small_ref, vn_ref, tn_ref, ttn_ref = refs[:4]
        refs = refs[4:]
        if step > 0 and n_rem > 1:
            rem_ref = refs.pop(0)
        a_ref, xa, xb, beta_ref, inv_ref, tau_ref = refs
    lane64 = lax.broadcasted_iota(jnp.int32, WIDE, 1)
    row64 = lax.broadcasted_iota(jnp.int32, WIDE, 0)
    if step > 0:
        for g in range(step):
            sl = span(8 * g)
            yt_ref[:, sl] = jnp.where(lane64 < NB, 0.0, yt_ref[:, sl])
        s_mat = gram(vt_ref, yt_ref)
        m_mat = mm(mm(tt_ref[...], s_mat, 1), t_ref[...])
        lhs = jnp.concatenate([tt_ref[...], -0.5 * m_mat], axis=1)
        for t in range(N // 512):
            sl = span(t, 512)
            wt_ref[:, sl] = mm(lhs, jnp.concatenate([yt_ref[:, sl], vt_ref[:, sl]], axis=0))
    if not n_rem:
        return
    if step == 1:
        x, core, y = place()
        for dx in range(2):
            for f in range(2):
                row = 2 * (1 - x if dx else x) + (1 - core if f else core)
                lanes = pl.ds(pl.multiple_of(row * QTR, QTR), QTR)
                here, there = 2 * dx + f, 4 + 2 * dx + f
                first = jnp.where(y == 1, pieces[here][0], pieces[there][0])
                for ch in range(8):
                    a_ref[row * 8 + ch] = first[:, span(ch)]
                one, two = pieces[here][1], pieces[there][1]
                rem_ref[0, :, lanes] = jnp.where(y == 0, one, two)
                rem_ref[1, :, lanes] = jnp.where(y == 1, one, two)
    if step > 0:
        lefts = []
        for q in range(step, PANELS):
            sl = span(8 * q)
            wc = wt_ref[:, sl].T[:NB]
            vc = vt_ref[:, sl].T[:NB]
            lefts.append(jnp.concatenate([wc, vc], axis=1))
        lhs = jnp.concatenate(lefts, axis=0)
        for t in range(N // 256):
            sl = span(t, TR)
            upd = mm(lhs, jnp.concatenate([vt_ref[:, sl], wt_ref[:, sl]], axis=0))
            for h in range(2):
                old = a_ref[2 * t + h] if step == 1 else pt_ref[0, :, span(2 * t + h)]
                a_ref[2 * t + h] = old - upd[:NB, span(h)]
            for q in range(1, n_rem):
                old = rem_ref[q - 1, :, sl] if step == 1 else pt_ref[q, :, sl]
                rem_ref[q - 1, :, sl] = old - upd[span(q, NB)]
    else:
        for ch in range(N_CH):
            a_ref[ch] = pt_ref[:, span(ch)]
    small_ref[0] = jnp.where((lane64 >= row64) & (lane64 < NB), a_ref[step * 8], 0.0)
    for g in range(step + 1):
        a_ref[g * 8] = jnp.where(lane64 < NB, 0.0, a_ref[g * 8])
    pc = ((step + 1) % PANELS) * (QTR // LANE)
    pl0 = NB * ((step + 1) // PANELS)
    stats = (beta_ref, inv_ref, tau_ref)
    qr_panel(a_ref, (xa, xb), stats, pc, pl0)
    finish_panel(a_ref, stats, vn_ref, small_ref.at[1], pc, pl0)
    t_new = build_tri(gram(vn_ref, vn_ref), tau_ref[:, :NB])
    tn_ref[...] = t_new
    t_wide = jnp.concatenate([t_new, jnp.zeros((NB, NB), F32)], axis=1)
    small_ref[2] = t_wide
    ttn_ref[...] = t_wide.T[:NB]


def panel_call(step, *args):
    n_rem = PANELS - step
    outs = []
    full = jax.ShapeDtypeStruct((NB, N), F32)
    small = jax.ShapeDtypeStruct((NB, NB), F32)
    scratch = []
    if step > 0:
        outs.append(full)
    if n_rem:
        outs += [jax.ShapeDtypeStruct((3, NB, 128), F32), full, small, small]
        if step > 0 and n_rem > 1:
            outs.append(jax.ShapeDtypeStruct((n_rem - 1, NB, N), F32))
        scratch = [pltpu.VMEM((N_CH, NB, 128), F32), pltpu.VMEM((N_CH, 8, 128), F32), pltpu.VMEM((N_CH, 8, 128), F32)] + [pltpu.VMEM(WIDE, F32)] * 3
    vspec = pl.BlockSpec(memory_space=pltpu.VMEM)
    return pl.pallas_call(
        functools.partial(panel_kernel, step),
        out_shape=outs,
        in_specs=[vspec] * len(args),
        out_specs=[vspec] * len(outs),
        scratch_shapes=scratch,
        compiler_params=pltpu.CompilerParams(vmem_limit_bytes=VMEM_LIMIT),
        cost_estimate=pl.CostEstimate(flops=20_000_000_000, bytes_accessed=8_000_000, transcendentals=0),
        name=f"panel{step}",
    )(*args)


def barrier(neighbours):
    sem = pltpu.get_barrier_semaphore()
    for dev in neighbours:
        pl.semaphore_signal(sem, inc=1, device_id=dev, device_id_type=MESH)
    pl.semaphore_wait(sem, len(neighbours))


def remote(src, dst, send, recv, dev):
    return pltpu.make_async_remote_copy(src_ref=src, dst_ref=dst, send_sem=send, recv_sem=recv, device_id=dev, device_id_type=MESH)


def place():
    my_row = lax.axis_index('row')
    my_col = lax.axis_index('col')
    return lax.div(my_row, 2), lax.rem(my_row, 2), my_col


def device(x, core, y):
    return {'row': 2 * x + core, 'col': y}


def gather_kernel(slab_ref, pt_ref, send, recv, fwd_send, fwd_recv):
    x, core, y = place()
    other = 1 - core
    barrier([device(x, other, y), device(1 - x, core, y), device(1 - x, other, y), device(x, core, 1 - y), device(x, other, 1 - y)])
    n_part = PANELS
    width = QTR // n_part

    def lanes(row, part=None):
        if part is None:
            return pl.ds(pl.multiple_of(row * QTR, QTR), QTR)
        return pl.ds(pl.multiple_of(row * QTR + part * width, width), width)

    def push(to_core, dev, part, s_sem, r_sem):
        return remote(slab_ref.at[to_core, :, part * width : (part + 1) * width], pt_ref.at[:, lanes(2 * x + core, part)], s_sem, r_sem, dev)

    def onward(row, part, idx):
        ref = pt_ref.at[:, lanes(row, part)]
        return remote(ref, ref, fwd_send.at[idx, part], fwd_recv.at[idx, part], device(1 - x, core, y))

    my_row = 2 * x + core
    for part in range(n_part):
        to_y = [push(core, device(x, core, 1 - y), part, send.at[0, part], recv.at[0, part]), push(other, device(x, other, 1 - y), part, send.at[1, part], recv.at[1, part])]
        to_x = [push(core, device(1 - x, core, y), part, send.at[2, part], recv.at[2, part]), push(other, device(1 - x, other, y), part, send.at[3, part], recv.at[3, part])]
        to_p = push(other, device(x, other, y), part, send.at[4, part], recv.at[4, part])

        @pl.when(y == 0)
        def _():
            for cp in to_y + to_x + [to_p]:
                cp.start()

    @pl.when(y == 0)
    def _():
        pt_ref[:, lanes(my_row)] = slab_ref[core]
        for part in range(n_part):
            for idx, (tc, dev) in enumerate([(core, device(x, core, 1)), (other, device(x, other, 1)), (core, device(1 - x, core, 0)), (other, device(1 - x, other, 0)), (other, device(x, other, 0))]):
                cp = push(tc, dev, part, send.at[idx, part], recv.at[idx, part])
                cp.wait_send()
                if idx >= 2:
                    cp.wait_recv()

    @pl.when(y == 1)
    def _():
        for part in range(n_part):
            for idx, row in enumerate([my_row, 2 * x + other]):
                push(core, device(x, core, 0), part, send.at[idx, part], recv.at[idx, part]).wait_recv()
                onward(row, part, idx).start()
        for part in range(n_part):
            for idx in range(2):
                onward(my_row, part, idx).wait()


def gather_call(slab):
    vspec = pl.BlockSpec(memory_space=pltpu.VMEM)
    return pl.pallas_call(
        gather_kernel,
        out_shape=jax.ShapeDtypeStruct((NB, N), F32),
        in_specs=[vspec],
        out_specs=vspec,
        scratch_shapes=[*([pltpu.SemaphoreType.DMA((5, 4))] * 2), *([pltpu.SemaphoreType.DMA((2, 4))] * 2)],
        compiler_params=pltpu.CompilerParams(collective_id=0, has_side_effects=True, vmem_limit_bytes=VMEM_LIMIT),
        name="gather",
    )(slab)


def rest_of_panels(slab, my_row, pt):
    core = lax.rem(my_row, 2)
    own = lax.dynamic_index_in_dim(slab, core, 0, keepdims=False)
    cross = lax.dynamic_index_in_dim(slab, 1 - core, 0, keepdims=False)
    own, cross, pt = lax.optimization_barrier((own, cross, pt))

    def pairs(dx, dy, f):
        flip = 4 * dy + 2 * dx + f
        return [(d, d ^ flip) for d in range(8)]

    pieces = []
    for dy in range(2):
        for dx in range(2):
            for f in range(2):
                payload = cross if f else own
                pieces.append(payload if (dx, dy, f) == (0, 0, 0) else lax.ppermute(payload, ('col', 'row'), pairs(dx, dy, f)))
    return pieces, pt


def needed(x, y):
    return [quarter(row) for row in (y, 2 + y, 2 * x + 1 - y)]


def swap_kernel(w_ref, small_ref, w_out, small_out, send, recv):
    x, core, y = place()
    partner = device(x, 1 - core, y)
    barrier([partner])
    copies = [remote(w_ref.at[:, sl], w_out.at[1, :, sl], send.at[q], recv.at[q], partner) for q, sl in enumerate(needed(x, y))]
    copies.append(remote(small_ref, small_out, send.at[3], recv.at[3], partner))
    for cp in copies:
        cp.start()
    w_out[0] = w_ref[...]
    for cp in copies:
        cp.wait()


def swap_call(w, small):
    whole = pl.BlockSpec(memory_space=pltpu.VMEM)
    return pl.pallas_call(
        swap_kernel,
        out_shape=[jax.ShapeDtypeStruct((2, NB, N), F32), jax.ShapeDtypeStruct(small.shape, F32)],
        in_specs=[whole] * 2,
        out_specs=[whole] * 2,
        scratch_shapes=[pltpu.SemaphoreType.DMA((4,))] * 2,
        compiler_params=pltpu.CompilerParams(collective_id=5, has_side_effects=True, vmem_limit_bytes=VMEM_LIMIT),
        name="swap",
    )(w, small)


def step_kernel(update, products, *refs):
    refs = list(refs)
    take = lambda n: [refs.pop(0) for _ in range(n)]
    (l_ref,) = take(1)
    if products:
        (va,) = take(1)
    if update:
        uu, ww = take(2)
        if products:
            wa = ww
            take(1)
        (lo_ref,) = take(1)
    if products:
        yt_out, vv_out, vo_ref = take(3)
        vv, yt, vc3, vr3, acc1, acc2, p1_ref, p2_ref = take(8)
        r_part, r_own, r_p1, r_p2, sbuf, qbuf, send, recv = take(8)
        v_send, v_recv = take(2)
    if update:
        if products:
            (ww,) = take(1)
        left6, right6 = take(2)
    mat = pl.program_id(0)
    ti = pl.program_id(1)
    x, core, y = place()
    my_row = 2 * x + core
    other = 1 - core
    partner = device(x, other, y)
    x_nbr = device(1 - x, core, y)
    y_nbr = device(x, core, 1 - y)
    y_cross = device(x, other, 1 - y)
    slot = lax.rem(core + mat, 2)
    low_half = lax.broadcasted_iota(jnp.int32, (NB, LANE), 1) < NB

    if products:
        swaps = [(va, vv)] + ([(wa, ww)] if update else [])
        swaps = [remote(src.at[:, sl], dst.at[1, :, sl], v_send.at[i, q], v_recv.at[i, q], partner) for i, (src, dst) in enumerate(swaps) for q, sl in enumerate(needed(x, y))]

        @pl.when((mat == 0) & (ti == 0))
        def _():
            barrier([partner, x_nbr, y_nbr, y_cross])
            for cp in swaps:
                cp.start()
            vv[0] = va[...]
            if update:
                ww[0] = wa[...]

        @pl.when((mat == other) & (ti == 0))
        def _():
            for cp in swaps:
                cp.wait()

    def pick(ref, base, ch):
        return ref[slot, :, pl.ds(pl.multiple_of(base * QTR + ch * LANE, LANE), LANE)]

    def col_chunks(ref, u):
        qa = pick(ref, y, u)
        qb = pick(ref, y + 2, u)
        return halves(low_half, qa, qb)

    @pl.when(ti == 0)
    def _():
        if products:
            acc2[...] = jnp.zeros_like(acc2)
            vc3[3 * NB :, :] = jnp.zeros((NB, COLS), BF16)
            for u in range(8):
                for h, part in enumerate(col_chunks(vv, u)):
                    for q, piece in enumerate(split3(part)):
                        vc3[span(q, NB), span(2 * u + h)] = piece
                mine_rows = pick(vv, my_row, u)
                for q, piece in enumerate(split3(mine_rows)):
                    vr3[span(q, NB), span(u)] = piece
                vo_ref[0, 0, span(u), :] = mine_rows.T
        if update:
            for u in range(8):
                vcs = col_chunks(uu, u)
                wcs = col_chunks(ww, u)
                for h in range(2):
                    r1, r2, r3 = split3(jnp.concatenate([wcs[h], vcs[h]], axis=0))
                    for q, piece in enumerate((r3, r2, r1, r2, r1, r1)):
                        right6[span(q), span(2 * u + h)] = piece
                left = jnp.concatenate([pick(uu, my_row, u), pick(ww, my_row, u)], axis=0).T
                a1, a2, a3 = split3(left)
                for q, piece in enumerate((a1, a2, a3, a1, a2, a1)):
                    left6[span(u), span(q)] = piece

    row_sl = pl.ds(pl.multiple_of(ti * TR, TR), TR)

    def run(tj, diag):
        col_sl = pl.ds(pl.multiple_of(tj * TC, TC), TC)
        tile = l_ref[0, :, col_sl]
        if diag or not products:
            ri = lax.broadcasted_iota(jnp.int32, (TR, TC), 0) + ti * TR
            ci = lax.broadcasted_iota(jnp.int32, (TR, TC), 1) + tj * TC
            rg = (lax.div(ri, NB) * 4 + my_row) * NB + lax.rem(ri, NB)
            cg = (lax.div(ci, NB) * 2 + y) * NB + lax.rem(ci, NB)
        if update:
            upd = bdot(left6[row_sl, :], right6[:, col_sl])
            tile = tile - (jnp.where(rg >= cg, upd, 0.0) if diag else upd)
            if not products:
                done = PANELS * NB
                tile = jnp.where((rg >= done) & (cg >= done), tile, 0.0)
            lo_ref[0, :, col_sl] = tile
        if products:
            parts = split3(tile)[::-1]
            vcols = vc3[:, col_sl]
            vrows = vr3[:, row_sl]
            acc2[:, col_sl] += sum_of([bdot(vrows, part) for part in parts])
            if diag:
                parts = [jnp.where(rg == cg, jnp.zeros_like(part), part) for part in parts]
            p1 = fold_rows(bdot(jnp.concatenate(parts[::-1], axis=0), vcols, 1, 1))
            if diag:
                tot = acc1[...] + p1
                tot = (tot[:, :LANE] + tot[:, LANE:]).T
                p1_ref[mat, :, row_sl] = tot[NB:] + tot[:NB]
            else:
                acc1[...] += p1

    if products:
        acc1[...] = jnp.zeros_like(acc1)

    @pl.loop(0, ti)
    def _(tj):
        run(tj, False)

    run(ti, True)

    if update:

        @pl.loop(ti + 1, 4)
        def _(tj):
            lo_ref[0, :, pl.ds(pl.multiple_of(tj * TC, TC), TC)] = jnp.zeros((TR, TC), F32)

    if not products:
        return

    @pl.when(ti == 3)
    def _():
        for u in range(8):
            ev = fold_rows(acc2[:, span(2 * u)])
            od = fold_rows(acc2[:, span(2 * u + 1)])
            p2_ref[mat, 0, :, span(u)], p2_ref[mat, 1, :, span(u)] = halves(low_half, ev, od)

    mine_part = yt.at[:, quarter(my_q := 2 * x + y)]
    part_y = yt.at[:, half_quarter(2 * x + 1 - y, 0)]
    part_x = yt.at[:, half_quarter(2 * (1 - x) + y, 1)]

    def helper_copies(q):
        part = remote(p2_ref.at[q], r_part, send.at[0], recv.at[0], partner)
        far = remote(p1_ref.at[q], r_p1, send.at[1], recv.at[1], y_cross)
        near = remote(p1_ref.at[q], r_own, send.at[1], recv.at[2], partner)
        return part, far, near

    def owner_copies(q):
        far = remote(p1_ref.at[q], r_p1, send.at[2], recv.at[1], y_nbr)
        over_x = remote(sbuf, r_p2, send.at[3], recv.at[3], x_nbr)
        g_x = remote(qbuf, mine_part, send.at[4], recv.at[4], x_nbr)
        g_y = remote(qbuf, mine_part, send.at[5], recv.at[5], y_nbr)
        f_x = remote(part_y, part_y, send.at[6], recv.at[6], x_nbr)
        f_y = remote(part_x, part_x, send.at[7], recv.at[7], y_nbr)
        return far, over_x, g_x, g_y, f_x, f_y

    def help_out(q):
        part, far, near = helper_copies(q)
        part.start()
        pl.when(core != y)(far.start)
        pl.when(core == y)(near.start)

    def help_end(q):
        part, far, near = helper_copies(q)
        part.wait_send()
        far.wait_send()

    def stage_a(q):
        pl.when(core != y)(owner_copies(q)[0].start)

    def stage_b(q):
        part, _, near = helper_copies(q)
        part.wait_recv()
        sbuf[...] = p2_ref[q, 1 - x] + r_part[1 - x]
        owner_copies(q)[1].start()
        qbuf[...] = p2_ref[q, x] + r_part[x]

        @pl.when(core == y)
        def _():
            qbuf[...] += p1_ref[q]

        @pl.when(core != y)
        def _():
            near.wait_recv()
            qbuf[...] += r_own[...]

    def stage_c(q):
        far, over_x, g_x, g_y, _, _ = owner_copies(q)
        far.wait_recv()
        qbuf[...] += r_p1[...]
        over_x.wait()
        qbuf[...] += r_p2[...]
        g_x.start()
        g_y.start()
        mine_part[...] = qbuf[...]

    def stage_d(q):
        _, _, g_x, g_y, f_x, f_y = owner_copies(q)
        g_y.wait_recv()
        f_x.start()
        g_x.wait_recv()
        f_y.start()

    def stage_e(q):
        far, _, g_x, g_y, f_x, f_y = owner_copies(q)
        pl.when(core != y)(far.wait_send)
        g_x.wait_send()
        g_y.wait_send()
        f_x.wait()
        f_y.wait()

    last = (mat == 1) & (ti == 3)
    for cond, stage in (((mat == 0) & (ti == 3), stage_a), ((mat == 1) & (ti == 0), stage_b), ((mat == 1) & (ti == 1), stage_c), ((mat == 1) & (ti == 2), stage_d), (last, stage_e)):
        pl.when(cond & (core == 0))(functools.partial(stage, 0))
    pl.when((mat == 0) & (ti == 3) & (core == 1))(functools.partial(help_out, 0))

    @pl.when(last & (core == 0))
    def _():
        help_out(1)
        help_end(1)

    @pl.when(last & (core == 1))
    def _():
        help_end(0)
        for stage in (stage_a, stage_b, stage_c, stage_d, stage_e):
            stage(1)

    @pl.when(last)
    def _():
        yt_out[...] = yt[...]
        for ch in range(N_CH):
            vv_out[:, :, span(ch)] = vv[:, :, span(ch)]


def step_call(k, low, v_own, prev, v_out):
    products = v_own is not None
    update = prev is not None
    strip = pl.BlockSpec((1, TR, COLS), lambda m, i: (m, i, 0))
    whole = pl.BlockSpec(memory_space=pltpu.VMEM)
    left = pl.BlockSpec(memory_space=pl.ANY)
    full, both = jax.ShapeDtypeStruct((NB, N), F32), jax.ShapeDtypeStruct((2, NB, N), F32)
    args, in_specs = [low], [strip]
    outs, out_specs, scratch, alias = [], [], [], {}
    if products:
        args.append(v_own)
        in_specs.append(whole)
    if update:
        args += list(prev)
        in_specs += [whole] * len(prev)
        outs.append(jax.ShapeDtypeStruct(low.shape, F32))
        out_specs.append(strip)
    if products:
        if update:
            alias = {len(args): len(outs) + 2}
            args.append(v_out)
            in_specs.append(left)
        outs += [full, both, jax.ShapeDtypeStruct((2, PANELS, QTR, NB), F32)]
        out_specs += [whole, whole, pl.BlockSpec((1, 1, QTR, NB), lambda m, i: (m, k, 0, 0))]
        qtr, two = pltpu.VMEM((NB, QTR), F32), pltpu.VMEM((2, NB, QTR), F32)
        scratch += [pltpu.VMEM((2, NB, N), F32), pltpu.VMEM((NB, N), F32)] + [pltpu.VMEM((TR, COLS), BF16), pltpu.VMEM((3 * NB, QTR), BF16), pltpu.VMEM((TR, TR), F32), pltpu.VMEM((3 * NB, COLS), F32)]
        scratch += [two, pltpu.VMEM((2, 2, NB, QTR), F32), two] + [qtr] * 5 + [pltpu.SemaphoreType.DMA((8,))] * 2 + [pltpu.SemaphoreType.DMA((2, 3))] * 2
    if update:
        if products:
            scratch.append(pltpu.VMEM((2, NB, N), F32))
        scratch += [pltpu.VMEM((QTR, 6 * LANE), BF16), pltpu.VMEM((6 * LANE, COLS), BF16)]
    return pl.pallas_call(
        functools.partial(step_kernel, update, products),
        out_shape=outs,
        grid=(2, 4),
        in_specs=in_specs,
        out_specs=out_specs,
        scratch_shapes=scratch,
        input_output_aliases=alias,
        compiler_params=pltpu.CompilerParams(vmem_limit_bytes=VMEM_LIMIT, dimension_semantics=("arbitrary",) * 2, **(dict(collective_id=1 + k, has_side_effects=True) if products else {})),
        cost_estimate=pl.CostEstimate(flops=15_000_000_000, bytes_accessed=32_000_000, transcendentals=0),
        name="step",
    )(*args)


def solution(mesh):
    def per_device(lower_tri):
        n_mat, n_rblk, blk, n_cloc = lower_tri.shape
        n_rloc = n_rblk * blk
        my_row = lax.axis_index('row')
        core = lax.rem(my_row, 2)
        low = lower_tri.reshape(n_mat, n_rloc, n_cloc)
        slab = jnp.swapaxes(low[:, :, : 2 * NB], 1, 2).reshape(n_mat, 2, NB, n_rloc)
        pt = gather_call(slab[:, 0])
        pts, pt = rest_of_panels(slab, my_row, pt)
        small, vt, t, tt = panel_call(0, pt)
        smalls = [small]
        yt, v_both, v_out = step_call(0, low, vt, None, None)
        for k in range(1, PANELS):
            wt, small, v_new, t, tt, *pts = panel_call(k, vt, yt, t, tt, *pts)
            smalls.append(small)
            low, yt, v_both, v_out = step_call(k, low, v_new, (v_both, wt), v_out)
            vt = v_new
        (wt,) = panel_call(PANELS, vt, yt, t, tt)
        packed = jnp.stack(smalls)
        w_both, packed_other = swap_call(wt, packed)
        (low,) = step_call(PANELS, low, None, (v_both, w_both), None)
        both = jnp.stack([packed, packed_other])
        both = jnp.where(core == 0, both, both[::-1])
        d_mat = jnp.swapaxes(both[:, :, 0, :, :NB], 2, 3)
        r_mat = jnp.concatenate([both[:, :-1, 1, :, :NB], both[:, -1:, 1, :, NB:]], axis=1)
        band = jnp.stack([d_mat, jnp.swapaxes(r_mat, 2, 3)], axis=2)
        return low.reshape(lower_tri.shape), band, v_out.reshape(n_mat, PANELS, n_rblk, blk, blk), both[:, :, 2, :, :NB]

    spec_low = P('sys', 'row', None, 'col')
    return jax.shard_map(per_device, mesh=mesh, in_specs=(spec_low,), out_specs=(spec_low, P('sys'), P('sys', None, 'row', None, None), P('sys')), check_vma=False)
```

```python
import functools

import jax
import jax.numpy as jnp
from jax import lax
from jax.experimental import pallas as pl
from jax.experimental.pallas import tpu as pltpu
from jax.sharding import PartitionSpec as P

PANELS = 4
NB = 64
N = 4096
QTR = 1024
LANE = 128
COLS = 2048
N_CH = N // LANE
TR, TC = 256, 512
TILE = (8, LANE)
WIDE = (NB, LANE)
F32 = jnp.float32
BF16 = jnp.bfloat16
MESH = pl.DeviceIdType.MESH
VMEM_LIMIT = 60 * 1024 * 1024


def span(i, width=LANE):
    return slice(i * width, (i + 1) * width)


def lane_of(shape):
    return lax.broadcasted_iota(jnp.int32, shape, 1)


def lane_tile(i):
    return pl.ds(pl.multiple_of(i * LANE, LANE), LANE)


def quarter(row):
    return pl.ds(pl.multiple_of(row * QTR, QTR), QTR)


def half_quarter(row, half):
    width = QTR // 2
    return pl.ds(pl.multiple_of(row * QTR + half * width, width), width)


def sum_of(terms):
    return functools.reduce(lambda a, b: a + b, terms)


def halves(low_half, a, b):
    return jnp.where(low_half, a, pltpu.roll(b, NB, 1)), jnp.where(low_half, pltpu.roll(a, NB, 1), b)


def split3(a):
    hi = a.astype(BF16)
    rest = a - hi.astype(F32)
    mid = rest.astype(BF16)
    low = (rest - mid.astype(F32)).astype(BF16)
    return hi, mid, low


def bdot(a, b, ca=1, cb=0):
    return lax.dot_general(a, b, (((ca,), (cb,)), ((), ())), preferred_element_type=F32)


def fold_rows(x):
    n = x.shape[0] // 3
    return x[2 * n :] + x[n : 2 * n] + x[:n]


def mm(a, b, cb=0):
    lhs = jnp.concatenate(split3(a))
    b1, b2, b3 = split3(b)
    return fold_rows(bdot(lhs, b3, 1, cb) + bdot(lhs, b2, 1, cb) + bdot(lhs, b1, 1, cb))


def gram(a_ref, b_ref, mask=None):
    acc = None
    for t in range(N // 512):
        sl = span(t, 512)
        lhs = jnp.concatenate(split3(a_ref[:, sl]))
        rhs = jnp.concatenate(split3(b_ref[:, sl]))
        part = bdot(lhs, rhs, 1, 1)
        acc = part if acc is None else acc + part
    acc = fold_rows(acc)
    return sum_of([acc[:, span(q, NB)] for q in reversed(range(3))])


def bcast(v):
    return jnp.broadcast_to(v, TILE)


def qr_step(a_ref, xcur, xnext, stats, pc, pl0, gi, s, last_of_pair, accs):
    beta_ref, inv_ref, tau_ref = stats
    lane = lane_of(TILE)
    sub = lax.broadcasted_iota(jnp.int32, (8, 1), 0)
    n_g = 8 - gi
    j = gi * 8 + s
    p = pl0 + j
    rows = [span(gi + g, 8) for g in range(n_g)]
    dots = [jnp.sum(acc, axis=1, keepdims=True) for acc in accs]
    pvs = [jnp.sum(jnp.where(lane == p, a_ref[pc, r, :], 0.0), axis=1, keepdims=True) for r in rows]
    sigma = jnp.sum(jnp.where(sub == s, dots[0], 0.0), axis=0, keepdims=True)
    alpha = jnp.sum(jnp.where(sub == s, pvs[0], 0.0), axis=0, keepdims=True)
    sq = alpha * alpha + sigma
    inv_norm = lax.rsqrt(sq)
    norm = jnp.sqrt(sq)
    pos = alpha >= 0
    beta = jnp.where(pos, -norm, norm)
    ninvb = jnp.where(pos, inv_norm, -inv_norm)
    denom = alpha - beta
    inv_den = 1.0 / denom
    tau = denom * ninvb
    cs = [(pv + d * inv_den) * ninvb for pv, d in zip(pvs, dots)]
    cs[0] = jnp.where(sub > s, cs[0], 0.0)
    beta_ref[pl.ds(j, 1), :] = jnp.broadcast_to(beta, (1, 128))
    inv_ref[pl.ds(j, 1), :] = jnp.broadcast_to(inv_den, (1, 128))
    tau_ref[pl.ds(j, 1), :] = jnp.broadcast_to(tau, (1, 128))
    c_next = jnp.sum(jnp.where(sub == s + 1, cs[0], 0.0), axis=0, keepdims=True)
    if last_of_pair and n_g > 1:
        c_next = c_next + jnp.where(s == 7, cs[1][0:1], 0.0)
    jn = jnp.minimum(j + 1, NB - 1)
    c_next = bcast(c_next)
    den_b = bcast(denom)
    for ch in range(N_CH):
        xt = xcur[ch]
        if ch == pc:
            xt = jnp.where(lane == p, den_b, xt)
        xn = a_ref[ch, pl.ds(jn, 8, stride=0), :] - c_next * xt
        if ch == pc:
            xn = jnp.where(lane > p + 1, xn, 0.0)
        xnext[ch] = xn
    cs = [bcast(c) for c in cs]
    out = [jnp.zeros(TILE, F32) for _ in range(n_g)]
    for ch in range(N_CH):
        xt = xcur[ch]
        if ch == pc:
            xt = jnp.where(lane == p, den_b, xt)
        xn = xnext[ch]
        for g in range(n_g):
            a = a_ref[ch, rows[g], :] - cs[g] * xt
            a_ref[ch, rows[g], :] = a
            out[g] = out[g] + a * xn
    return tuple(out)


def qr_panel(a_ref, x_refs, stats, pc, pl0):
    lane = lane_of(TILE)
    accs = [jnp.zeros(TILE, F32) for _ in range(8)]
    for ch in range(N_CH):
        x = bcast(a_ref[ch, 0:1, :])
        if ch == pc:
            x = jnp.where(lane > pl0, x, 0.0)
        x_refs[0][ch] = x
        for g in range(8):
            accs[g] = accs[g] + a_ref[ch, span(g, 8), :] * x
    accs = tuple(accs)
    for gi in range(8):

        def pair(h, accs, gi=gi):
            for par in range(2):
                accs = qr_step(a_ref, x_refs[par], x_refs[1 - par], stats, pc, pl0, gi, h * 2 + par, par == 1, accs)
            return accs

        accs = lax.fori_loop(0, 4, pair, accs)[1:]


def finish_panel(a_ref, stats, vt_ref, rt_ref, pc, pl0):
    beta_ref, inv_ref, tau_ref = stats
    lane = lane_of(TILE)
    sub = lax.broadcasted_iota(jnp.int32, TILE, 0)
    for g in range(8):
        rows = span(g, 8)
        inv = inv_ref[rows, :]
        for ch in range(N_CH):
            sl = span(ch)
            a = a_ref[ch, rows, :]
            v = a * inv
            if ch == pc:
                rel = lane - pl0 - (g * 8 + sub)
                rt_ref[rows, :] = jnp.where(rel < 0, a, jnp.where(rel == 0, beta_ref[rows, :], 0.0))
                v = jnp.where(rel > 0, v, jnp.where(rel == 0, 1.0, 0.0))
            vt_ref[rows, sl] = v


def build_tri(gram_mat, tau_col):
    row = lax.broadcasted_iota(jnp.int32, (NB, NB), 0)
    col = lane_of((NB, NB))
    t = jnp.where(row == col, tau_col, 0.0)
    for lg in range(6):
        rb = lax.shift_right_logical(row, lg)
        cb = lax.shift_right_logical(col, lg)
        u = jnp.where((cb == rb + 1) & (lax.rem(rb, 2) == 0), gram_mat, 0.0)
        t = t - mm(mm(t, u), t)
    return t


def panel_kernel(step, *refs):
    refs = list(refs)
    n_rem = PANELS - step
    if step > 0:
        vt_ref, yt_ref, t_pair = refs[:3]
        refs = refs[3:]
    if step == 1:
        pieces, refs = refs[:8], refs[8:]
    elif n_rem:
        pt_ref = refs.pop(0)
    if step > 0:
        wt_ref = refs.pop(0)
    if n_rem:
        small_ref, vn_ref = refs[:2]
        refs = refs[2:]
        if step > 0 and n_rem > 1:
            rem_ref = refs.pop(0)
        a_ref, xa, xb, beta_ref, inv_ref, tau_ref = refs
    lane64 = lane_of(WIDE)
    row64 = lax.broadcasted_iota(jnp.int32, WIDE, 0)
    if step > 0:
        for g in range(step):
            sl = span(8 * g)
            yt_ref[:, sl] = jnp.where(lane64 < NB, 0.0, yt_ref[:, sl])
        s_mat = gram(vt_ref, yt_ref)
        t_mat, t_tr = t_pair[0, :, :NB], t_pair[1, :, :NB]
        m_mat = mm(mm(t_tr, s_mat, 1), t_mat)
        lhs = jnp.concatenate([t_tr, -0.5 * m_mat], axis=1)
        for t in range(N // 512):
            sl = span(t, 512)
            wt_ref[:, sl] = mm(lhs, jnp.concatenate([yt_ref[:, sl], vt_ref[:, sl]]))
    if not n_rem:
        return
    if step == 1:
        x, core, y = place()
        for dx in range(2):
            for f in range(2):
                row = 2 * (1 - x if dx else x) + (1 - core if f else core)
                lanes = pl.ds(pl.multiple_of(row * QTR, QTR), QTR)
                here, there = 2 * dx + f, 4 + 2 * dx + f
                first = jnp.where(y == 1, pieces[here][0], pieces[there][0])
                for ch in range(8):
                    a_ref[row * 8 + ch] = first[:, span(ch)]
                one, two = pieces[here][1], pieces[there][1]
                rem_ref[0, :, lanes] = jnp.where(y == 0, one, two)
                rem_ref[1, :, lanes] = jnp.where(y == 1, one, two)
    if step > 0:
        lefts = []
        for q in range(step, PANELS):
            sl = span(8 * q)
            wc = wt_ref[:, sl].T[:NB]
            vc = vt_ref[:, sl].T[:NB]
            lefts.append(jnp.concatenate([wc, vc], axis=1))
        lhs = jnp.concatenate(lefts)
        for t in range(N // 256):
            sl = span(t, TR)
            upd = mm(lhs, jnp.concatenate([vt_ref[:, sl], wt_ref[:, sl]]))
            for h in range(2):
                old = a_ref[2 * t + h] if step == 1 else pt_ref[0, :, span(2 * t + h)]
                a_ref[2 * t + h] = old - upd[:NB, span(h)]
            for q in range(1, n_rem):
                old = rem_ref[q - 1, :, sl] if step == 1 else pt_ref[q, :, sl]
                rem_ref[q - 1, :, sl] = old - upd[span(q, NB)]
    else:
        for ch in range(N_CH):
            a_ref[ch] = pt_ref[:, span(ch)]
    small_ref[0] = jnp.where((lane64 >= row64) & (lane64 < NB), a_ref[step * 8], 0.0)
    for g in range(step + 1):
        a_ref[g * 8] = jnp.where(lane64 < NB, 0.0, a_ref[g * 8])
    pc = ((step + 1) % PANELS) * (QTR // LANE)
    pl0 = NB * ((step + 1) // PANELS)
    stats = (beta_ref, inv_ref, tau_ref)
    qr_panel(a_ref, (xa, xb), stats, pc, pl0)
    finish_panel(a_ref, stats, vn_ref, small_ref.at[1], pc, pl0)
    small_ref[2] = tau_ref[...]


def panel_call(step, *args):
    n_rem = PANELS - step
    outs = []
    full = jax.ShapeDtypeStruct((NB, N), F32)
    scratch = []
    if step > 0:
        outs.append(full)
    if n_rem:
        outs += [jax.ShapeDtypeStruct((3, NB, LANE), F32), full]
        if step > 0 and n_rem > 1:
            outs.append(jax.ShapeDtypeStruct((n_rem - 1, NB, N), F32))
        scratch = [pltpu.VMEM((N_CH, NB, 128), F32), pltpu.VMEM((N_CH, 8, 128), F32), pltpu.VMEM((N_CH, 8, 128), F32)] + [pltpu.VMEM(WIDE, F32)] * 3
    vspec = pl.BlockSpec(memory_space=pltpu.VMEM)
    return pl.pallas_call(
        functools.partial(panel_kernel, step),
        out_shape=outs,
        in_specs=[vspec] * len(args),
        out_specs=[vspec] * len(outs),
        scratch_shapes=scratch,
        compiler_params=pltpu.CompilerParams(vmem_limit_bytes=VMEM_LIMIT),
        cost_estimate=pl.CostEstimate(flops=20_000_000_000, bytes_accessed=8_000_000, transcendentals=0),
        name=f"panel{step}",
    )(*args)


def barrier(neighbours):
    sem = pltpu.get_barrier_semaphore()
    for dev in neighbours:
        pl.semaphore_signal(sem, inc=1, device_id=dev, device_id_type=MESH)
    pl.semaphore_wait(sem, len(neighbours))


def remote(src, dst, send, recv, dev):
    return pltpu.make_async_remote_copy(src_ref=src, dst_ref=dst, send_sem=send, recv_sem=recv, device_id=dev, device_id_type=MESH)


def place():
    my_row = lax.axis_index('row')
    my_col = lax.axis_index('col')
    return lax.div(my_row, 2), lax.rem(my_row, 2), my_col


def device(x, core, y):
    return {'row': 2 * x + core, 'col': y}


def gather_kernel(slab_ref, pt_ref, send, recv, fwd_send, fwd_recv):
    x, core, y = place()
    other = 1 - core
    barrier([device(x, other, y), device(1 - x, core, y), device(1 - x, other, y), device(x, core, 1 - y), device(x, other, 1 - y)])
    n_part = PANELS
    width = QTR // n_part

    def lanes(row, part=None):
        if part is None:
            return pl.ds(pl.multiple_of(row * QTR, QTR), QTR)
        return pl.ds(pl.multiple_of(row * QTR + part * width, width), width)

    def push(to_core, dev, part, s_sem, r_sem):
        return remote(slab_ref.at[to_core, :, part * width : (part + 1) * width], pt_ref.at[:, lanes(2 * x + core, part)], s_sem, r_sem, dev)

    def onward(row, part, idx):
        ref = pt_ref.at[:, lanes(row, part)]
        return remote(ref, ref, fwd_send.at[idx, part], fwd_recv.at[idx, part], device(1 - x, core, y))

    my_row = 2 * x + core
    for part in range(n_part):
        to_y = [push(core, device(x, core, 1 - y), part, send.at[0, part], recv.at[0, part]), push(other, device(x, other, 1 - y), part, send.at[1, part], recv.at[1, part])]
        to_x = [push(core, device(1 - x, core, y), part, send.at[2, part], recv.at[2, part]), push(other, device(1 - x, other, y), part, send.at[3, part], recv.at[3, part])]
        to_p = push(other, device(x, other, y), part, send.at[4, part], recv.at[4, part])

        @pl.when(y == 0)
        def _():
            for cp in to_y + to_x + [to_p]:
                cp.start()

    @pl.when(y == 0)
    def _():
        pt_ref[:, lanes(my_row)] = slab_ref[core]
        for part in range(n_part):
            for idx, (tc, dev) in enumerate([(core, device(x, core, 1)), (other, device(x, other, 1)), (core, device(1 - x, core, 0)), (other, device(1 - x, other, 0)), (other, device(x, other, 0))]):
                cp = push(tc, dev, part, send.at[idx, part], recv.at[idx, part])
                cp.wait_send()
                if idx >= 2:
                    cp.wait_recv()

    @pl.when(y == 1)
    def _():
        for part in range(n_part):
            for idx, row in enumerate([my_row, 2 * x + other]):
                push(core, device(x, core, 0), part, send.at[idx, part], recv.at[idx, part]).wait_recv()
                onward(row, part, idx).start()
        for part in range(n_part):
            for idx in range(2):
                onward(my_row, part, idx).wait()


def gather_call(slab):
    vspec = pl.BlockSpec(memory_space=pltpu.VMEM)
    return pl.pallas_call(
        gather_kernel,
        out_shape=jax.ShapeDtypeStruct((NB, N), F32),
        in_specs=[vspec],
        out_specs=vspec,
        scratch_shapes=[*([pltpu.SemaphoreType.DMA((5, 4))] * 2), *([pltpu.SemaphoreType.DMA((2, 4))] * 2)],
        compiler_params=pltpu.CompilerParams(collective_id=0, has_side_effects=True, vmem_limit_bytes=VMEM_LIMIT),
        name="gather",
    )(slab)


def rest_of_panels(slab, my_row, pt):
    core = lax.rem(my_row, 2)
    own = lax.dynamic_index_in_dim(slab, core, 0, keepdims=False)
    cross = lax.dynamic_index_in_dim(slab, 1 - core, 0, keepdims=False)
    own, cross, pt = lax.optimization_barrier((own, cross, pt))

    def pairs(dx, dy, f):
        flip = 4 * dy + 2 * dx + f
        return [(d, d ^ flip) for d in range(8)]

    pieces = []
    for dy in range(2):
        for dx in range(2):
            for f in range(2):
                payload = cross if f else own
                pieces.append(payload if (dx, dy, f) == (0, 0, 0) else lax.ppermute(payload, ('col', 'row'), pairs(dx, dy, f)))
    return pieces, pt


def needed(x, y):
    return [quarter(row) for row in (y, 2 + y, 2 * x + 1 - y)]


def swap_kernel(w_ref, *refs):
    smalls, refs = refs[:PANELS], refs[PANELS:]
    t_pairs, (w_out, pack_out, send, recv) = refs[:PANELS], refs[PANELS:]
    x, core, y = place()
    partner = device(x, 1 - core, y)
    barrier([partner])
    moves = [(w_ref.at[:, sl], w_out.at[1, :, sl]) for sl in needed(x, y)]
    for k in range(PANELS):
        moves.append((smalls[k].at[:2], pack_out.at[1, k, :2]))
        moves.append((t_pairs[k].at[0], pack_out.at[1, k, 2]))
    copies = [remote(src, dst, send.at[i], recv.at[i], partner) for i, (src, dst) in enumerate(moves)]
    for cp in copies:
        cp.start()
    w_out[0] = w_ref[...]
    for k in range(PANELS):
        pack_out[0, k, :2] = smalls[k][:2]
        pack_out[0, k, 2] = t_pairs[k][0]
    for cp in copies:
        cp.wait()


def swap_call(w, smalls, t_pairs):
    whole = pl.BlockSpec(memory_space=pltpu.VMEM)
    return pl.pallas_call(
        swap_kernel,
        out_shape=[jax.ShapeDtypeStruct((2, NB, N), F32), jax.ShapeDtypeStruct((2, PANELS, 3, NB, LANE), F32)],
        in_specs=[whole] * (1 + 2 * PANELS),
        out_specs=[whole] * 2,
        scratch_shapes=[pltpu.SemaphoreType.DMA((3 + 2 * PANELS,))] * 2,
        compiler_params=pltpu.CompilerParams(collective_id=5, has_side_effects=True, vmem_limit_bytes=VMEM_LIMIT),
        name="swap",
    )(w, *smalls, *t_pairs)


def step_kernel(update, products, *refs):
    refs = list(refs)
    take = lambda n: [refs.pop(0) for _ in range(n)]
    (l_ref,) = take(1)
    if products:
        va, small_ref = take(2)
    if update:
        uu, ww = take(2)
        wa = ww
        if not products:
            v_rows = take(PANELS)
        (lo_ref,) = take(1)
        if not products:
            (vo_ref,) = take(1)
    if products:
        yt_out, vv_out, t_pair = take(3)
        vv, yt, vc3, vr3, acc1, acc2, p1_ref, p2_ref = take(8)
        r_part, r_own, r_p1, r_p2, sbuf, qbuf, send, recv = take(8)
        v_send, v_recv = take(2)
    if update:
        if products:
            (ww,) = take(1)
        left6, right6 = take(2)
    mat = pl.program_id(0)
    ti = pl.program_id(1)
    x, core, y = place()
    my_row = 2 * x + core
    other = 1 - core
    partner = device(x, other, y)
    x_nbr = device(1 - x, core, y)
    y_nbr = device(x, core, 1 - y)
    y_cross = device(x, other, 1 - y)
    slot = lax.rem(core + mat, 2)
    low_half = lane_of(WIDE) < NB

    if products:
        swaps = [(va, vv)] + ([(wa, ww)] if update else [])
        swaps = [remote(src.at[:, sl], dst.at[1, :, sl], v_send.at[i, q], v_recv.at[i, q], partner) for i, (src, dst) in enumerate(swaps) for q, sl in enumerate(needed(x, y))]

        @pl.when((mat == 0) & (ti == 0))
        def _():
            barrier([partner, x_nbr, y_nbr, y_cross])
            for cp in swaps:
                cp.start()
            vv[0] = va[...]
            if update:
                ww[0] = wa[...]
            t_mat = build_tri(gram(va, va), small_ref[2, :, :NB])
            t_pair[0] = jnp.concatenate([t_mat, jnp.zeros_like(t_mat)], axis=1)
            t_pair[1] = jnp.concatenate([t_pair[0], t_pair[0]]).T[:NB]

        @pl.when((mat == other) & (ti == 0))
        def _():
            for cp in swaps:
                cp.wait()

    def pick(ref, base, ch):
        return ref[slot, :, lane_tile(base * 8 + ch)]

    def col_chunks(ref, u):
        qa = pick(ref, y, u)
        qb = pick(ref, y + 2, u)
        return halves(low_half, qa, qb)

    @pl.when(ti == 0)
    def _():
        if not products:
            for k in range(PANELS):
                for u in range(8):
                    vo_ref[0, k, span(u), :] = v_rows[k][0, :, span(u)].T

        if products:
            acc2[...] = jnp.zeros_like(acc2)
            vc3[3 * NB :, :] = jnp.zeros((NB, COLS), BF16)
            for u in range(8):
                for h, part in enumerate(col_chunks(vv, u)):
                    for q, piece in enumerate(split3(part)):
                        vc3[span(q, NB), lane_tile(2 * u + h)] = piece
                for q, piece in enumerate(split3(pick(vv, my_row, u))):
                    vr3[span(q, NB), lane_tile(u)] = piece

        if update:
            for u in range(8):
                vcs = col_chunks(uu, u)
                wcs = col_chunks(ww, u)
                for h in range(2):
                    r1, r2, r3 = split3(jnp.concatenate([wcs[h], vcs[h]]))
                    for q, piece in enumerate((r3, r2, r1, r2, r1, r1)):
                        right6[span(q), lane_tile(2 * u + h)] = piece
                left = jnp.concatenate([pick(uu, my_row, u), pick(ww, my_row, u)]).T
                a1, a2, a3 = split3(left)
                for q, piece in enumerate((a1, a2, a3, a1, a2, a1)):
                    left6[lane_tile(u), span(q)] = piece

    row_sl = pl.ds(pl.multiple_of(ti * TR, TR), TR)

    def run(tj, diag):
        col_sl = pl.ds(pl.multiple_of(tj * TC, TC), TC)
        tile = l_ref[0, :, col_sl]
        if diag or not products:
            ri = lax.broadcasted_iota(jnp.int32, (TR, TC), 0) + ti * TR
            ci = lane_of((TR, TC)) + tj * TC
            rg = (lax.div(ri, NB) * 4 + my_row) * NB + lax.rem(ri, NB)
            cg = (lax.div(ci, NB) * 2 + y) * NB + lax.rem(ci, NB)
        if update:
            upd = bdot(left6[row_sl, :], right6[:, col_sl])
            tile = tile - (jnp.where(rg >= cg, upd, 0.0) if diag else upd)
            if not products:
                done = PANELS * NB
                tile = jnp.where((rg >= done) & (cg >= done), tile, 0.0)
            lo_ref[0, :, col_sl] = tile
        if products:
            parts = split3(tile)[::-1]
            vcols = vc3[:, col_sl]
            vrows = vr3[:, row_sl]
            acc2[:, col_sl] += sum_of([bdot(vrows, part) for part in parts])
            if diag:
                parts = [jnp.where(rg == cg, jnp.zeros_like(part), part) for part in parts]
            p1 = fold_rows(bdot(jnp.concatenate(parts[::-1]), vcols, 1, 1))
            if diag:
                tot = acc1[...] + p1
                tot = (tot[:, :LANE] + tot[:, LANE:]).T
                p1_ref[mat, :, row_sl] = tot[NB:] + tot[:NB]
            else:
                acc1[...] += p1

    if products:
        acc1[...] = jnp.zeros_like(acc1)

    @pl.loop(0, ti)
    def _(tj):
        run(tj, False)

    run(ti, True)

    if update:

        @pl.loop(ti + 1, 4)
        def _(tj):
            lo_ref[0, :, pl.ds(pl.multiple_of(tj * TC, TC), TC)] = jnp.zeros((TR, TC), F32)

    if not products:
        return

    @pl.when(ti == 3)
    def _():
        for u in range(8):
            ev = fold_rows(acc2[:, lane_tile(2 * u)])
            od = fold_rows(acc2[:, lane_tile(2 * u + 1)])
            p2_ref[mat, 0, :, lane_tile(u)], p2_ref[mat, 1, :, lane_tile(u)] = halves(low_half, ev, od)

    mine_part = yt.at[:, quarter(my_q := 2 * x + y)]
    part_y = yt.at[:, half_quarter(2 * x + 1 - y, 0)]
    part_x = yt.at[:, half_quarter(2 * (1 - x) + y, 1)]

    def helper_copies(q):
        part = remote(p2_ref.at[q], r_part, send.at[0], recv.at[0], partner)
        far = remote(p1_ref.at[q], r_p1, send.at[1], recv.at[1], y_cross)
        near = remote(p1_ref.at[q], r_own, send.at[1], recv.at[2], partner)
        return part, far, near

    def owner_copies(q):
        far = remote(p1_ref.at[q], r_p1, send.at[2], recv.at[1], y_nbr)
        over_x = remote(sbuf, r_p2, send.at[3], recv.at[3], x_nbr)
        g_x, g_y = [[remote(qbuf.at[:, span(h, QTR // 2)], yt.at[:, half_quarter(2 * x + y, h)], send.at[i + h], recv.at[i + h], dev) for h in (0, 1)] for i, dev in ((4, x_nbr), (6, y_nbr))]
        f_x = remote(part_y, part_y, send.at[8], recv.at[8], x_nbr)
        f_y = remote(part_x, part_x, send.at[9], recv.at[9], y_nbr)
        return far, over_x, g_x, g_y, f_x, f_y

    def help_out(q):
        part, far, near = helper_copies(q)
        part.start()
        pl.when(core != y)(far.start)
        pl.when(core == y)(near.start)

    def help_end(q):
        part, far, near = helper_copies(q)
        part.wait_send()
        far.wait_send()

    def stage_a(q):
        pl.when(core != y)(owner_copies(q)[0].start)

    def stage_b(q):
        part, _, near = helper_copies(q)
        part.wait_recv()
        sbuf[...] = p2_ref[q, 1 - x] + r_part[1 - x]
        owner_copies(q)[1].start()
        qbuf[...] = p2_ref[q, x] + r_part[x]

        @pl.when(core == y)
        def _():
            qbuf[...] += p1_ref[q]

        @pl.when(core != y)
        def _():
            near.wait_recv()
            qbuf[...] += r_own[...]

    def stage_c(q):
        far, over_x, g_x, g_y, _, _ = owner_copies(q)
        far.wait_recv()
        qbuf[...] += r_p1[...]
        over_x.wait()
        qbuf[...] += r_p2[...]
        for cp in (g_y[0], g_x[1], g_y[1], g_x[0]):
            cp.start()
        mine_part[...] = qbuf[...]

    def stage_d(q):
        _, _, g_x, g_y, f_x, f_y = owner_copies(q)
        g_y[0].wait_recv()
        f_x.start()
        g_x[1].wait_recv()
        f_y.start()

    def stage_e(q):
        far, _, g_x, g_y, f_x, f_y = owner_copies(q)
        pl.when(core != y)(far.wait_send)
        for cp in g_x + g_y:
            cp.wait_send()
        g_x[0].wait_recv()
        g_y[1].wait_recv()
        f_x.wait()
        f_y.wait()

    at = 4 * mat + ti
    last = at == 7
    for when, stage in enumerate((stage_a, stage_b, stage_c, stage_d, stage_e), start=3):
        pl.when((at == when) & (core == 0))(functools.partial(stage, 0))
    pl.when((at == 3) & (core == 1))(functools.partial(help_out, 0))

    @pl.when(last & (core == 0))
    def _():
        help_out(1)
        help_end(1)

    @pl.when(last & (core == 1))
    def _():
        help_end(0)
        for stage in (stage_a, stage_b, stage_c, stage_d, stage_e):
            stage(1)

    @pl.when(last)
    def _():
        yt_out[...] = yt[...]
        for ch in range(N_CH):
            vv_out[:, :, span(ch)] = vv[:, :, span(ch)]


def step_call(low, v_own, prev, v_rows=()):
    products = v_own is not None
    update = prev is not None
    strip = pl.BlockSpec((1, TR, COLS), lambda m, i: (m, i, 0))
    whole = pl.BlockSpec(memory_space=pltpu.VMEM)
    full, both = jax.ShapeDtypeStruct((NB, N), F32), jax.ShapeDtypeStruct((2, NB, N), F32)
    args, in_specs = [low], [strip]
    outs, out_specs, scratch = [], [], []
    if products:
        args += list(v_own)
        in_specs += [whole] * 2
    if update:
        args += list(prev)
        in_specs += [whole] * len(prev)
        outs.append(jax.ShapeDtypeStruct(low.shape, F32))
        out_specs.append(strip)
    if not products:
        args += v_rows
        in_specs += [pl.BlockSpec((1, NB, QTR), lambda m, i: (lax.rem(lax.axis_index('row') + m, 2), 0, lax.axis_index('row')))] * PANELS
        outs.append(jax.ShapeDtypeStruct((2, PANELS, QTR, NB), F32))
        out_specs.append(pl.BlockSpec((1, PANELS, QTR, NB), lambda m, i: (m, 0, 0, 0)))
    if products:
        outs += [full, both, jax.ShapeDtypeStruct((2, NB, LANE), F32)]
        out_specs += [whole] * 3
        qtr, two = pltpu.VMEM((NB, QTR), F32), pltpu.VMEM((2, NB, QTR), F32)
        scratch += [pltpu.VMEM((2, NB, N), F32), pltpu.VMEM((NB, N), F32)] + [pltpu.VMEM((TR, COLS), BF16), pltpu.VMEM((3 * NB, QTR), BF16), pltpu.VMEM((TR, TR), F32), pltpu.VMEM((3 * NB, COLS), F32)]
        scratch += [two, pltpu.VMEM((2, 2, NB, QTR), F32), two] + [qtr] * 5 + [pltpu.SemaphoreType.DMA((10,))] * 2 + [pltpu.SemaphoreType.DMA((2, 3))] * 2
    if update:
        if products:
            scratch.append(pltpu.VMEM((2, NB, N), F32))
        scratch += [pltpu.VMEM((QTR, 6 * LANE), BF16), pltpu.VMEM((6 * LANE, COLS), BF16)]
    return pl.pallas_call(
        functools.partial(step_kernel, update, products),
        out_shape=outs,
        grid=(2, 4),
        in_specs=in_specs,
        out_specs=out_specs,
        scratch_shapes=scratch,
        compiler_params=pltpu.CompilerParams(vmem_limit_bytes=VMEM_LIMIT, dimension_semantics=("arbitrary",) * 2, **(dict(collective_id=1 + update, has_side_effects=True) if products else {})),
        cost_estimate=pl.CostEstimate(flops=15_000_000_000, bytes_accessed=32_000_000, transcendentals=0),
        name="step",
    )(*args)


def solution(mesh):
    def per_device(lower_tri):
        n_mat, n_rblk, blk, n_cloc = lower_tri.shape
        n_rloc = n_rblk * blk
        my_row = lax.axis_index('row')
        core = lax.rem(my_row, 2)
        low = lower_tri.reshape(n_mat, n_rloc, n_cloc)
        slab = jnp.swapaxes(low[:, :, : 2 * NB], 1, 2).reshape(n_mat, 2, NB, n_rloc)
        pt = gather_call(slab[:, 0])
        pts, pt = rest_of_panels(slab, my_row, pt)
        small, vt = panel_call(0, pt)
        yt, v_both, t_pair = step_call(low, (vt, small), None)
        smalls, t_pairs, v_rows = [small], [t_pair], [v_both]
        for k in range(1, PANELS):
            wt, small, vt_new, *pts = panel_call(k, vt, yt, t_pair, *pts)
            low, yt, v_both, t_pair = step_call(low, (vt_new, small), (v_both, wt))
            smalls.append(small)
            t_pairs.append(t_pair)
            v_rows.append(v_both)
            vt = vt_new
        (wt,) = panel_call(PANELS, vt, yt, t_pair)
        w_both, both = swap_call(wt, smalls, t_pairs)
        low, v_out = step_call(low, None, (v_both, w_both), v_rows)
        both = jnp.where(core == 0, both, both[::-1])
        d_mat = jnp.swapaxes(both[:, :, 0, :, :NB], 2, 3)
        r_mat = jnp.concatenate([both[:, :-1, 1, :, :NB], both[:, -1:, 1, :, NB:]], axis=1)
        band = jnp.stack([d_mat, jnp.swapaxes(r_mat, 2, 3)], axis=2)
        return low.reshape(lower_tri.shape), band, v_out.reshape(n_mat, PANELS, n_rblk, blk, blk), both[:, :, 2, :, :NB]

    spec_low = P('sys', 'row', None, 'col')
    return jax.shard_map(per_device, mesh=mesh, in_specs=(spec_low,), out_specs=(spec_low, P('sys'), P('sys', None, 'row', None, None), P('sys')), check_vma=False)
```

```python
import functools

import jax
import jax.numpy as jnp
from jax import lax
from jax.experimental import pallas as pl
from jax.experimental.pallas import tpu as pltpu
from jax.sharding import PartitionSpec as P

PANELS = 4
NB = 64
N = 4096
QTR = 1024
LANE = 128
COLS = 2048
N_CH = N // LANE
TR, TC = 256, 512
GATHER_PARTS = 8
TILE = (8, LANE)
WIDE = (NB, LANE)
F32 = jnp.float32
BF16 = jnp.bfloat16
MESH = pl.DeviceIdType.MESH
VMEM_LIMIT = 60 * 1024 * 1024


def span(i, width=LANE):
    return slice(i * width, (i + 1) * width)


def lane_of(shape):
    return lax.broadcasted_iota(jnp.int32, shape, 1)


def lane_tile(i):
    return pl.ds(pl.multiple_of(i * LANE, LANE), LANE)


def quarter(row):
    return pl.ds(pl.multiple_of(row * QTR, QTR), QTR)


def half_quarter(row, half):
    width = QTR // 2
    return pl.ds(pl.multiple_of(row * QTR + half * width, width), width)


def sum_of(terms):
    return functools.reduce(lambda a, b: a + b, terms)


def halves(low_half, a, b):
    return jnp.where(low_half, a, pltpu.roll(b, NB, 1)), jnp.where(low_half, pltpu.roll(a, NB, 1), b)


def split3(a):
    hi = a.astype(BF16)
    rest = a - hi.astype(F32)
    mid = rest.astype(BF16)
    low = (rest - mid.astype(F32)).astype(BF16)
    return hi, mid, low


def bdot(a, b, ca=1, cb=0):
    return lax.dot_general(a, b, (((ca,), (cb,)), ((), ())), preferred_element_type=F32)


def fold_rows(x):
    n = x.shape[0] // 3
    return x[2 * n :] + x[n : 2 * n] + x[:n]


def mm(a, b, cb=0):
    lhs = jnp.concatenate(split3(a))
    b1, b2, b3 = split3(b)
    return fold_rows(bdot(lhs, b3, cb=cb) + bdot(lhs, b2, cb=cb) + bdot(lhs, b1, cb=cb))


def gram(a_ref, b_ref, mask=None):
    acc = None
    for t in range(N // 512):
        sl = span(t, 512)
        lhs = jnp.concatenate(split3(a_ref[:, sl]))
        rhs = jnp.concatenate(split3(b_ref[:, sl]))
        part = bdot(lhs, rhs, 1, 1)
        acc = part if acc is None else acc + part
    acc = fold_rows(acc)
    return sum_of([acc[:, span(q, NB)] for q in reversed(range(3))])


def bcast(v):
    return jnp.broadcast_to(v, TILE)


def qr_step(a_ref, xcur, xnext, stats, pc, pl0, gi, s, last_of_pair, accs):
    beta_ref, inv_ref, tau_ref = stats
    lane = lane_of(TILE)
    sub = lax.broadcasted_iota(jnp.int32, (8, 1), 0)
    n_g = 8 - gi
    j = gi * 8 + s
    p = pl0 + j
    rows = [span(gi + g, 8) for g in range(n_g)]
    dots = [jnp.sum(acc, axis=1, keepdims=True) for acc in accs]
    pvs = [jnp.sum(jnp.where(lane == p, a_ref[pc, r, :], 0.0), axis=1, keepdims=True) for r in rows]
    sigma = jnp.sum(jnp.where(sub == s, dots[0], 0.0), axis=0, keepdims=True)
    alpha = jnp.sum(jnp.where(sub == s, pvs[0], 0.0), axis=0, keepdims=True)
    sq = alpha * alpha + sigma
    inv_norm = lax.rsqrt(sq)
    norm = jnp.sqrt(sq)
    pos = alpha >= 0
    beta = jnp.where(pos, -norm, norm)
    ninvb = jnp.where(pos, inv_norm, -inv_norm)
    denom = alpha - beta
    inv_den = 1.0 / denom
    tau = denom * ninvb
    cs = [(pv + d * inv_den) * ninvb for pv, d in zip(pvs, dots)]
    cs[0] = jnp.where(sub > s, cs[0], 0.0)
    beta_ref[pl.ds(j, 1), :] = jnp.broadcast_to(beta, (1, 128))
    inv_ref[pl.ds(j, 1), :] = jnp.broadcast_to(inv_den, (1, 128))
    tau_ref[pl.ds(j, 1), :] = jnp.broadcast_to(tau, (1, 128))
    c_next = jnp.sum(jnp.where(sub == s + 1, cs[0], 0.0), axis=0, keepdims=True)
    if last_of_pair and n_g > 1:
        c_next = c_next + jnp.where(s == 7, cs[1][0:1], 0.0)
    jn = jnp.minimum(j + 1, NB - 1)
    c_next = bcast(c_next)
    den_b = bcast(denom)
    for ch in range(N_CH):
        xt = xcur[ch]
        if ch == pc:
            xt = jnp.where(lane == p, den_b, xt)
        xn = a_ref[ch, pl.ds(jn, 8, stride=0), :] - c_next * xt
        if ch == pc:
            xn = jnp.where(lane > p + 1, xn, 0.0)
        xnext[ch] = xn
    cs = [bcast(c) for c in cs]
    out = [jnp.zeros(TILE, F32) for _ in range(n_g)]
    for ch in range(N_CH):
        xt = xcur[ch]
        if ch == pc:
            xt = jnp.where(lane == p, den_b, xt)
        xn = xnext[ch]
        for g in range(n_g):
            a = a_ref[ch, rows[g], :] - cs[g] * xt
            a_ref[ch, rows[g], :] = a
            out[g] = out[g] + a * xn
    return tuple(out)


def qr_panel(a_ref, x_refs, stats, pc, pl0):
    lane = lane_of(TILE)
    accs = [jnp.zeros(TILE, F32) for _ in range(8)]
    for ch in range(N_CH):
        x = bcast(a_ref[ch, 0:1, :])
        if ch == pc:
            x = jnp.where(lane > pl0, x, 0.0)
        x_refs[0][ch] = x
        for g in range(8):
            accs[g] = accs[g] + a_ref[ch, span(g, 8), :] * x
    accs = tuple(accs)
    for gi in range(8):

        def pair(h, accs, gi=gi):
            for par in range(2):
                accs = qr_step(a_ref, x_refs[par], x_refs[1 - par], stats, pc, pl0, gi, h * 2 + par, par == 1, accs)
            return accs

        accs = lax.fori_loop(0, 4, pair, accs)[1:]


def finish_panel(a_ref, stats, vt_ref, rt_ref, pc, pl0):
    beta_ref, inv_ref, tau_ref = stats
    lane = lane_of(TILE)
    sub = lax.broadcasted_iota(jnp.int32, TILE, 0)
    for g in range(8):
        rows = span(g, 8)
        inv = inv_ref[rows, :]
        for ch in range(N_CH):
            sl = span(ch)
            a = a_ref[ch, rows, :]
            v = a * inv
            if ch == pc:
                rel = lane - pl0 - (g * 8 + sub)
                rt_ref[rows, :] = jnp.where(rel < 0, a, jnp.where(rel == 0, beta_ref[rows, :], 0.0))
                v = jnp.where(rel > 0, v, jnp.where(rel == 0, 1.0, 0.0))
            vt_ref[rows, sl] = v


def build_tri(gram_mat, tau_col):
    row = lax.broadcasted_iota(jnp.int32, (NB, NB), 0)
    col = lane_of((NB, NB))
    t = jnp.where(row == col, tau_col, 0.0)
    for lg in range(6):
        rb = lax.shift_right_logical(row, lg)
        cb = lax.shift_right_logical(col, lg)
        u = jnp.where((cb == rb + 1) & (lax.rem(rb, 2) == 0), gram_mat, 0.0)
        t = t - mm(mm(t, u), t)
    return t


def panel_kernel(step, *refs):
    refs = list(refs)
    n_rem = PANELS - step
    if step > 0:
        vt_ref, yt_ref, t_pair = refs[:3]
        refs = refs[3:]
    if step == 1:
        pieces, refs = refs[:8], refs[8:]
    elif n_rem:
        pt_ref = refs.pop(0)
    if step > 0:
        wt_ref = refs.pop(0)
    if n_rem:
        small_ref, vn_ref = refs[:2]
        refs = refs[2:]
        if step > 0 and n_rem > 1:
            rem_ref = refs.pop(0)
        a_ref, xa, xb, beta_ref, inv_ref, tau_ref = refs
    lane64 = lane_of(WIDE)
    row64 = lax.broadcasted_iota(jnp.int32, WIDE, 0)
    if step > 0:
        for g in range(step):
            sl = span(8 * g)
            yt_ref[:, sl] = jnp.where(lane64 < NB, 0.0, yt_ref[:, sl])
        s_mat = gram(vt_ref, yt_ref)
        t_mat, t_tr = t_pair[0, :, :NB], t_pair[1, :, :NB]
        m_mat = mm(mm(t_tr, s_mat, 1), t_mat)
        lhs = jnp.concatenate([t_tr, -0.5 * m_mat], axis=1)
        for t in range(N // 512):
            sl = span(t, 512)
            wt_ref[:, sl] = mm(lhs, jnp.concatenate([yt_ref[:, sl], vt_ref[:, sl]]))
    if not n_rem:
        return
    if step == 1:
        x, core, y = place()
        for dx in range(2):
            for f in range(2):
                row = 2 * (1 - x if dx else x) + (1 - core if f else core)
                lanes = pl.ds(pl.multiple_of(row * QTR, QTR), QTR)
                here, there = 2 * dx + f, 4 + 2 * dx + f
                first = jnp.where(y == 1, pieces[here][0], pieces[there][0])
                for ch in range(8):
                    a_ref[row * 8 + ch] = first[:, span(ch)]
                one, two = pieces[here][1], pieces[there][1]
                rem_ref[0, :, lanes] = jnp.where(y == 0, one, two)
                rem_ref[1, :, lanes] = jnp.where(y == 1, one, two)
    if step > 0:
        lefts = []
        for q in range(step, PANELS):
            sl = span(8 * q)
            wc = wt_ref[:, sl].T[:NB]
            vc = vt_ref[:, sl].T[:NB]
            lefts.append(jnp.concatenate([wc, vc], axis=1))
        lhs = jnp.concatenate(lefts)
        for t in range(N // 256):
            sl = span(t, TR)
            upd = mm(lhs, jnp.concatenate([vt_ref[:, sl], wt_ref[:, sl]]))
            for h in range(2):
                old = a_ref[2 * t + h] if step == 1 else pt_ref[0, :, span(2 * t + h)]
                a_ref[2 * t + h] = old - upd[:NB, span(h)]
            for q in range(1, n_rem):
                old = rem_ref[q - 1, :, sl] if step == 1 else pt_ref[q, :, sl]
                rem_ref[q - 1, :, sl] = old - upd[span(q, NB)]
    else:
        for ch in range(N_CH):
            a_ref[ch] = pt_ref[:, span(ch)]
    small_ref[0] = jnp.where((lane64 >= row64) & (lane64 < NB), a_ref[step * 8], 0.0)
    for g in range(step + 1):
        a_ref[g * 8] = jnp.where(lane64 < NB, 0.0, a_ref[g * 8])
    pc = ((step + 1) % PANELS) * (QTR // LANE)
    pl0 = NB * ((step + 1) // PANELS)
    stats = (beta_ref, inv_ref, tau_ref)
    qr_panel(a_ref, (xa, xb), stats, pc, pl0)
    finish_panel(a_ref, stats, vn_ref, small_ref.at[1], pc, pl0)
    small_ref[2] = tau_ref[...]


def panel_call(step, *args):
    n_rem = PANELS - step
    outs = []
    full = jax.ShapeDtypeStruct((NB, N), F32)
    scratch = []
    if step > 0:
        outs.append(full)
    if n_rem:
        outs += [jax.ShapeDtypeStruct((3, NB, LANE), F32), full]
        if step > 0 and n_rem > 1:
            outs.append(jax.ShapeDtypeStruct((n_rem - 1, NB, N), F32))
        scratch = [pltpu.VMEM((N_CH, NB, 128), F32), pltpu.VMEM((N_CH, 8, 128), F32), pltpu.VMEM((N_CH, 8, 128), F32)] + [pltpu.VMEM(WIDE, F32)] * 3
    vspec = pl.BlockSpec(memory_space=pltpu.VMEM)
    return pl.pallas_call(
        functools.partial(panel_kernel, step),
        out_shape=outs,
        in_specs=[vspec] * len(args),
        out_specs=[vspec] * len(outs),
        scratch_shapes=scratch,
        compiler_params=pltpu.CompilerParams(vmem_limit_bytes=VMEM_LIMIT),
        cost_estimate=pl.CostEstimate(flops=20_000_000_000, bytes_accessed=8_000_000, transcendentals=0),
        name=f"panel{step}",
    )(*args)


def barrier(neighbours):
    sem = pltpu.get_barrier_semaphore()
    for dev in neighbours:
        pl.semaphore_signal(sem, inc=1, device_id=dev, device_id_type=MESH)
    pl.semaphore_wait(sem, len(neighbours))


def remote(src, dst, send, recv, dev):
    return pltpu.make_async_remote_copy(src_ref=src, dst_ref=dst, send_sem=send, recv_sem=recv, device_id=dev, device_id_type=MESH)


def place():
    my_row = lax.axis_index('row')
    my_col = lax.axis_index('col')
    return lax.div(my_row, 2), lax.rem(my_row, 2), my_col


def device(x, core, y):
    return {'row': 2 * x + core, 'col': y}


def gather_kernel(slab_ref, pt_ref, send, recv, fwd_send, fwd_recv):
    x, core, y = place()
    other = 1 - core
    barrier([device(x, other, y), device(1 - x, core, y), device(1 - x, other, y), device(x, core, 1 - y), device(x, other, 1 - y)])
    n_part = GATHER_PARTS
    width = QTR // n_part

    def lanes(row, part=None):
        if part is None:
            return pl.ds(pl.multiple_of(row * QTR, QTR), QTR)
        return pl.ds(pl.multiple_of(row * QTR + part * width, width), width)

    def push(to_core, dev, part, s_sem, r_sem):
        return remote(slab_ref.at[to_core, :, part * width : (part + 1) * width], pt_ref.at[:, lanes(2 * x + core, part)], s_sem, r_sem, dev)

    def onward(row, part, idx):
        ref = pt_ref.at[:, lanes(row, part)]
        return remote(ref, ref, fwd_send.at[idx, part], fwd_recv.at[idx, part], device(1 - x, core, y))

    my_row = 2 * x + core
    for part in range(n_part):
        to_y = [push(core, device(x, core, 1 - y), part, send.at[0, part], recv.at[0, part]), push(other, device(x, other, 1 - y), part, send.at[1, part], recv.at[1, part])]
        to_x = [push(core, device(1 - x, core, y), part, send.at[2, part], recv.at[2, part]), push(other, device(1 - x, other, y), part, send.at[3, part], recv.at[3, part])]
        to_p = push(other, device(x, other, y), part, send.at[4, part], recv.at[4, part])

        @pl.when(y == 0)
        def _():
            for cp in to_y + to_x + [to_p]:
                cp.start()

    @pl.when(y == 0)
    def _():
        pt_ref[:, lanes(my_row)] = slab_ref[core]
        for part in range(n_part):
            for idx, (tc, dev) in enumerate([(core, device(x, core, 1)), (other, device(x, other, 1)), (core, device(1 - x, core, 0)), (other, device(1 - x, other, 0)), (other, device(x, other, 0))]):
                cp = push(tc, dev, part, send.at[idx, part], recv.at[idx, part])
                cp.wait_send()
                if idx >= 2:
                    cp.wait_recv()

    @pl.when(y == 1)
    def _():
        for part in range(n_part):
            for idx, row in enumerate([my_row, 2 * x + other]):
                push(core, device(x, core, 0), part, send.at[idx, part], recv.at[idx, part]).wait_recv()
                onward(row, part, idx).start()
        for part in range(n_part):
            for idx in range(2):
                onward(my_row, part, idx).wait()


def gather_call(slab):
    vspec = pl.BlockSpec(memory_space=pltpu.VMEM)
    return pl.pallas_call(
        gather_kernel,
        out_shape=jax.ShapeDtypeStruct((NB, N), F32),
        in_specs=[vspec],
        out_specs=vspec,
        scratch_shapes=[*([pltpu.SemaphoreType.DMA((5, GATHER_PARTS))] * 2), *([pltpu.SemaphoreType.DMA((2, GATHER_PARTS))] * 2)],
        compiler_params=pltpu.CompilerParams(collective_id=0, has_side_effects=True, vmem_limit_bytes=VMEM_LIMIT),
        name="gather",
    )(slab)


def rest_of_panels(slab, my_row, pt):
    core = lax.rem(my_row, 2)
    own = lax.dynamic_index_in_dim(slab, core, 0, keepdims=False)
    cross = lax.dynamic_index_in_dim(slab, 1 - core, 0, keepdims=False)
    own, cross, pt = lax.optimization_barrier((own, cross, pt))

    def pairs(dx, dy, f):
        flip = 4 * dy + 2 * dx + f
        return [(d, d ^ flip) for d in range(8)]

    pieces = []
    for dy in range(2):
        for dx in range(2):
            for f in range(2):
                payload = cross if f else own
                pieces.append(payload if (dx, dy, f) == (0, 0, 0) else lax.ppermute(payload, ('col', 'row'), pairs(dx, dy, f)))
    return pieces, pt


def needed(x, y):
    return [quarter(row) for row in (y, 2 + y, 2 * x + 1 - y)]


def swap_kernel(w_ref, *refs):
    smalls, refs = refs[:PANELS], refs[PANELS:]
    t_pairs, (w_out, pack_out, send, recv) = refs[:PANELS], refs[PANELS:]
    x, core, y = place()
    partner = device(x, 1 - core, y)
    barrier([partner])
    moves = [(w_ref.at[:, sl], w_out.at[1, :, sl]) for sl in needed(x, y)]
    for k in range(PANELS):
        moves.append((smalls[k].at[:2], pack_out.at[1, k, :2]))
        moves.append((t_pairs[k].at[0], pack_out.at[1, k, 2]))
    copies = [remote(src, dst, send.at[i], recv.at[i], partner) for i, (src, dst) in enumerate(moves)]
    for cp in copies:
        cp.start()
    w_out[0] = w_ref[...]
    for k in range(PANELS):
        pack_out[0, k, :2] = smalls[k][:2]
        pack_out[0, k, 2] = t_pairs[k][0]
    for cp in copies:
        cp.wait()


def swap_call(w, smalls, t_pairs):
    whole = pl.BlockSpec(memory_space=pltpu.VMEM)
    return pl.pallas_call(
        swap_kernel,
        out_shape=[jax.ShapeDtypeStruct((2, NB, N), F32), jax.ShapeDtypeStruct((2, PANELS, 3, NB, LANE), F32)],
        in_specs=[whole] * (1 + 2 * PANELS),
        out_specs=[whole] * 2,
        scratch_shapes=[pltpu.SemaphoreType.DMA((3 + 2 * PANELS,))] * 2,
        compiler_params=pltpu.CompilerParams(collective_id=5, has_side_effects=True, vmem_limit_bytes=VMEM_LIMIT),
        name="swap",
    )(w, *smalls, *t_pairs)


def step_kernel(update, products, *refs):
    refs = list(refs)
    take = lambda n: [refs.pop(0) for _ in range(n)]
    (l_ref,) = take(1)
    if products:
        va, small_ref = take(2)
    if update:
        uu, ww = take(2)
        wa = ww
        if not products:
            v_rows = take(PANELS)
        (lo_ref,) = take(1)
        if not products:
            (vo_ref,) = take(1)
    if products:
        yt_out, vv_out, t_pair = take(3)
        vv, yt, vc3, vr3, acc1, acc2, p1_ref, p2_ref = take(8)
        r_part, r_own, r_p1, r_p2, sbuf, qbuf, send, recv = take(8)
        v_send, v_recv = take(2)
    if update:
        if products:
            (ww,) = take(1)
        left6, right6 = take(2)
    mat = pl.program_id(0)
    ti = pl.program_id(1)
    x, core, y = place()
    my_row = 2 * x + core
    other = 1 - core
    partner = device(x, other, y)
    x_nbr = device(1 - x, core, y)
    y_nbr = device(x, core, 1 - y)
    y_cross = device(x, other, 1 - y)
    slot = lax.rem(core + mat, 2)
    low_half = lane_of(WIDE) < NB

    if products:
        swaps = [(va, vv)] + ([(wa, ww)] if update else [])
        swaps = [remote(src.at[:, sl], dst.at[1, :, sl], v_send.at[i, q], v_recv.at[i, q], partner) for i, (src, dst) in enumerate(swaps) for q, sl in enumerate(needed(x, y))]

        @pl.when((mat == 0) & (ti == 0))
        def _():
            barrier([partner, x_nbr, y_nbr, y_cross])
            for cp in swaps:
                cp.start()
            vv[0] = va[...]
            if update:
                ww[0] = wa[...]
            t_mat = build_tri(gram(va, va), small_ref[2, :, :NB])
            t_pair[0] = jnp.concatenate([t_mat, jnp.zeros_like(t_mat)], axis=1)
            t_pair[1] = jnp.concatenate([t_pair[0], t_pair[0]]).T[:NB]

        @pl.when((mat == other) & (ti == 0))
        def _():
            for cp in swaps:
                cp.wait()

    def pick(ref, base, ch):
        return ref[slot, :, lane_tile(base * 8 + ch)]

    def col_chunks(ref, u):
        qa = pick(ref, y, u)
        qb = pick(ref, y + 2, u)
        return halves(low_half, qa, qb)

    @pl.when(ti == 0)
    def _():
        if not products:
            for k in range(PANELS):
                for u in range(8):
                    vo_ref[0, k, span(u), :] = v_rows[k][0, :, span(u)].T

        if products:
            acc2[...] = jnp.zeros_like(acc2)
            vc3[3 * NB :, :] = jnp.zeros((NB, COLS), BF16)
            for u in range(8):
                for h, part in enumerate(col_chunks(vv, u)):
                    for q, piece in enumerate(split3(part)):
                        vc3[span(q, NB), lane_tile(2 * u + h)] = piece
                for q, piece in enumerate(split3(pick(vv, my_row, u))):
                    vr3[span(q, NB), lane_tile(u)] = piece

        if update:
            for u in range(8):
                vcs = col_chunks(uu, u)
                wcs = col_chunks(ww, u)
                for h in range(2):
                    r1, r2, r3 = split3(jnp.concatenate([wcs[h], vcs[h]]))
                    for q, piece in enumerate((r3, r2, r1, r2, r1, r1)):
                        right6[span(q), lane_tile(2 * u + h)] = piece
                left = jnp.concatenate([pick(uu, my_row, u), pick(ww, my_row, u)]).T
                a1, a2, a3 = split3(left)
                for q, piece in enumerate((a1, a2, a3, a1, a2, a1)):
                    left6[lane_tile(u), span(q)] = piece

    row_sl = pl.ds(pl.multiple_of(ti * TR, TR), TR)

    def run(tj, diag):
        col_sl = pl.ds(pl.multiple_of(tj * TC, TC), TC)
        tile = l_ref[0, :, col_sl]
        if diag or not products:
            ri = lax.broadcasted_iota(jnp.int32, (TR, TC), 0) + ti * TR
            ci = lane_of((TR, TC)) + tj * TC
            rg = (lax.div(ri, NB) * 4 + my_row) * NB + lax.rem(ri, NB)
            cg = (lax.div(ci, NB) * 2 + y) * NB + lax.rem(ci, NB)
        if update:
            upd = bdot(left6[row_sl, :], right6[:, col_sl])
            tile = tile - (jnp.where(rg >= cg, upd, 0.0) if diag else upd)
            if not products:
                done = PANELS * NB
                tile = jnp.where((rg >= done) & (cg >= done), tile, 0.0)
            lo_ref[0, :, col_sl] = tile
        if products:
            parts = split3(tile)
            vcols = vc3[:, col_sl]
            vrows = vr3[:, row_sl]
            part1, part2, part3 = [bdot(vrows[: (3 - q) * NB], part) for q, part in enumerate(parts)]
            top, mid = span(0, NB), span(1, NB)
            acc2[top, col_sl] += part3 + part2[top] + part1[top]
            acc2[mid, col_sl] += part2[mid] + part1[mid]
            acc2[2 * NB :, col_sl] += part1[2 * NB :]
            if diag:
                parts = [jnp.where(rg == cg, jnp.zeros_like(part), part) for part in parts]
            p1 = fold_rows(bdot(jnp.concatenate(parts), vcols, 1, 1))
            if diag:
                tot = acc1[...] + p1
                tot = (tot[:, :LANE] + tot[:, LANE:]).T
                p1_ref[mat, :, row_sl] = tot[NB:] + tot[:NB]
            else:
                acc1[...] += p1

    if products:
        acc1[...] = jnp.zeros_like(acc1)

    @pl.loop(0, ti)
    def _(tj):
        run(tj, False)

    run(ti, True)

    if update:

        @pl.loop(ti + 1, 4)
        def _(tj):
            lo_ref[0, :, pl.ds(pl.multiple_of(tj * TC, TC), TC)] = jnp.zeros((TR, TC), F32)

    if not products:
        return

    @pl.when(ti == 3)
    def _():
        for u in range(8):
            ev = fold_rows(acc2[:, lane_tile(2 * u)])
            od = fold_rows(acc2[:, lane_tile(2 * u + 1)])
            p2_ref[mat, 0, :, lane_tile(u)], p2_ref[mat, 1, :, lane_tile(u)] = halves(low_half, ev, od)

    mine_part = yt.at[:, quarter(my_q := 2 * x + y)]
    part_y = yt.at[:, half_quarter(2 * x + 1 - y, 0)]
    part_x = yt.at[:, half_quarter(2 * (1 - x) + y, 1)]

    def helper_copies(q):
        part = remote(p2_ref.at[q], r_part, send.at[0], recv.at[0], partner)
        far = remote(p1_ref.at[q], r_p1, send.at[1], recv.at[1], y_cross)
        near = remote(p1_ref.at[q], r_own, send.at[1], recv.at[2], partner)
        return part, far, near

    def owner_copies(q):
        far = remote(p1_ref.at[q], r_p1, send.at[2], recv.at[1], y_nbr)
        over_x = remote(sbuf, r_p2, send.at[3], recv.at[3], x_nbr)
        g_x, g_y = [[remote(qbuf.at[:, span(h, QTR // 2)], yt.at[:, half_quarter(2 * x + y, h)], send.at[i + h], recv.at[i + h], dev) for h in (0, 1)] for i, dev in ((4, x_nbr), (6, y_nbr))]
        f_x = remote(part_y, part_y, send.at[8], recv.at[8], x_nbr)
        f_y = remote(part_x, part_x, send.at[9], recv.at[9], y_nbr)
        return far, over_x, g_x, g_y, f_x, f_y

    def help_out(q):
        part, far, near = helper_copies(q)
        part.start()
        pl.when(core != y)(far.start)
        pl.when(core == y)(near.start)

    def help_end(q):
        part, far, near = helper_copies(q)
        part.wait_send()
        far.wait_send()

    def stage_a(q):
        pl.when(core != y)(owner_copies(q)[0].start)

    def stage_b(q):
        part, _, near = helper_copies(q)
        part.wait_recv()
        sbuf[...] = p2_ref[q, 1 - x] + r_part[1 - x]
        owner_copies(q)[1].start()
        qbuf[...] = p2_ref[q, x] + r_part[x]

        @pl.when(core == y)
        def _():
            qbuf[...] += p1_ref[q]

        @pl.when(core != y)
        def _():
            near.wait_recv()
            qbuf[...] += r_own[...]

    def stage_c(q):
        far, over_x, g_x, g_y, _, _ = owner_copies(q)
        far.wait_recv()
        qbuf[...] += r_p1[...]
        over_x.wait()
        qbuf[...] += r_p2[...]
        for cp in (g_y[0], g_x[1], g_y[1], g_x[0]):
            cp.start()
        mine_part[...] = qbuf[...]

    def stage_d(q):
        _, _, g_x, g_y, f_x, f_y = owner_copies(q)
        g_y[0].wait_recv()
        f_x.start()
        g_x[1].wait_recv()
        f_y.start()

    def stage_e(q):
        far, _, g_x, g_y, f_x, f_y = owner_copies(q)
        pl.when(core != y)(far.wait_send)
        for cp in g_x + g_y:
            cp.wait_send()
        g_x[0].wait_recv()
        g_y[1].wait_recv()
        f_x.wait()
        f_y.wait()

    at = 4 * mat + ti
    last = at == 7
    for when, stage in ((3, stage_a), (5, stage_b), (6, stage_c)):
        pl.when((at == when) & (core == 0))(functools.partial(stage, 0))
    pl.when((at == 3) & (core == 1))(functools.partial(help_out, 0))

    @pl.when(last & (core == 0))
    def _():
        help_out(1)
        stage_d(0)
        stage_e(0)
        help_end(1)

    @pl.when(last & (core == 1))
    def _():
        help_end(0)
        for stage in (stage_a, stage_b, stage_c, stage_d, stage_e):
            stage(1)

    @pl.when(last)
    def _():
        yt_out[...] = yt[...]
        for ch in range(N_CH):
            vv_out[:, :, span(ch)] = vv[:, :, span(ch)]


def step_call(low, v_own, prev, v_rows=()):
    products = v_own is not None
    update = prev is not None
    strip = pl.BlockSpec((1, TR, COLS), lambda m, i: (m, i, 0))
    whole = pl.BlockSpec(memory_space=pltpu.VMEM)
    full, both = jax.ShapeDtypeStruct((NB, N), F32), jax.ShapeDtypeStruct((2, NB, N), F32)
    args, in_specs = [low], [strip]
    outs, out_specs, scratch = [], [], []
    if products:
        args += list(v_own)
        in_specs += [whole] * 2
    if update:
        args += list(prev)
        in_specs += [whole] * len(prev)
        outs.append(jax.ShapeDtypeStruct(low.shape, F32))
        out_specs.append(strip)
    if not products:
        args += v_rows
        in_specs += [pl.BlockSpec((1, NB, QTR), lambda m, i: (lax.rem(lax.axis_index('row') + m, 2), 0, lax.axis_index('row')))] * PANELS
        outs.append(jax.ShapeDtypeStruct((2, PANELS, QTR, NB), F32))
        out_specs.append(pl.BlockSpec((1, PANELS, QTR, NB), lambda m, i: (m, 0, 0, 0)))
    if products:
        outs += [full, both, jax.ShapeDtypeStruct((2, NB, LANE), F32)]
        out_specs += [whole] * 3
        qtr, two = pltpu.VMEM((NB, QTR), F32), pltpu.VMEM((2, NB, QTR), F32)
        scratch += [pltpu.VMEM((2, NB, N), F32), pltpu.VMEM((NB, N), F32)] + [pltpu.VMEM((TR, COLS), BF16), pltpu.VMEM((3 * NB, QTR), BF16), pltpu.VMEM((TR, TR), F32), pltpu.VMEM((3 * NB, COLS), F32)]
        scratch += [two, pltpu.VMEM((2, 2, NB, QTR), F32), two] + [qtr] * 5 + [pltpu.SemaphoreType.DMA((10,))] * 2 + [pltpu.SemaphoreType.DMA((2, 3))] * 2
    if update:
        if products:
            scratch.append(pltpu.VMEM((2, NB, N), F32))
        scratch += [pltpu.VMEM((QTR, 6 * LANE), BF16), pltpu.VMEM((6 * LANE, COLS), BF16)]
    return pl.pallas_call(
        functools.partial(step_kernel, update, products),
        out_shape=outs,
        grid=(2, 4),
        in_specs=in_specs,
        out_specs=out_specs,
        scratch_shapes=scratch,
        compiler_params=pltpu.CompilerParams(vmem_limit_bytes=VMEM_LIMIT, dimension_semantics=("arbitrary",) * 2, **(dict(collective_id=1 + update, has_side_effects=True) if products else {})),
        cost_estimate=pl.CostEstimate(flops=15_000_000_000, bytes_accessed=32_000_000, transcendentals=0),
        name="step",
    )(*args)


def solution(mesh):
    def per_device(lower_tri):
        n_mat, n_rblk, blk, n_cloc = lower_tri.shape
        n_rloc = n_rblk * blk
        my_row = lax.axis_index('row')
        core = lax.rem(my_row, 2)
        low = lower_tri.reshape(n_mat, n_rloc, n_cloc)
        slab = jnp.swapaxes(low[:, :, : 2 * NB], 1, 2).reshape(n_mat, 2, NB, n_rloc)
        pt = gather_call(slab[:, 0])
        pts, pt = rest_of_panels(slab, my_row, pt)
        small, vt = panel_call(0, pt)
        yt, v_both, t_pair = step_call(low, (vt, small), None)
        smalls, t_pairs, v_rows = [small], [t_pair], [v_both]
        for k in range(1, PANELS):
            wt, small, vt_new, *pts = panel_call(k, vt, yt, t_pair, *pts)
            low, yt, v_both, t_pair = step_call(low, (vt_new, small), (v_both, wt))
            smalls.append(small)
            t_pairs.append(t_pair)
            v_rows.append(v_both)
            vt = vt_new
        (wt,) = panel_call(PANELS, vt, yt, t_pair)
        w_both, both = swap_call(wt, smalls, t_pairs)
        low, v_out = step_call(low, None, (v_both, w_both), v_rows)
        both = jnp.where(core == 0, both, both[::-1])
        d_mat = jnp.swapaxes(both[:, :, 0, :, :NB], 2, 3)
        r_mat = jnp.concatenate([both[:, :-1, 1, :, :NB], both[:, -1:, 1, :, NB:]], axis=1)
        band = jnp.stack([d_mat, jnp.swapaxes(r_mat, 2, 3)], axis=2)
        return low.reshape(lower_tri.shape), band, v_out.reshape(n_mat, PANELS, n_rblk, blk, blk), both[:, :, 2, :, :NB]

    spec_low = P('sys', 'row', None, 'col')
    return jax.shard_map(per_device, mesh=mesh, in_specs=(spec_low,), out_specs=(spec_low, P('sys'), P('sys', None, 'row', None, None), P('sys')), check_vma=False)
```

```python
import functools

import jax
import jax.numpy as jnp
from jax import lax
from jax.experimental import pallas as pl
from jax.experimental.pallas import tpu as pltpu
from jax.sharding import PartitionSpec as P

PANELS = 4
NB = 64
N = 4096
QTR = 1024
HALF = 512
LANE = 128
COLS = 2048
N_CH = N // LANE
TR, TC = 256, 512
GATHER_PARTS = 8
TILE = (8, LANE)
WIDE = (NB, LANE)
F32 = jnp.float32
BF16 = jnp.bfloat16
MESH = pl.DeviceIdType.MESH
VMEM_LIMIT = 60 * 1024 * 1024


def span(i, width=LANE):
    return slice(i * width, (i + 1) * width)


def lane_of(shape):
    return lax.broadcasted_iota(jnp.int32, shape, 1)


def lane_tile(i):
    return pl.ds(pl.multiple_of(i * LANE, LANE), LANE)


def quarter(row):
    return pl.ds(pl.multiple_of(row * QTR, QTR), QTR)


def half_quarter(row, half):
    return pl.ds(pl.multiple_of(row * QTR + half * HALF, HALF), HALF)


def sum_of(terms):
    return functools.reduce(lambda a, b: a + b, terms)


def halves(low_half, a, b):
    return jnp.where(low_half, a, pltpu.roll(b, NB, 1)), jnp.where(low_half, pltpu.roll(a, NB, 1), b)


def split3(a):
    hi = a.astype(BF16)
    rest = a - hi.astype(F32)
    mid = rest.astype(BF16)
    low = (rest - mid.astype(F32)).astype(BF16)
    return hi, mid, low


def bdot(a, b, ca=1, cb=0):
    return lax.dot_general(a, b, (((ca,), (cb,)), ((), ())), preferred_element_type=F32)


def fold_rows(x):
    n = x.shape[0] // 3
    return x[2 * n :] + x[n : 2 * n] + x[:n]


def mm(a, b, cb=0):
    lhs = jnp.concatenate(split3(a))
    b1, b2, b3 = split3(b)
    return fold_rows(bdot(lhs, b3, cb=cb) + bdot(lhs, b2, cb=cb) + bdot(lhs, b1, cb=cb))


def gram(a_ref, b_ref, mask=None):
    acc = None
    for t in range(N // HALF):
        sl = span(t, HALF)
        lhs = jnp.concatenate(split3(a_ref[:, sl]))
        rhs = jnp.concatenate(split3(b_ref[:, sl]))
        part = bdot(lhs, rhs, 1, 1)
        acc = part if acc is None else acc + part
    acc = fold_rows(acc)
    return sum_of([acc[:, span(q, NB)] for q in reversed(range(3))])


def bcast(v):
    return jnp.broadcast_to(v, TILE)


def qr_step(a_ref, xcur, xnext, stats, pc, pl0, gi, s, last_of_pair, accs):
    beta_ref, inv_ref, tau_ref = stats
    lane = lane_of(TILE)
    sub = lax.broadcasted_iota(jnp.int32, (8, 1), 0)
    n_g = 8 - gi
    j = gi * 8 + s
    p = pl0 + j
    rows = [span(gi + g, 8) for g in range(n_g)]
    dots = [jnp.sum(acc, axis=1, keepdims=True) for acc in accs]
    pvs = [jnp.sum(jnp.where(lane == p, a_ref[pc, r, :], 0.0), axis=1, keepdims=True) for r in rows]
    sigma = jnp.sum(jnp.where(sub == s, dots[0], 0.0), axis=0, keepdims=True)
    alpha = jnp.sum(jnp.where(sub == s, pvs[0], 0.0), axis=0, keepdims=True)
    sq = alpha * alpha + sigma
    inv_norm = lax.rsqrt(sq)
    norm = jnp.sqrt(sq)
    pos = alpha >= 0
    beta = jnp.where(pos, -norm, norm)
    ninvb = jnp.where(pos, inv_norm, -inv_norm)
    denom = alpha - beta
    inv_den = 1.0 / denom
    tau = denom * ninvb
    cs = [(pv + d * inv_den) * ninvb for pv, d in zip(pvs, dots)]
    cs[0] = jnp.where(sub > s, cs[0], 0.0)
    beta_ref[pl.ds(j, 1), :] = jnp.broadcast_to(beta, (1, 128))
    inv_ref[pl.ds(j, 1), :] = jnp.broadcast_to(inv_den, (1, 128))
    tau_ref[pl.ds(j, 1), :] = jnp.broadcast_to(tau, (1, 128))
    c_next = jnp.sum(jnp.where(sub == s + 1, cs[0], 0.0), axis=0, keepdims=True)
    if last_of_pair and n_g > 1:
        c_next = c_next + jnp.where(s == 7, cs[1][0:1], 0.0)
    jn = jnp.minimum(j + 1, NB - 1)
    c_next = bcast(c_next)
    den_b = bcast(denom)
    for ch in range(N_CH):
        xt = xcur[ch]
        if ch == pc:
            xt = jnp.where(lane == p, den_b, xt)
        xn = a_ref[ch, pl.ds(jn, 8, stride=0), :] - c_next * xt
        if ch == pc:
            xn = jnp.where(lane > p + 1, xn, 0.0)
        xnext[ch] = xn
    cs = [bcast(c) for c in cs]
    out = [jnp.zeros(TILE, F32) for _ in range(n_g)]
    for ch in range(N_CH):
        xt = xcur[ch]
        if ch == pc:
            xt = jnp.where(lane == p, den_b, xt)
        xn = xnext[ch]
        for g in range(n_g):
            a = a_ref[ch, rows[g], :] - cs[g] * xt
            a_ref[ch, rows[g], :] = a
            out[g] = out[g] + a * xn
    return tuple(out)


def qr_panel(a_ref, x_refs, stats, pc, pl0):
    lane = lane_of(TILE)
    accs = [jnp.zeros(TILE, F32) for _ in range(8)]
    for ch in range(N_CH):
        x = bcast(a_ref[ch, 0:1, :])
        if ch == pc:
            x = jnp.where(lane > pl0, x, 0.0)
        x_refs[0][ch] = x
        for g in range(8):
            accs[g] = accs[g] + a_ref[ch, span(g, 8), :] * x
    accs = tuple(accs)
    for gi in range(8):

        def pair(h, accs, gi=gi):
            for par in range(2):
                accs = qr_step(a_ref, x_refs[par], x_refs[1 - par], stats, pc, pl0, gi, h * 2 + par, par == 1, accs)
            return accs

        accs = lax.fori_loop(0, 4, pair, accs)[1:]


def finish_panel(a_ref, stats, vt_ref, rt_ref, pc, pl0):
    beta_ref, inv_ref, tau_ref = stats
    lane = lane_of(TILE)
    sub = lax.broadcasted_iota(jnp.int32, TILE, 0)
    for g in range(8):
        rows = span(g, 8)
        inv = inv_ref[rows, :]
        for ch in range(N_CH):
            sl = span(ch)
            a = a_ref[ch, rows, :]
            v = a * inv
            if ch == pc:
                rel = lane - pl0 - (g * 8 + sub)
                rt_ref[rows, :] = jnp.where(rel < 0, a, jnp.where(rel == 0, beta_ref[rows, :], 0.0))
                v = jnp.where(rel > 0, v, jnp.where(rel == 0, 1.0, 0.0))
            vt_ref[rows, sl] = v


def build_tri(gram_mat, tau_col):
    row = lax.broadcasted_iota(jnp.int32, (NB, NB), 0)
    col = lane_of((NB, NB))
    t = jnp.where(row == col, tau_col, 0.0)
    for lg in range(6):
        rb = lax.shift_right_logical(row, lg)
        cb = lax.shift_right_logical(col, lg)
        u = jnp.where((cb == rb + 1) & (lax.rem(rb, 2) == 0), gram_mat, 0.0)
        t = t - mm(mm(t, u), t)
    return t


def panel_kernel(step, *refs):
    refs = list(refs)
    n_rem = PANELS - step
    if step > 0:
        vt_ref, yt_ref, t_pair = refs[:3]
        refs = refs[3:]
    if step == 1:
        pieces, refs = refs[:8], refs[8:]
    elif n_rem:
        pt_ref = refs.pop(0)
    if step > 0:
        wt_ref = refs.pop(0)
    if n_rem:
        small_ref, vn_ref = refs[:2]
        refs = refs[2:]
        if step > 0 and n_rem > 1:
            rem_ref = refs.pop(0)
        a_ref, xa, xb, beta_ref, inv_ref, tau_ref = refs
    lane64 = lane_of(WIDE)
    row64 = lax.broadcasted_iota(jnp.int32, WIDE, 0)
    if step > 0:
        for g in range(step):
            sl = span(8 * g)
            yt_ref[:, sl] = jnp.where(lane64 < NB, 0.0, yt_ref[:, sl])
        s_mat = gram(vt_ref, yt_ref)
        t_mat, t_tr = t_pair[0, :, :NB], t_pair[1, :, :NB]
        m_mat = mm(mm(t_tr, s_mat, 1), t_mat)
        lhs = jnp.concatenate([t_tr, -0.5 * m_mat], axis=1)
        for t in range(N // HALF):
            sl = span(t, HALF)
            wt_ref[:, sl] = mm(lhs, jnp.concatenate([yt_ref[:, sl], vt_ref[:, sl]]))
    if not n_rem:
        return
    if step == 1:
        x, core, y = place()
        for dx in range(2):
            for f in range(2):
                row = 2 * (1 - x if dx else x) + (1 - core if f else core)
                lanes = pl.ds(pl.multiple_of(row * QTR, QTR), QTR)
                here, there = 2 * dx + f, 4 + 2 * dx + f
                first = jnp.where(y == 1, pieces[here][0], pieces[there][0])
                for ch in range(8):
                    a_ref[row * 8 + ch] = first[:, span(ch)]
                one, two = pieces[here][1], pieces[there][1]
                rem_ref[0, :, lanes] = jnp.where(y == 0, one, two)
                rem_ref[1, :, lanes] = jnp.where(y == 1, one, two)
    if step > 0:
        lefts = []
        for q in range(step, PANELS):
            sl = span(8 * q)
            wc = wt_ref[:, sl].T[:NB]
            vc = vt_ref[:, sl].T[:NB]
            lefts.append(jnp.concatenate([wc, vc], axis=1))
        lhs = jnp.concatenate(lefts)
        for t in range(N // 256):
            sl = span(t, TR)
            upd = mm(lhs, jnp.concatenate([vt_ref[:, sl], wt_ref[:, sl]]))
            for h in range(2):
                old = a_ref[2 * t + h] if step == 1 else pt_ref[0, :, span(2 * t + h)]
                a_ref[2 * t + h] = old - upd[:NB, span(h)]
            for q in range(1, n_rem):
                old = rem_ref[q - 1, :, sl] if step == 1 else pt_ref[q, :, sl]
                rem_ref[q - 1, :, sl] = old - upd[span(q, NB)]
    else:
        for ch in range(N_CH):
            a_ref[ch] = pt_ref[:, span(ch)]
    small_ref[0] = jnp.where((lane64 >= row64) & (lane64 < NB), a_ref[step * 8], 0.0)
    for g in range(step + 1):
        a_ref[g * 8] = jnp.where(lane64 < NB, 0.0, a_ref[g * 8])
    pc = ((step + 1) % PANELS) * (QTR // LANE)
    pl0 = NB * ((step + 1) // PANELS)
    stats = (beta_ref, inv_ref, tau_ref)
    qr_panel(a_ref, (xa, xb), stats, pc, pl0)
    finish_panel(a_ref, stats, vn_ref, small_ref.at[1], pc, pl0)
    small_ref[2] = tau_ref[...]


def panel_call(step, *args):
    n_rem = PANELS - step
    outs = []
    full = jax.ShapeDtypeStruct((NB, N), F32)
    scratch = []
    if step > 0:
        outs.append(full)
    if n_rem:
        outs += [jax.ShapeDtypeStruct((3, NB, LANE), F32), full]
        if step > 0 and n_rem > 1:
            outs.append(jax.ShapeDtypeStruct((n_rem - 1, NB, N), F32))
        scratch = [pltpu.VMEM((N_CH, NB, 128), F32), pltpu.VMEM((N_CH, 8, 128), F32), pltpu.VMEM((N_CH, 8, 128), F32)] + [pltpu.VMEM(WIDE, F32)] * 3
    vspec = pl.BlockSpec(memory_space=pltpu.VMEM)
    return pl.pallas_call(
        functools.partial(panel_kernel, step),
        out_shape=outs,
        in_specs=[vspec] * len(args),
        out_specs=[vspec] * len(outs),
        scratch_shapes=scratch,
        compiler_params=pltpu.CompilerParams(vmem_limit_bytes=VMEM_LIMIT),
        cost_estimate=pl.CostEstimate(flops=20_000_000_000, bytes_accessed=8_000_000, transcendentals=0),
        name=f"panel{step}",
    )(*args)


def barrier(neighbours):
    sem = pltpu.get_barrier_semaphore()
    for dev in neighbours:
        pl.semaphore_signal(sem, inc=1, device_id=dev, device_id_type=MESH)
    pl.semaphore_wait(sem, len(neighbours))


def remote(src, dst, send, recv, dev):
    return pltpu.make_async_remote_copy(src_ref=src, dst_ref=dst, send_sem=send, recv_sem=recv, device_id=dev, device_id_type=MESH)


def place():
    my_row = lax.axis_index('row')
    my_col = lax.axis_index('col')
    return lax.div(my_row, 2), lax.rem(my_row, 2), my_col


def device(x, core, y):
    return {'row': 2 * x + core, 'col': y}


def gather_kernel(slab_ref, pt_ref, send, recv, fwd_send, fwd_recv):
    x, core, y = place()
    other = 1 - core
    barrier([device(x, other, y), device(1 - x, core, y), device(1 - x, other, y), device(x, core, 1 - y), device(x, other, 1 - y)])
    n_part = GATHER_PARTS
    width = QTR // n_part

    def lanes(row, part=None):
        if part is None:
            return pl.ds(pl.multiple_of(row * QTR, QTR), QTR)
        return pl.ds(pl.multiple_of(row * QTR + part * width, width), width)

    def push(to_core, dev, part, s_sem, r_sem):
        return remote(slab_ref.at[to_core, :, part * width : (part + 1) * width], pt_ref.at[:, lanes(2 * x + core, part)], s_sem, r_sem, dev)

    def onward(row, part, idx):
        ref = pt_ref.at[:, lanes(row, part)]
        return remote(ref, ref, fwd_send.at[idx, part], fwd_recv.at[idx, part], device(1 - x, core, y))

    my_row = 2 * x + core
    for part in range(n_part):
        to_y = [push(core, device(x, core, 1 - y), part, send.at[0, part], recv.at[0, part]), push(other, device(x, other, 1 - y), part, send.at[1, part], recv.at[1, part])]
        to_x = [push(core, device(1 - x, core, y), part, send.at[2, part], recv.at[2, part]), push(other, device(1 - x, other, y), part, send.at[3, part], recv.at[3, part])]
        to_p = push(other, device(x, other, y), part, send.at[4, part], recv.at[4, part])

        @pl.when(y == 0)
        def _():
            for cp in to_y + to_x + [to_p]:
                cp.start()

    @pl.when(y == 0)
    def _():
        pt_ref[:, lanes(my_row)] = slab_ref[core]
        for part in range(n_part):
            for idx, (tc, dev) in enumerate([(core, device(x, core, 1)), (other, device(x, other, 1)), (core, device(1 - x, core, 0)), (other, device(1 - x, other, 0)), (other, device(x, other, 0))]):
                cp = push(tc, dev, part, send.at[idx, part], recv.at[idx, part])
                cp.wait_send()
                if idx >= 2:
                    cp.wait_recv()

    @pl.when(y == 1)
    def _():
        for part in range(n_part):
            for idx, row in enumerate([my_row, 2 * x + other]):
                push(core, device(x, core, 0), part, send.at[idx, part], recv.at[idx, part]).wait_recv()
                onward(row, part, idx).start()
        for part in range(n_part):
            for idx in range(2):
                onward(my_row, part, idx).wait()


def gather_call(slab):
    vspec = pl.BlockSpec(memory_space=pltpu.VMEM)
    return pl.pallas_call(
        gather_kernel,
        out_shape=jax.ShapeDtypeStruct((NB, N), F32),
        in_specs=[vspec],
        out_specs=vspec,
        scratch_shapes=[*([pltpu.SemaphoreType.DMA((5, GATHER_PARTS))] * 2), *([pltpu.SemaphoreType.DMA((2, GATHER_PARTS))] * 2)],
        compiler_params=pltpu.CompilerParams(collective_id=0, has_side_effects=True, vmem_limit_bytes=VMEM_LIMIT),
        name="gather",
    )(slab)


def rest_of_panels(slab, my_row, pt):
    core = lax.rem(my_row, 2)
    own = lax.dynamic_index_in_dim(slab, core, 0, keepdims=False)
    cross = lax.dynamic_index_in_dim(slab, 1 - core, 0, keepdims=False)
    own, cross, pt = lax.optimization_barrier((own, cross, pt))

    def pairs(dx, dy, f):
        flip = 4 * dy + 2 * dx + f
        return [(d, d ^ flip) for d in range(8)]

    pieces = []
    for dy in range(2):
        for dx in range(2):
            for f in range(2):
                payload = cross if f else own
                pieces.append(payload if (dx, dy, f) == (0, 0, 0) else lax.ppermute(payload, ('col', 'row'), pairs(dx, dy, f)))
    return pieces, pt


def needed(x, y):
    return [quarter(row) for row in (y, 2 + y, 2 * x + 1 - y)]


def swap_kernel(w_ref, *refs):
    smalls, refs = refs[:PANELS], refs[PANELS:]
    t_pairs, (w_out, pack_out, send, recv) = refs[:PANELS], refs[PANELS:]
    x, core, y = place()
    partner = device(x, 1 - core, y)
    barrier([partner])
    moves = [(w_ref.at[:, sl], w_out.at[1, :, sl]) for sl in needed(x, y)]
    for k in range(PANELS):
        moves.append((smalls[k].at[:2], pack_out.at[1, k, :2]))
        moves.append((t_pairs[k].at[0], pack_out.at[1, k, 2]))
    copies = [remote(src, dst, send.at[i], recv.at[i], partner) for i, (src, dst) in enumerate(moves)]
    for cp in copies:
        cp.start()
    w_out[0] = w_ref[...]
    for k in range(PANELS):
        pack_out[0, k, :2] = smalls[k][:2]
        pack_out[0, k, 2] = t_pairs[k][0]
    for cp in copies:
        cp.wait()


def swap_call(w, smalls, t_pairs):
    whole = pl.BlockSpec(memory_space=pltpu.VMEM)
    return pl.pallas_call(
        swap_kernel,
        out_shape=[jax.ShapeDtypeStruct((2, NB, N), F32), jax.ShapeDtypeStruct((2, PANELS, 3, NB, LANE), F32)],
        in_specs=[whole] * (1 + 2 * PANELS),
        out_specs=[whole] * 2,
        scratch_shapes=[pltpu.SemaphoreType.DMA((3 + 2 * PANELS,))] * 2,
        compiler_params=pltpu.CompilerParams(collective_id=5, has_side_effects=True, vmem_limit_bytes=VMEM_LIMIT),
        name="swap",
    )(w, *smalls, *t_pairs)


def step_kernel(update, products, *refs):
    refs = list(refs)
    take = lambda n: [refs.pop(0) for _ in range(n)]
    (l_ref,) = take(1)
    if products:
        va, small_ref = take(2)
    if update:
        uu, ww = take(2)
        wa = ww
        if not products:
            v_rows = take(PANELS)
        (lo_ref,) = take(1)
        if not products:
            (vo_ref,) = take(1)
    if products:
        yt_out, vv_out, t_pair = take(3)
        vv, yt, vc3, vr3, acc1, acc2, p1_ref, p2_ref = take(8)
        r_part, r_own, r_p1, r_p2, sbuf, qbuf, send, recv = take(8)
        v_send, v_recv = take(2)
    if update:
        if products:
            (ww,) = take(1)
        left6, right6 = take(2)
    mat = pl.program_id(0)
    ti = pl.program_id(1)
    x, core, y = place()
    my_row = 2 * x + core
    other = 1 - core
    partner = device(x, other, y)
    x_nbr = device(1 - x, core, y)
    y_nbr = device(x, core, 1 - y)
    y_cross = device(x, other, 1 - y)
    slot = lax.rem(core + mat, 2)
    low_half = lane_of(WIDE) < NB

    if products:
        swaps = [(va, vv)] + ([(wa, ww)] if update else [])
        swaps = [remote(src.at[:, sl], dst.at[1, :, sl], v_send.at[i, q], v_recv.at[i, q], partner) for i, (src, dst) in enumerate(swaps) for q, sl in enumerate(needed(x, y))]

        @pl.when((mat == 0) & (ti == 0))
        def _():
            barrier([partner, x_nbr, y_nbr, y_cross])
            for cp in swaps:
                cp.start()
            vv[0] = va[...]
            if update:
                ww[0] = wa[...]
            t_mat = build_tri(gram(va, va), small_ref[2, :, :NB])
            t_pair[0] = jnp.concatenate([t_mat, jnp.zeros_like(t_mat)], axis=1)
            t_pair[1] = jnp.concatenate([t_pair[0], t_pair[0]]).T[:NB]

        @pl.when((mat == other) & (ti == 0))
        def _():
            for cp in swaps:
                cp.wait()

    def pick(ref, base, ch):
        return ref[slot, :, lane_tile(base * 8 + ch)]

    def col_chunks(ref, u):
        qa = pick(ref, y, u)
        qb = pick(ref, y + 2, u)
        return halves(low_half, qa, qb)

    @pl.when(ti == 0)
    def _():
        if not products:
            for k in range(PANELS):
                for u in range(8):
                    vo_ref[0, k, span(u), :] = v_rows[k][0, :, span(u)].T

        if products:
            acc2[...] = jnp.zeros_like(acc2)
            vc3[3 * NB :, :] = jnp.zeros((NB, COLS), BF16)
            for u in range(8):
                for h, part in enumerate(col_chunks(vv, u)):
                    for q, piece in enumerate(split3(part)):
                        vc3[span(q, NB), lane_tile(2 * u + h)] = piece
                for q, piece in enumerate(split3(pick(vv, my_row, u))):
                    vr3[span(q, NB), lane_tile(u)] = piece

        if update:
            for u in range(8):
                vcs = col_chunks(uu, u)
                wcs = col_chunks(ww, u)
                for h in range(2):
                    r1, r2, r3 = split3(jnp.concatenate([wcs[h], vcs[h]]))
                    for q, piece in enumerate((r3, r2, r1, r2, r1, r1)):
                        right6[span(q), lane_tile(2 * u + h)] = piece
                left = jnp.concatenate([pick(uu, my_row, u), pick(ww, my_row, u)]).T
                a1, a2, a3 = split3(left)
                for q, piece in enumerate((a1, a2, a3, a1, a2, a1)):
                    left6[lane_tile(u), span(q)] = piece

    row_sl = pl.ds(pl.multiple_of(ti * TR, TR), TR)

    def run(tj, diag):
        col_sl = pl.ds(pl.multiple_of(tj * TC, TC), TC)
        tile = l_ref[0, :, col_sl]
        if diag or not products:
            ri = lax.broadcasted_iota(jnp.int32, (TR, TC), 0) + ti * TR
            ci = lane_of((TR, TC)) + tj * TC
            rg = (lax.div(ri, NB) * 4 + my_row) * NB + lax.rem(ri, NB)
            cg = (lax.div(ci, NB) * 2 + y) * NB + lax.rem(ci, NB)
        if update:
            upd = bdot(left6[row_sl, :], right6[:, col_sl])
            tile = tile - (jnp.where(rg >= cg, upd, 0.0) if diag else upd)
            if not products:
                done = PANELS * NB
                tile = jnp.where((rg >= done) & (cg >= done), tile, 0.0)
            lo_ref[0, :, col_sl] = tile
        if products:
            parts = split3(tile)
            vcols = vc3[:, col_sl]
            vrows = vr3[:, row_sl]
            part1, part2, part3 = [bdot(vrows[: (3 - q) * NB], part) for q, part in enumerate(parts)]
            top, mid = span(0, NB), span(1, NB)
            acc2[top, col_sl] += part3 + part2[top] + part1[top]
            acc2[mid, col_sl] += part2[mid] + part1[mid]
            acc2[2 * NB :, col_sl] += part1[2 * NB :]
            if diag:
                parts = [jnp.where(rg == cg, jnp.zeros_like(part), part) for part in parts]
            p1 = fold_rows(bdot(jnp.concatenate(parts), vcols, 1, 1))
            if diag:
                tot = acc1[...] + p1
                tot = (tot[:, :LANE] + tot[:, LANE:]).T
                p1_ref[mat, :, row_sl] = tot[NB:] + tot[:NB]
            else:
                acc1[...] += p1

    if products:
        acc1[...] = jnp.zeros_like(acc1)

    @pl.loop(0, ti)
    def _(tj):
        run(tj, False)

    run(ti, True)

    if update:

        @pl.loop(ti + 1, 4)
        def _(tj):
            lo_ref[0, :, pl.ds(pl.multiple_of(tj * TC, TC), TC)] = jnp.zeros((TR, TC), F32)

    if not products:
        return

    @pl.when(ti == 3)
    def _():
        for u in range(8):
            ev = fold_rows(acc2[:, lane_tile(2 * u)])
            od = fold_rows(acc2[:, lane_tile(2 * u + 1)])
            p2_ref[mat, 0, :, lane_tile(u)], p2_ref[mat, 1, :, lane_tile(u)] = halves(low_half, ev, od)

    mine_part = yt.at[:, quarter(my_q := 2 * x + y)]
    part_y = yt.at[:, half_quarter(2 * x + 1 - y, 0)]
    part_x = yt.at[:, half_quarter(2 * (1 - x) + y, 1)]

    def helper_copies(q):
        part = [remote(p2_ref.at[q, hx], r_part.at[hx], send.at[i], recv.at[i], partner) for i, hx in ((0, 1 - x), (10, x))]
        far = remote(p1_ref.at[q], r_p1, send.at[1], recv.at[1], y_cross)
        near = remote(p1_ref.at[q], r_own, send.at[1], recv.at[2], partner)
        return part, far, near

    def owner_copies(q):
        far = remote(p1_ref.at[q], r_p1, send.at[2], recv.at[1], y_nbr)
        over_x = [remote(sbuf.at[:, span(h, HALF)], r_p2.at[:, span(h, HALF)], send.at[i], recv.at[i], x_nbr) for h, i in enumerate((3, 11))]
        g_x, g_y = [[remote(qbuf.at[:, span(h, HALF)], yt.at[:, half_quarter(2 * x + y, h)], send.at[i + h], recv.at[i + h], dev) for h in range(2)] for i, dev in ((4, x_nbr), (6, y_nbr))]
        f_x = remote(part_y, part_y, send.at[8], recv.at[8], x_nbr)
        f_y = remote(part_x, part_x, send.at[9], recv.at[9], y_nbr)
        return far, over_x, g_x, g_y, f_x, f_y

    def help_out(q):
        part, far, near = helper_copies(q)
        for cp in part:
            cp.start()
        pl.when(core != y)(far.start)
        pl.when(core == y)(near.start)

    def help_end(q):
        part, far, near = helper_copies(q)
        for cp in part:
            cp.wait_send()
        far.wait_send()

    def stage_a(q):
        pl.when(core != y)(owner_copies(q)[0].start)

    def stage_b(q):
        part, _, near = helper_copies(q)
        first, second = part
        first.wait_recv()
        sbuf[...] = p2_ref[q, 1 - x] + r_part[1 - x]
        for cp in owner_copies(q)[1]:
            cp.start()
        second.wait_recv()
        qbuf[...] = p2_ref[q, x] + r_part[x]

        @pl.when(core == y)
        def _():
            qbuf[...] += p1_ref[q]

        @pl.when(core != y)
        def _():
            near.wait_recv()
            qbuf[...] += r_own[...]

    def stage_c(q):
        far, over_x, g_x, g_y, _, _ = owner_copies(q)
        far.wait_recv()
        qbuf[...] += r_p1[...]
        for h, copies in enumerate(zip(over_x, g_y, g_x)):
            came, to_y, to_x = copies
            came.wait()
            qbuf[:, span(h, HALF)] += r_p2[:, span(h, HALF)]
            to_y.start()
            to_x.start()
        mine_part[...] = qbuf[...]

    def stage_d(q):
        _, _, g_x, g_y, f_x, f_y = owner_copies(q)
        g_y[0].wait_recv()
        f_x.start()
        g_x[1].wait_recv()
        f_y.start()

    def stage_e(q):
        far, _, g_x, g_y, f_x, f_y = owner_copies(q)
        pl.when(core != y)(far.wait_send)
        for cp in g_x + g_y:
            cp.wait_send()
        g_x[0].wait_recv()
        g_y[1].wait_recv()
        f_x.wait()
        f_y.wait()

    at = 4 * mat + ti
    last = at == 7
    for when, stage in ((3, stage_a), (5, stage_b), (6, stage_c)):
        pl.when((at == when) & (core == 0))(functools.partial(stage, 0))
    pl.when((at == 3) & (core == 1))(functools.partial(help_out, 0))

    @pl.when(last & (core == 0))
    def _():
        help_out(1)
        stage_d(0)
        stage_e(0)
        help_end(1)

    @pl.when(last & (core == 1))
    def _():
        help_end(0)
        for stage in (stage_a, stage_b, stage_c, stage_d, stage_e):
            stage(1)

    @pl.when(last)
    def _():
        yt_out[...] = yt[...]
        for ch in range(N_CH):
            vv_out[:, :, span(ch)] = vv[:, :, span(ch)]


def step_call(low, v_own, prev, v_rows=()):
    products = v_own is not None
    update = prev is not None
    strip = pl.BlockSpec((1, TR, COLS), lambda m, i: (m, i, 0))
    whole = pl.BlockSpec(memory_space=pltpu.VMEM)
    full, both = jax.ShapeDtypeStruct((NB, N), F32), jax.ShapeDtypeStruct((2, NB, N), F32)
    args, in_specs = [low], [strip]
    outs, out_specs, scratch = [], [], []
    if products:
        args += list(v_own)
        in_specs += [whole] * 2
    if update:
        args += list(prev)
        in_specs += [whole] * len(prev)
        outs.append(jax.ShapeDtypeStruct(low.shape, F32))
        out_specs.append(strip)
    if not products:
        args += v_rows
        in_specs += [pl.BlockSpec((1, NB, QTR), lambda m, i: (lax.rem(lax.axis_index('row') + m, 2), 0, lax.axis_index('row')))] * PANELS
        outs.append(jax.ShapeDtypeStruct((2, PANELS, QTR, NB), F32))
        out_specs.append(pl.BlockSpec((1, PANELS, QTR, NB), lambda m, i: (m, 0, 0, 0)))
    if products:
        outs += [full, both, jax.ShapeDtypeStruct((2, NB, LANE), F32)]
        out_specs += [whole] * 3
        qtr, two = pltpu.VMEM((NB, QTR), F32), pltpu.VMEM((2, NB, QTR), F32)
        scratch += [pltpu.VMEM((2, NB, N), F32), pltpu.VMEM((NB, N), F32)] + [pltpu.VMEM((TR, COLS), BF16), pltpu.VMEM((3 * NB, QTR), BF16), pltpu.VMEM((TR, TR), F32), pltpu.VMEM((3 * NB, COLS), F32)]
        scratch += [two, pltpu.VMEM((2, 2, NB, QTR), F32), two] + [qtr] * 5 + [pltpu.SemaphoreType.DMA((12,))] * 2 + [pltpu.SemaphoreType.DMA((2, 3))] * 2
    if update:
        if products:
            scratch.append(pltpu.VMEM((2, NB, N), F32))
        scratch += [pltpu.VMEM((QTR, 6 * LANE), BF16), pltpu.VMEM((6 * LANE, COLS), BF16)]
    return pl.pallas_call(
        functools.partial(step_kernel, update, products),
        out_shape=outs,
        grid=(2, 4),
        in_specs=in_specs,
        out_specs=out_specs,
        scratch_shapes=scratch,
        compiler_params=pltpu.CompilerParams(vmem_limit_bytes=VMEM_LIMIT, dimension_semantics=("arbitrary",) * 2, **(dict(collective_id=1 + update, has_side_effects=True) if products else {})),
        cost_estimate=pl.CostEstimate(flops=15_000_000_000, bytes_accessed=32_000_000, transcendentals=0),
        name="step",
    )(*args)


def solution(mesh):
    def per_device(lower_tri):
        n_mat, n_rblk, blk, n_cloc = lower_tri.shape
        n_rloc = n_rblk * blk
        my_row = lax.axis_index('row')
        core = lax.rem(my_row, 2)
        low = lower_tri.reshape(n_mat, n_rloc, n_cloc)
        slab = jnp.swapaxes(low[:, :, : 2 * NB], 1, 2).reshape(n_mat, 2, NB, n_rloc)
        pt = gather_call(slab[:, 0])
        pts, pt = rest_of_panels(slab, my_row, pt)
        small, vt = panel_call(0, pt)
        yt, v_both, t_pair = step_call(low, (vt, small), None)
        smalls, t_pairs, v_rows = [small], [t_pair], [v_both]
        for k in range(1, PANELS):
            wt, small, vt_new, *pts = panel_call(k, vt, yt, t_pair, *pts)
            low, yt, v_both, t_pair = step_call(low, (vt_new, small), (v_both, wt))
            smalls.append(small)
            t_pairs.append(t_pair)
            v_rows.append(v_both)
            vt = vt_new
        (wt,) = panel_call(PANELS, vt, yt, t_pair)
        w_both, both = swap_call(wt, smalls, t_pairs)
        low, v_out = step_call(low, None, (v_both, w_both), v_rows)
        both = jnp.where(core == 0, both, both[::-1])
        d_mat = jnp.swapaxes(both[:, :, 0, :, :NB], 2, 3)
        r_mat = jnp.concatenate([both[:, :-1, 1, :, :NB], both[:, -1:, 1, :, NB:]], axis=1)
        band = jnp.stack([d_mat, jnp.swapaxes(r_mat, 2, 3)], axis=2)
        return low.reshape(lower_tri.shape), band, v_out.reshape(n_mat, PANELS, n_rblk, blk, blk), both[:, :, 2, :, :NB]

    spec_low = P('sys', 'row', None, 'col')
    return jax.shard_map(per_device, mesh=mesh, in_specs=(spec_low,), out_specs=(spec_low, P('sys'), P('sys', None, 'row', None, None), P('sys')), check_vma=False)
```
